256 devices in a mesh: dp: 32 (over x, y, core), tensor: 8 (over z).
Axes of the slice: x: 4, y: 4, z: 8, core: 2. Of those that a mesh axis runs over, the one named last changes fastest.
Arguments:
- proxy_hidden: bfloat16 [1536, 4096], P('dp', 'tensor'), may hold values from -176.625 to 176.625
- reference_hidden: bfloat16 [1536, 4096], P('dp', 'tensor'), may hold values from -176.625 to 176.625
- proxy_head: bfloat16 [128256, 4096], P(('dp', 'tensor')), may hold values from -0.09375 to 0.09375
- reference_head: bfloat16 [128256, 4096], P(('dp', 'tensor')), may hold values from -0.09375 to 0.09375
- targets: int32 [1536], P('dp'), may hold values from 0 to 128255
- domains: int32 [1536], P('dp'), may hold values from 0 to 127
- keep_mask: int32 [1536], P('dp'), may hold values 0 or 1
- prior_weights: float32 [128], replicated, may hold values from 0.5 to 2
Outputs:
- excess: float32 [1536], P('dp')
- log_weights: float32 [128], replicated
The draws below stay inside these ranges and needn't reach their ends.
All inputs are finite; a program needn't handle non-finite values. No bound on the sum of `keep_mask` on one device may be relied on, other than what follows from the above.
Results may differ from the reference program's by a relative error of at most 0.00045.
Values may be sent and summed in bfloat16 or wider, within the bound.
A program may use at most 128 MiB of HBM per device.

```python
import math
import jax
import jax.numpy as jnp
from jax import lax

D = 4096
VOCAB_DEV = 501
DOMAINS = 128
STEPS = 3
TOKENS = 1536
VOCAB = 128256


def head_rows(key, salt, rows):
    base = jax.random.fold_in(key, salt)

    def one_row(row_id):
        values = jax.random.normal(jax.random.fold_in(base, row_id), (D,), jnp.float32)
        return jnp.clip(values, -6.0, 6.0) * D ** (-0.5)
    return jax.vmap(one_row)(rows)


def hidden_matrix(key, salt):
    base = jax.random.fold_in(key, salt)
    values = jnp.clip(jax.random.normal(base, (TOKENS, D), jnp.float32), -6.0, 6.0) * 3.0
    return values.astype(jnp.bfloat16)


def draw_proxy_head(key, part):
    return head_rows(key, 101, jnp.arange(VOCAB, dtype=jnp.int32)).astype(jnp.bfloat16)


def draw_reference_head(key, part):
    return head_rows(key, 102, jnp.arange(VOCAB, dtype=jnp.int32)).astype(jnp.bfloat16)


def draw_proxy_hidden(key, part):
    return hidden_matrix(key, 201)


def draw_reference_hidden(key, part):
    return hidden_matrix(key, 202)


def set_ends(entries, key, smallest, largest):
    longest = entries.shape.index(max(entries.shape))
    spots = []
    for shift in (0, 1):
        where = [jax.random.randint(jax.random.fold_in(key, axis), (), 0, length) for axis, length in enumerate(entries.shape)]
        where[longest] = (where[longest] + shift) % entries.shape[longest]
        spots.append(tuple(where))
    return entries.at[spots[0]].set(smallest).at[spots[1]].set(largest)


def setup_inputs(seed: int = 0) -> dict:
    streams_of = jax.random.split(jax.random.key(seed), 9)
    return {
        "proxy_hidden": draw_proxy_hidden(jax.random.fold_in(streams_of[8], 71), 0),
        "reference_hidden": draw_reference_hidden(jax.random.fold_in(streams_of[8], 71), 0),
        "proxy_head": draw_proxy_head(jax.random.fold_in(streams_of[8], 71), 0),
        "reference_head": draw_reference_head(jax.random.fold_in(streams_of[8], 71), 0),
        "targets": set_ends(jax.random.randint(streams_of[4], (TOKENS,), 0, VOCAB), jax.random.fold_in(streams_of[4], 1), 0, VOCAB - 1).astype(jnp.int32),
        "domains": set_ends(jax.random.randint(streams_of[5], (TOKENS,), 0, DOMAINS), jax.random.fold_in(streams_of[5], 1), 0, DOMAINS - 1).astype(jnp.int32),
        "keep_mask": set_ends((jax.random.randint(streams_of[6], (TOKENS,), 0, 8) < 7).astype(jnp.int32), jax.random.fold_in(streams_of[6], 1), 0, 1),
        "prior_weights": jnp.clip(jnp.exp(jax.random.uniform(streams_of[7], (DOMAINS,), jnp.float32, math.log(0.5), math.log(2.0))), 0.5, 2.0),
    }


step_size = 1.0
smoothing = 0.001


def model_loss(hidden, head, targets):
    blocks = VOCAB // VOCAB_DEV
    grouped = head.reshape(blocks, VOCAB_DEV, D)
    firsts = jnp.arange(blocks, dtype=jnp.int32) * VOCAB_DEV
    columns = jnp.arange(VOCAB_DEV, dtype=jnp.int32)

    def visit(state, inputs):
        run_peak, run_total, run_hit = state
        block_head, first_col = inputs
        logits = lax.dot_general(hidden, block_head, (((1,), (1,)), ((), ())), preferred_element_type=jnp.float32)
        new_peak = jnp.maximum(run_peak, jnp.max(logits, axis=1))
        run_total = run_total * jnp.exp(run_peak - new_peak) + jnp.sum(jnp.exp(logits - new_peak[:, None]), axis=1)
        matched = (targets - first_col)[:, None] == columns[None, :]
        run_hit = run_hit + jnp.sum(jnp.where(matched, logits, 0.0), axis=1)
        return (new_peak, run_total, run_hit), None

    zeros_row = jnp.zeros((TOKENS,), jnp.float32)
    start_state = (jnp.full((TOKENS,), -jnp.inf, jnp.float32), zeros_row, zeros_row)
    final_state, _unused = lax.scan(visit, start_state, (grouped, firsts))
    final_peak, final_total, final_hit = final_state
    return final_peak + jnp.log(final_total) - final_hit


def update_weights(prior_weights, clipped, domains, keep):
    weights = prior_weights / jnp.sum(prior_weights)
    batch_rows = clipped.shape[0] // STEPS
    labels = jnp.arange(DOMAINS, dtype=jnp.int32)
    for section_index in range(STEPS):
        row_start = section_index * batch_rows
        block_loss = clipped[row_start:row_start + batch_rows]
        block_keep = keep[row_start:row_start + batch_rows]
        member = (domains[row_start:row_start + batch_rows][:, None] == labels[None, :]).astype(jnp.float32)
        domain_sum = jnp.dot(block_loss, member, precision=lax.Precision.HIGHEST)
        domain_count = jnp.dot(block_keep, member, precision=lax.Precision.HIGHEST)
        domain_gain = domain_sum / jnp.maximum(domain_count, 1.0)
        raised = weights * jnp.exp(step_size * domain_gain)
        weights = (1.0 - smoothing) * raised / jnp.sum(raised) + smoothing / DOMAINS
    return jnp.log(weights)


def reference(proxy_hidden, reference_hidden, proxy_head, reference_head, targets, domains, keep_mask, prior_weights):
    proxy_loss = model_loss(proxy_hidden, proxy_head, targets)
    reference_loss = model_loss(reference_hidden, reference_head, targets)
    keep = keep_mask.astype(jnp.float32)
    loss_gap = proxy_loss - reference_loss
    excess = loss_gap * keep
    clipped = jnp.maximum(loss_gap, 0.0) * keep
    log_weights = update_weights(prior_weights, clipped, domains, keep)
    return excess, log_weights
```

```python
import jax
import jax.numpy as jnp
from jax import lax
from jax.experimental import pallas as pl
from jax.experimental.pallas import tpu as pltpu
from jax.sharding import Mesh
from jax.sharding import PartitionSpec as P

DOMAINS = 128
STEPS = 3
DP = ("dp_0", "dp_1", "dp_2")
DP_TENSOR = ("dp_0", "dp_1", "dp_2", "tensor")
AXIS = {"x": "dp_0", "y": "dp_1", "z": "tensor"}
MESH = pl.DeviceIdType.MESH

step_size = 1.0
smoothing = 0.001

KB = 1024
RATE = 46.6e3
HOP = 2.4
START = 2.0
LEAD = 3.0
RING4 = (0, 1, -1, 2)
RING8 = (0, 1, -1, 2, -2, 3, -3, 4)


def ring(add, axis, size, token, deps, far, rank):
    for k in range(1, far + 1):
        half = (0, 1) if k == far else (None, None)
        part = size // 2 if k == far else size
        for sign, h in ((1, half[0]), (-1, half[1])):
            source = token(-sign * (k - 1), h)
            given = token(far if k == far else -sign * k, h)
            need = deps if k == 1 else [token(-sign * (k - 1), None)]
            add(axis, sign, part, source, need, given, rank + 0.01 * k)


def gather_plan():
    copies = []

    def add(axis, sign, size, source, need, given, rank):
        copies.append(
            dict(axis=axis, sign=sign, size=size, source=source, need=need, given=given, rank=rank)
        )

    piece = 32 * KB
    for colour, first, last in (("A", "y", "x"), ("B", "x", "y")):
        ring(add, "z", piece, lambda d, h: (colour, "z", d, h), [(colour, "z", 0, None)], 4, 0)
        for dz in RING8:
            have = [(colour, "z", dz, None)]
            ring(add, first, piece, lambda d, h: (colour, "f", dz, d, h), have, 2, 1)
            full = have + [(colour, "f", dz, d, None) for d in (1, -1, 2)]
            ring(add, last, 4 * piece, lambda d, h: (colour, "l", dz, d, h), full, 2, 3)
    piece = 16 * KB
    for colour, first, last in (("C0", "x", "y"), ("C1", "y", "x")):
        own = [(colour, "f", 0, None)]
        ring(add, first, piece, lambda d, h: (colour, "f", d, h), own, 2, 0)
        full = own + [(colour, "f", d, None) for d in (1, -1, 2)]
        ring(add, last, 4 * piece, lambda d, h: (colour, "l", d, h), full, 2, 0)
        for j in RING4:
            have = full if j == 0 else [(colour, "l", j, None)]
            ring(add, "z", 4 * piece, lambda d, h: (colour, "z", j, d, h), have, 4, 2)
    return copies


def parts_of(token, known):
    if token in known:
        return [token]
    return [token[:-1] + (0,), token[:-1] + (1,)]


OWN = {("A", "z", 0, None), ("B", "z", 0, None), ("C0", "f", 0, None), ("C1", "f", 0, None)}


def schedule(copies, computes):
    known = {c["given"] for c in copies} | OWN
    for c in copies:
        c["deps"] = [p for t in c["need"] for p in parts_of(t, known)]
    have = {t: START for t in OWN}
    free = {}
    waiting = list(range(len(copies)))
    while waiting:
        best = None
        for i in waiting:
            c = copies[i]
            if all(d in have for d in c["deps"]):
                ready = max(have[d] for d in c["deps"])
                link = (c["axis"], c["sign"])
                begin = max(ready, free.get(link, START))
                key = (begin, c["rank"], ready, i)
                if best is None or key < best:
                    best = key
        begin, _, ready, i = best
        c = copies[i]
        c["start"], c["ready"] = begin, ready
        free[(c["axis"], c["sign"])] = begin + c["size"] / RATE
        have[c["given"]] = begin + c["size"] / RATE + HOP
        waiting.remove(i)
    events = []
    for i, c in enumerate(copies):
        events.append((have[c["given"]], 0, i, "recv"))
        events.append((max(c["ready"], c["start"] - LEAD), 1, i, "send"))
    for i, (_, tokens) in enumerate(computes):
        when = max(have[p] for t in tokens for p in parts_of(t, known))
        events.append((when, 2, i, "compute"))
    return [(kind, i) for _, _, i, kind in sorted(events)]


def group_tokens(group, dzs):
    out = []
    for dz in dzs:
        if group == "C":
            for colour in ("C0", "C1"):
                for j in RING4:
                    if dz != 0:
                        out.append((colour, "z", j, dz, None))
                    elif j != 0:
                        out += [(colour, "l", j, None), (colour, "f", j, None)]
        else:
            for colour in ("A", "B"):
                if group == 0:
                    out += [(colour, "z", dz, None)]
                    out += [(colour, "f", dz, d, None) for d in (1, -1, 2)]
                elif group == 1:
                    out += [(colour, "l", dz, d, None) for d in (1, -1)]
                else:
                    out += [(colour, "l", dz, 2, None)]
    return out


WORK = [
    (0, (0, 1, -1)), (0, (2, -2)), (0, (3, -3, 4)),
    (1, (0, 1, -1)), (1, (2, -2)), (1, (3, -3, 4)),
    (2, (0, 1, -1)), (2, (2, -2)), (2, (3, -3)), (2, (4,)),
    ("C", (0, 1, -1)), ("C", (2, -2)), ("C", (3, -3)), ("C", (4,)),
]


def flat(x):
    return x.reshape(x.shape[0] * x.shape[1], x.shape[2]) if x.ndim == 3 else x


def kernel(
    copies, order, rows,
    ph, rh, pw, rw, meta_in, out,
    G, W, acc0, acc1, acc2, accC, M0, M1, st, zbuf, ybuf, xbuf, dbuf,
    own_sem, head_sem, swap_send, swap_recv, g_send, g_recv, m_send, m_recv, s_send, s_recv,
):
    x, y, c, z = (lax.axis_index(a) for a in ("dp_0", "dp_1", "dp_2", "tensor"))
    other = 1 - c
    pos = {"x": (x, 4), "y": (y, 4), "z": (z, 8)}

    def at(axis, d):
        p, n = pos[axis]
        return lax.rem(p + (d % n), n) if d % n else p

    def peer(axis, d):
        return {AXIS[axis]: at(axis, d)}

    def cols(dz, half=None):
        begin = at("z", dz) * 512
        if half is None:
            return pl.ds(pl.multiple_of(begin, 512), 512)
        return pl.ds(pl.multiple_of(begin + 256 * half, 256), 256)

    def view(token):
        colour, phase, half = token[0], token[1], token[-1]
        if colour in ("A", "B"):
            k = 0 if colour == "A" else 1
            last, first = ("x", "y") if colour == "A" else ("y", "x")
            ms = slice(0, 2) if half is None else half
            dz = token[2]
            if phase == "z":
                return G.at[k, ms, at(last, 0), at(first, 0), :, cols(dz)]
            if phase == "f":
                return G.at[k, ms, at(last, 0), at(first, token[3]), :, cols(dz)]
            return G.at[k, ms, at(last, token[3]), :, :, cols(dz)]
        d = token[2]
        if phase == "f":
            if colour == "C0":
                return G.at[2, 0, at("x", d), y, :, cols(0, half)]
            return G.at[2, 1, x, at("y", d), :, cols(0, half)]
        cs = cols(0 if phase == "l" else token[3], half)
        if colour == "C0":
            return G.at[2, 0, :, at("y", d), :, cs]
        return G.at[2, 1, at("x", d), :, :, cs]

    def gather_copy(i, token, sign):
        ref = view(token)
        return pltpu.make_async_remote_copy(
            src_ref=ref, dst_ref=ref, send_sem=g_send.at[i], recv_sem=g_recv.at[i],
            device_id=peer(copies[i]["axis"], sign), device_id_type=MESH,
        )

    own = []
    for m, src in enumerate((ph, rh)):
        for k in range(3):
            dst = G.at[k, m, y, x, :, cols(0)] if k == 1 else G.at[k, m, x, y, :, cols(0)]
            own.append(pltpu.make_async_copy(src.at[pl.ds(16 * k, 16), :], dst, own_sem.at[3 * m + k]))
    own.append(pltpu.make_async_copy(meta_in, M0.at[y], own_sem.at[6]))
    for copy in own:
        copy.start()
    heads = (pw, rw)
    mine = [pltpu.make_async_copy(heads[m], W.at[m, 0], head_sem.at[m]) for m in (0, 1)]
    for copy in mine:
        copy.start()

    barrier = pltpu.get_barrier_semaphore()
    peers = [peer("z", d) for d in range(1, 8)] + [peer(a, d) for a in "xy" for d in (1, 2, 3)]
    peers.append({"dp_2": other})
    for target in peers:
        pl.semaphore_signal(barrier, inc=1, device_id=target, device_id_type=MESH)
    st[...] = jnp.zeros_like(st)
    pl.semaphore_wait(barrier, len(peers))

    for copy in own:
        copy.wait()

    def meta_copy(i, axis, d, sending):
        slot = at(axis, 0 if sending else -d)
        src, dst = (M0.at[slot], M0.at[slot]) if axis == "y" else (M0, M1.at[slot])
        return pltpu.make_async_remote_copy(
            src_ref=src, dst_ref=dst, send_sem=m_send.at[i], recv_sem=m_recv.at[i],
            device_id=peer(axis, d), device_id_type=MESH,
        )

    for d in (1, 2, 3):
        meta_copy(d - 1, "y", d, True).start()

    def swap_copy(i, m, dz):
        return pltpu.make_async_remote_copy(
            src_ref=heads[m].at[:, cols(dz)], dst_ref=W.at[m, 1, :, cols(dz)],
            send_sem=swap_send.at[i], recv_sem=swap_recv.at[i],
            device_id={"dp_2": other}, device_id_type=MESH,
        )

    swaps = {(m, dz): (2 * q + m) for q, dz in enumerate(RING8) for m in (0, 1)}

    f32 = jnp.float32
    lane = lax.broadcasted_iota(jnp.int32, (8, 128), 1)
    sub = lax.broadcasted_iota(jnp.int32, (8, 128), 0)
    accs = {0: acc0, 1: acc1, 2: acc2, "C": accC}

    def block(group, m, dz):
        cs = cols(dz)
        if group == "C":
            return G[2, m, :, :, :, cs].reshape(256, 512)
        pieces = []
        for d in {0: (0,), 1: (-1, 1), 2: (2,)}[group]:
            pieces.append(G[0, m, at("x", d), :, :, cs].reshape(64, 512))
            pieces.append(G[1, m, at("y", d), :, :, cs].reshape(64, 512))
        return jnp.concatenate(pieces, axis=0)

    done_heads = set()

    def compute(i):
        group, dzs = WORK[i]
        if "own" not in done_heads:
            for copy in mine:
                copy.wait()
            done_heads.add("own")
        for dz in dzs:
            for m in (0, 1):
                if (m, dz) not in done_heads:
                    swap_copy(swaps[(m, dz)], m, dz).wait_recv()
                    done_heads.add((m, dz))
        acc = accs[group]
        first = 0 in dzs

        def body(m, carry):
            rhs = [block(group, m, dz) for dz in dzs]
            for h in (0, 1):
                total = None
                for dz, r in zip(dzs, rhs):
                    part = lax.dot_general(
                        W[m, h, :, cols(dz)], r, (((1,), (1,)), ((), ())), preferred_element_type=f32
                    )
                    total = part if total is None else total + part
                acc[m, h] = total if first else acc[m, h] + total
            return carry

        lax.fori_loop(0, 2, body, 0)

    dev = ((x * 4 + y) * 2 + c) * 8 + z
    dev_other = ((x * 4 + y) * 2 + other) * 8 + z
    offsets = (dev * rows, dev_other * rows)

    def spread(quantity):
        j = lax.broadcasted_iota(jnp.int32, (128, 128), 0)
        l = lax.broadcasted_iota(jnp.int32, (128, 128), 1)
        low = l % 16
        sel_ab = (j == low + jnp.where(l < 64, 0, 16)).astype(f32)
        sel_c = (j == low + 32).astype(f32)
        ab = jnp.dot(quantity, sel_ab, precision=lax.Precision.HIGHEST, preferred_element_type=f32)
        cc = jnp.dot(quantity, sel_c, precision=lax.Precision.HIGHEST, preferred_element_type=f32)
        d = lax.broadcasted_iota(jnp.int32, (16, 128), 0)
        l = lax.broadcasted_iota(jnp.int32, (16, 128), 1)
        q = (l // 16) % 4
        result = jnp.zeros((8, 128), f32)
        for a in range(4):
            owner = jnp.where(l < 64, a * 4 + q, q * 4 + a)
            row = jnp.sum(jnp.where(d == owner, ab, 0.0), axis=0, keepdims=True)
            result = jnp.where(sub == a, row, result)
        for a in range(2):
            owner = (2 * a + l // 64) * 4 + q
            row = jnp.sum(jnp.where(d == owner, cc, 0.0), axis=0, keepdims=True)
            result = jnp.where(sub == 4 + a, row, result)
        return result

    def stats(group, wanted):
        acc = accs[group]
        width = acc.shape[-1]
        if group == "C":
            places = [sub == 4, sub == 5]
        else:
            places = [
                sub == jnp.where(lane < 64, at("x", d), at("y", d))
                for d in {0: (0,), 1: (-1, 1), 2: (2,)}[group]
            ]
        want = [jnp.sum(jnp.where(p, wanted, 0.0), axis=0, keepdims=True) for p in places]
        want = jnp.concatenate(want, axis=1).astype(jnp.int32) if len(want) > 1 else want[0].astype(jnp.int32)
        vocab = lax.broadcasted_iota(jnp.int32, (rows, width), 0)
        lses, hits = [], []
        for m in (0, 1):
            peak = jnp.maximum(
                jnp.max(acc[m, 0], axis=0, keepdims=True), jnp.max(acc[m, 1], axis=0, keepdims=True)
            )
            total = jnp.zeros((1, width), f32)
            hit = jnp.zeros((1, width), f32)
            for h in (0, 1):
                logits = acc[m, h]
                total += jnp.sum(jnp.exp(logits - peak), axis=0, keepdims=True)
                match = vocab == want - offsets[h]
                hit += jnp.sum(jnp.where(match, logits, 0.0), axis=0, keepdims=True)
            lses.append(peak + jnp.log(total))
            hits.append(hit)
        for k, row in enumerate((lses[0], lses[1], hits[0] - hits[1])):
            value = st[k]
            for b, place in enumerate(places):
                value = jnp.where(place, row[:, 128 * b : 128 * (b + 1)], value)
            st[k] = value

    started_swaps = False
    meta_done = False
    tables = {}
    pending = {g: sum(1 for w in WORK if w[0] == g) for g in accs}
    for kind, i in order:
        if kind == "send":
            gather_copy(i, copies[i]["source"], copies[i]["sign"]).start()
        elif kind == "recv":
            if not started_swaps:
                for (m, dz), s in swaps.items():
                    swap_copy(s, m, dz).start()
                started_swaps = True
            gather_copy(i, copies[i]["given"], copies[i]["sign"]).wait_recv()
        else:
            if not meta_done:
                meta_done = True
                for d in (1, 2, 3):
                    meta_copy(d - 1, "y", d, False).wait_recv()
                M1[x] = M0[...]
                for d in (1, 2, 3):
                    meta_copy(2 + d, "x", d, True).start()
            compute(i)
            group = WORK[i][0]
            pending[group] -= 1
            if not pending[group]:
                if not tables:
                    for d in (1, 2, 3):
                        meta_copy(2 + d, "x", d, False).wait_recv()
                    for k, name in enumerate(("targets", "domains", "keep")):
                        tables[name] = spread(M1[:, :, k, :].reshape(16, 128))
                stats(group, tables["targets"])

    def exchange(buf, axis, base):
        n = pos[axis][1]

        def copy(d, slot):
            return pltpu.make_async_remote_copy(
                src_ref=buf.at[slot], dst_ref=buf.at[slot],
                send_sem=s_send.at[base + d - 1], recv_sem=s_recv.at[base + d - 1],
                device_id=peer(axis, d), device_id_type=MESH,
            )

        for d in range(1, n):
            copy(d, at(axis, 0)).start()
        for d in range(1, n):
            copy(d, at(axis, -d)).wait_recv()
        parts = [[buf[s, k] for k in range(3)] for s in range(n)]
        combined = []
        for k in (0, 1):
            peak = parts[0][k]
            for s in range(1, n):
                peak = jnp.maximum(peak, parts[s][k])
            total = jnp.exp(parts[0][k] - peak)
            for s in range(1, n):
                total = total + jnp.exp(parts[s][k] - peak)
            combined.append(peak + jnp.log(total))
        hit = parts[0][2]
        for s in range(1, n):
            hit = hit + parts[s][2]
        combined.append(hit)
        return combined, [copy(d, at(axis, 0)) for d in range(1, n)]

    zbuf[z] = st[...]
    result, sent_z = exchange(zbuf, "z", 0)
    for k in range(3):
        ybuf[y, k] = result[k]
    result, sent_y = exchange(ybuf, "y", 7)
    for k in range(3):
        xbuf[x, k] = result[k]
    (lse0, lse1, hit), sent_x = exchange(xbuf, "x", 10)

    keep = tables["keep"]
    gap = (lse0 - lse1) - hit
    excess = gap * keep
    clipped = jnp.maximum(gap, 0.0) * keep
    q = (lane // 16) % 4
    low = lane % 16
    owner = jnp.where(sub < 4, jnp.where(lane < 64, sub * 4 + q, q * 4 + sub), (2 * (sub - 4) + lane // 64) * 4 + q)
    colour = jnp.where(sub < 4, jnp.where(lane < 64, 0, 1), 2)
    token = (owner * 2 + c) * 48 + 16 * colour + low
    batch = token // 512
    label = lax.broadcasted_iota(jnp.int32, (128, 128), 0).astype(f32)
    left, right = [], []
    for b in range(6):
        bb = batch[b : b + 1, :]
        top = jnp.where(bb == sub, clipped[b : b + 1, :], 0.0)
        low_rows = jnp.where(bb == sub - 3, keep[b : b + 1, :], 0.0)
        left.append(jnp.where(sub < 3, top, low_rows))
        right.append((tables["domains"][b : b + 1, :] == label).astype(f32))
    sums = lax.dot_general(
        jnp.concatenate(left, axis=1), jnp.concatenate(right, axis=1), (((1,), (1,)), ((), ())),
        precision=lax.Precision.HIGHEST, preferred_element_type=f32,
    )
    dbuf[c] = sums

    def last_copy(slot):
        return pltpu.make_async_remote_copy(
            src_ref=dbuf.at[slot], dst_ref=dbuf.at[slot], send_sem=s_send.at[13], recv_sem=s_recv.at[13],
            device_id={"dp_2": other}, device_id_type=MESH,
        )

    last_copy(c).start()
    me = x * 4 + y
    here = jnp.where((owner == me) & (sub < 6), excess, 0.0)
    j = lax.broadcasted_iota(jnp.int32, (128, 128), 0)
    l = lax.broadcasted_iota(jnp.int32, (128, 128), 1)
    sel_ab = (j == l % 16 + jnp.where(l < 64, 0, 16)).astype(f32)
    sel_c = (j == l % 16 + 32).astype(f32)
    spots = jnp.concatenate([jnp.where(sub < 4, here, 0.0), jnp.where(sub >= 4, here, 0.0)], axis=1)
    mine_out = lax.dot_general(
        spots, jnp.concatenate([sel_ab, sel_c], axis=1), (((1,), (1,)), ((), ())),
        precision=lax.Precision.HIGHEST, preferred_element_type=f32,
    )
    mine_row = jnp.sum(mine_out, axis=0, keepdims=True)
    prior = M0[y, 3:4, :]
    weights = prior / jnp.sum(prior, axis=1, keepdims=True)
    last_copy(other).wait_recv()
    both = dbuf[0] + dbuf[1]
    for s in range(STEPS):
        gain = both[s : s + 1, :] / jnp.maximum(both[3 + s : 4 + s, :], 1.0)
        raised = weights * jnp.exp(step_size * gain)
        weights = (1.0 - smoothing) * raised / jnp.sum(raised, axis=1, keepdims=True) + smoothing / DOMAINS
    out[...] = jnp.where(sub == 0, jnp.log(weights), mine_row)

    for i, cp in enumerate(copies):
        gather_copy(i, cp["source"], cp["sign"]).wait_send()
    for (m, dz), s in swaps.items():
        swap_copy(s, m, dz).wait_send()
    for d in (1, 2, 3):
        meta_copy(d - 1, "y", d, True).wait_send()
        meta_copy(2 + d, "x", d, True).wait_send()
    for copy in sent_z + sent_y + sent_x:
        copy.wait_send()
    last_copy(c).wait_send()


def local(ph, rh, pw, rw, targets, domains, keep_mask, prior):
    def line(a):
        return jnp.pad(a.astype(jnp.float32), (0, 128 - a.shape[0]))[None]

    meta = jnp.concatenate(
        [line(targets), line(domains), line(keep_mask), line(prior), jnp.zeros((4, 128), jnp.float32)]
    )
    rows = pw.shape[0]
    copies = gather_plan()
    order = schedule(copies, [(w, group_tokens(*w)) for w in WORK])
    f32, bf16 = jnp.float32, jnp.bfloat16
    dma = pltpu.SemaphoreType.DMA
    anywhere = pl.BlockSpec(memory_space=pl.ANY)

    def body(*refs):
        kernel(copies, order, rows, *refs)

    out = pl.pallas_call(
        body,
        name="doremi",
        out_shape=jax.ShapeDtypeStruct((8, 128), f32),
        in_specs=[anywhere] * 5,
        out_specs=pl.BlockSpec(memory_space=pltpu.VMEM),
        scratch_shapes=[
            pltpu.VMEM((3, 2, 4, 4, 16, 4096), bf16),
            pltpu.VMEM((2, 2, rows, 4096), bf16),
            pltpu.VMEM((2, 2, rows, 128), f32),
            pltpu.VMEM((2, 2, rows, 256), f32),
            pltpu.VMEM((2, 2, rows, 128), f32),
            pltpu.VMEM((2, 2, rows, 256), f32),
            pltpu.VMEM((4, 8, 128), f32),
            pltpu.VMEM((4, 4, 8, 128), f32),
            pltpu.VMEM((3, 8, 128), f32),
            pltpu.VMEM((8, 3, 8, 128), f32),
            pltpu.VMEM((4, 3, 8, 128), f32),
            pltpu.VMEM((4, 3, 8, 128), f32),
            pltpu.VMEM((2, 8, 128), f32),
            dma((7,)), dma((2,)), dma((16,)), dma((16,)),
            dma((len(copies),)), dma((len(copies),)),
            dma((6,)), dma((6,)), dma((14,)), dma((14,)),
        ],
        compiler_params=pltpu.CompilerParams(
            collective_id=0, has_side_effects=True, vmem_limit_bytes=60 * 1024 * 1024
        ),
        cost_estimate=pl.CostEstimate(flops=12_900_000_000, bytes_accessed=34_000_000, transcendentals=2_000_000),
    )(ph, rh, pw, rw, meta)
    return out[1, : targets.shape[0]], out[0]


def solution(mesh):
    split = Mesh(
        mesh.devices.reshape(4, 4, 2, mesh.shape["tensor"]), ("dp_0", "dp_1", "dp_2", "tensor")
    )
    return jax.shard_map(
        local,
        mesh=split,
        in_specs=(
            P(DP, "tensor"),
            P(DP, "tensor"),
            P(DP_TENSOR, None),
            P(DP_TENSOR, None),
            P(DP),
            P(DP),
            P(DP),
            P(),
        ),
        out_specs=(P(DP), P()),
        check_vma=False,
    )
```

```python
import jax
import jax.numpy as jnp
from jax import lax
from jax.experimental import pallas as pl
from jax.experimental.pallas import tpu as pltpu
from jax.sharding import Mesh
from jax.sharding import PartitionSpec as P

DOMAINS = 128
STEPS = 3
DP = ("dp_0", "dp_1", "dp_2")
DP_TENSOR = ("dp_0", "dp_1", "dp_2", "tensor")
AXIS = {"x": "dp_0", "y": "dp_1", "z": "tensor"}
MESH = pl.DeviceIdType.MESH

step_size = 1.0
smoothing = 0.001

KB = 1024
RATE = 46.6e3
HOP = 3.5
BACKLOG = 2.5
LAG = 0.45
FINE = (0, 1, -1)
RING4 = (0, 1, -1, 2)
RING8 = (0, 1, -1, 2, -2, 3, -3, 4)


def ring(add, axis, size, token, need, far, rank, arrival, lag=0.01):
    for k in range(1, far + 1):
        halves = (0, 1) if k == far else (None, None)
        for sign, half in ((1, halves[0]), (-1, halves[1])):
            offset = far if k == far else -sign * k
            add(
                dict(
                    axis=axis,
                    sign=sign,
                    size=size // 2 if k == far else size,
                    source=token(-sign * (k - 1), half),
                    need=need if k == 1 else [token(-sign * (k - 1), None)],
                    given=token(offset, half),
                    rank=rank + lag * (k - 1),
                    arrival=arrival + (offset,),
                )
            )


def gather_plan():
    copies = []
    add = copies.append
    piece = 32 * KB
    for colour, first, last in (("A", "y", "x"), ("B", "x", "y")):
        own = [(colour, "z", 0, None)]
        ring(add, "z", piece, lambda d, h: (colour, "z", d, h), own, 4, 0, (colour, "z"))
        for q, dz in enumerate(RING8):
            have = [(colour, "z", dz, None)]
            ring(add, first, piece, lambda d, h: (colour, "f", dz, d, h), have, 2, 1, (colour, "f", dz))
            rank = 3 + 0.1 * q
            if dz in FINE:
                for df in RING4:
                    need = have if df == 0 else [(colour, "f", dz, df, None)]
                    token = lambda d, h: (colour, "p", dz, df, d, h)
                    ring(add, last, piece, token, need, 2, rank, (colour, "p", dz, df), LAG)
            else:
                need = have + [(colour, "f", dz, d, None) for d in (1, -1, 2)]
                token = lambda d, h: (colour, "l", dz, d, h)
                ring(add, last, 4 * piece, token, need, 2, rank, (colour, "l", dz), LAG)
    piece = 16 * KB
    own = [("C", "o", 0, None)]
    ring(add, "z", 2 * piece, lambda d, h: ("C", "o", d, h), own, 4, 2, ("C", "o"))
    for colour, first, last in (("C0", "x", "y"), ("C1", "y", "x")):
        ring(add, first, piece, lambda d, h: (colour, "f", d, h), own, 2, 0, (colour, "f"))
        need = own + [(colour, "f", d, None) for d in (1, -1, 2)]
        ring(add, last, 4 * piece, lambda d, h: (colour, "l", d, h), need, 2, 0, (colour, "l"))
        for j in (1, -1, 2):
            need = [(colour, "f", j, None)]
            ring(add, "z", piece, lambda d, h: (colour, "y", j, d, h), need, 4, 2, ("C", "y", j))
        for j in (1, -1, 2):
            need = [(colour, "l", j, None)]
            ring(add, "z", 4 * piece, lambda d, h: (colour, "z", j, d, h), need, 4, 2, ("C", "z", j))
    return copies


OWN = {("A", "z", 0, None), ("B", "z", 0, None), ("C", "o", 0, None)}


def tokens_of(group, dzs):
    out = []
    for dz in dzs:
        if group == "C":
            if dz:
                out.append(("C", "o", dz, None))
            for colour in ("C0", "C1"):
                for j in (1, -1, 2):
                    if dz:
                        out += [(colour, "y", j, dz, None), (colour, "z", j, dz, None)]
                    else:
                        out += [(colour, "f", j, None), (colour, "l", j, None)]
            continue
        for colour in ("A", "B"):
            if group == 0:
                out += [(colour, "z", dz, None)] + [(colour, "f", dz, d, None) for d in (1, -1, 2)]
                continue
            for d in (1, -1) if group == 1 else (2,):
                if dz in FINE:
                    out += [(colour, "p", dz, df, d, None) for df in RING4]
                else:
                    out.append((colour, "l", dz, d, None))
    return out


WORK = [
    (0, (0,)), (0, (1, -1)), (0, (2, -2)), (0, (3, -3, 4)),
    (1, (0,)), (1, (1, -1)), (1, (2, -2)), (1, (3, -3)), (1, (4,)),
    (2, (0,)), (2, (1, -1)), (2, (2, -2)), (2, (3, -3)), (2, (4,)),
    ("C", (0,)), ("C", (1, -1)), ("C", (2, -2)), ("C", (3, -3)), ("C", (4,)),
]
STATS_TIME = {0: 0.34, 1: 0.74, 2: 0.34, "C": 0.74}


def schedule(copies, works):
    arrival_of = {c["given"]: c["arrival"] for c in copies}
    members = {}
    for i, c in enumerate(copies):
        members.setdefault(c["arrival"], []).append(i)

    def arrivals(tokens):
        found = set()
        for t in tokens:
            if t not in OWN:
                found |= {arrival_of[p] for p in (t, t[:-1] + (0,), t[:-1] + (1,)) if p in arrival_of}
        return found

    deps = [arrivals(c["need"]) for c in copies]
    needs = [arrivals(tokens_of(*w)) for w in works]
    links = {}
    for i, c in enumerate(copies):
        links.setdefault((c["axis"], c["sign"]), []).append(i)
    got, free, landed = set(), dict.fromkeys(links, 0.0), {}
    unsent, undone = set(range(len(copies))), set(range(len(works)))
    left = {g: sum(1 for w in works if w[0] == g) for g in STATS_TIME}
    now, order = 0.0, []
    while unsent or undone or len(got) < len(members):
        coming = {
            a: max(landed[i] for i in m)
            for a, m in members.items()
            if a not in got and all(i in landed for i in m)
        }
        here = sorted((when, str(a), a) for a, when in coming.items() if when <= now + 1e-9)
        if here:
            for _, _, a in here:
                got.add(a)
                order.append(("recv", a))
                now += 0.02
            continue
        sent = False
        for link, all_of in links.items():
            while free[link] - now < BACKLOG:
                ready = [i for i in all_of if i in unsent and deps[i] <= got]
                if not ready:
                    break
                i = min(ready, key=lambda i: (copies[i]["rank"], i))
                free[link] = max(now, free[link]) + copies[i]["size"] / RATE
                landed[i] = free[link] + HOP
                unsent.discard(i)
                order.append(("send", i))
                now += 0.012
                sent = True
        if sent:
            continue
        ready = [i for i in undone if needs[i] <= got]
        if ready:
            i = min(ready)
            undone.discard(i)
            order.append(("compute", i))
            now += 0.35 + 0.54 * len(works[i][1])
            left[works[i][0]] -= 1
            if not left[works[i][0]]:
                now += STATS_TIME[works[i][0]]
            continue
        times = list(coming.values())
        for link, all_of in links.items():
            if any(i in unsent and deps[i] <= got for i in all_of):
                times.append(free[link] - BACKLOG + 1e-6)
        now = max(now, min(times))
    return order


SEND_CLASS = {
    ("A", "z"): 0, ("A", "f"): 1, ("A", "p"): 2, ("A", "l"): 2,
    ("B", "z"): 3, ("B", "f"): 4, ("B", "p"): 5, ("B", "l"): 5,
    ("C", "o"): 6, ("C0", "y"): 6, ("C1", "y"): 6, ("C0", "z"): 6, ("C1", "z"): 6,
    ("C0", "f"): 7, ("C1", "f"): 7, ("C0", "l"): 8, ("C1", "l"): 8,
}


def kernel(
    copies, order, rows, tokens,
    ph, rh, pw, rw, tg, dm, kp, pr, out_excess, out_weights,
    G, W, acc0, acc1, acc2, accC, tgv, dmv, kpv, prv, M0, M1, st, zbuf, ybuf, xbuf, dbuf,
    own_sem, small_sem, head_sem, swap_send, swap_recv, g_send, g_recv, m_send, m_recv, s_send, s_recv,
):
    x, y, c, z = (lax.axis_index(a) for a in ("dp_0", "dp_1", "dp_2", "tensor"))
    other = 1 - c
    pos = {"x": (x, 4), "y": (y, 4), "z": (z, 8)}

    def at(axis, d):
        p, n = pos[axis]
        return lax.rem(p + (d % n), n) if d % n else p

    def peer(axis, d):
        return {AXIS[axis]: at(axis, d)}

    def cols(dz, half=None):
        begin = at("z", dz) * 512
        if half is None:
            return pl.ds(pl.multiple_of(begin, 512), 512)
        return pl.ds(pl.multiple_of(begin + 256 * half, 256), 256)

    def view(token):
        colour, phase, half = token[0], token[1], token[-1]
        ms = slice(0, 2) if half is None else half
        if colour in ("A", "B"):
            k = 0 if colour == "A" else 1
            last, first = ("x", "y") if colour == "A" else ("y", "x")
            dz = token[2]
            if phase == "z":
                return G.at[k, ms, at(last, 0), at(first, 0), :, cols(dz)]
            if phase == "f":
                return G.at[k, ms, at(last, 0), at(first, token[3]), :, cols(dz)]
            if phase == "p":
                return G.at[k, ms, at(last, token[4]), at(first, token[3]), :, cols(dz)]
            return G.at[k, ms, at(last, token[3]), :, :, cols(dz)]
        d = token[2]
        if colour == "C":
            return G.at[2, ms, x, y, :, cols(d)]
        if phase in ("f", "y"):
            cs = cols(0 if phase == "f" else token[3], half)
            if colour == "C0":
                return G.at[2, 0, at("x", d), y, :, cs]
            return G.at[2, 1, x, at("y", d), :, cs]
        cs = cols(0 if phase == "l" else token[3], half)
        if colour == "C0":
            return G.at[2, 0, :, at("y", d), :, cs]
        return G.at[2, 1, at("x", d), :, :, cs]

    arrival_at = {}
    for cp in copies:
        arrival_at.setdefault(cp["arrival"], [len(arrival_at), 0])[1] += cp["size"]
    amounts = {
        16 * KB: G.at[0, 0, 0, 0, :, pl.ds(0, 512)],
        32 * KB: G.at[0, :, 0, 0, :, pl.ds(0, 512)],
        64 * KB: G.at[0, 0, 0, :, :, pl.ds(0, 512)],
        128 * KB: G.at[0, :, 0, :, :, pl.ds(0, 512)],
    }

    def wait(ref, sem):
        pltpu.make_async_copy(ref, ref, sem).wait()

    def send(i):
        cp = copies[i]
        ref = view(cp["source"])
        pltpu.make_async_remote_copy(
            src_ref=ref, dst_ref=ref,
            send_sem=g_send.at[SEND_CLASS[cp["source"][:2]]], recv_sem=g_recv.at[arrival_at[cp["arrival"]][0]],
            device_id=peer(cp["axis"], cp["sign"]), device_id_type=MESH,
        ).start()

    def receive(arrival):
        index, size = arrival_at[arrival]
        wait(amounts[size], g_recv.at[index])

    for k, (src, dst) in enumerate(((tg, tgv), (dm, dmv), (kp, kpv), (pr, prv))):
        pltpu.make_async_copy(src, dst, small_sem.at[k]).start()
    for m, src in enumerate((ph, rh)):
        for k in range(3):
            dst = G.at[k, m, y, x, :, cols(0)] if k == 1 else G.at[k, m, x, y, :, cols(0)]
            pltpu.make_async_copy(src.at[pl.ds(16 * k, 16), :], dst, own_sem).start()
    heads = (pw, rw)
    for m in (0, 1):
        pltpu.make_async_copy(heads[m], W.at[m, 0], head_sem).start()

    barrier = pltpu.get_barrier_semaphore()
    peers = [peer("z", d) for d in range(1, 8)] + [peer(a, d) for a in "xy" for d in (1, 2, 3)]
    peers.append({"dp_2": other})
    for target in peers:
        pl.semaphore_signal(barrier, inc=1, device_id=target, device_id_type=MESH)
    st[...] = jnp.zeros_like(st)
    M0[y] = jnp.zeros((8, 128), jnp.float32)
    for k, (src, dst) in enumerate(((tg, tgv), (dm, dmv), (kp, kpv), (pr, prv))):
        pltpu.make_async_copy(src, dst, small_sem.at[k]).wait()
    for k, ref in enumerate((tgv, dmv, kpv)):
        M0[y, k : k + 1, 0:tokens] = ref[...].astype(jnp.float32)
    with jax.named_scope("entry_barrier"):
        pl.semaphore_wait(barrier, len(peers))
    with jax.named_scope("own_blocks"):
        wait(G.at[:, :, 0, 0, :, pl.ds(0, 512)], own_sem)

    def meta_send(axis, d):
        src, dst, k = (M0.at[y], M0.at[y], 0) if axis == "y" else (M0, M1.at[x], 1)
        pltpu.make_async_remote_copy(
            src_ref=src, dst_ref=dst, send_sem=m_send.at[k], recv_sem=m_recv.at[k],
            device_id=peer(axis, d), device_id_type=MESH,
        ).start()

    def swap(m, dz, q):
        pltpu.make_async_remote_copy(
            src_ref=heads[m].at[:, cols(dz)], dst_ref=W.at[m, 1, :, cols(dz)],
            send_sem=swap_send, recv_sem=swap_recv.at[q],
            device_id={"dp_2": other}, device_id_type=MESH,
        ).start()

    f32 = jnp.float32
    lane = lax.broadcasted_iota(jnp.int32, (8, 128), 1)
    sub = lax.broadcasted_iota(jnp.int32, (8, 128), 0)
    accs = {0: acc0, 1: acc1, 2: acc2, "C": accC}

    def block(group, m, dz):
        cs = cols(dz)
        if group == "C":
            return G[2, m, :, :, :, cs].reshape(256, 512)
        pieces = []
        for d in {0: (0,), 1: (-1, 1), 2: (2,)}[group]:
            pieces.append(G[0, m, at("x", d), :, :, cs].reshape(64, 512))
            pieces.append(G[1, m, at("y", d), :, :, cs].reshape(64, 512))
        return jnp.concatenate(pieces, axis=0)

    done_heads = set()

    def compute(i):
        group, dzs = WORK[i]
        if not done_heads:
            wait(W.at[:, 0], head_sem)
        for dz in dzs:
            if dz not in done_heads:
                wait(W.at[:, 1, :, cols(dz)], swap_recv.at[RING8.index(dz)])
                done_heads.add(dz)
        acc = accs[group]
        first = 0 in dzs

        def body(m, carry):
            rhs = [block(group, m, dz) for dz in dzs]
            for h in (0, 1):
                total = None
                for dz, r in zip(dzs, rhs):
                    part = lax.dot_general(
                        W[m, h, :, cols(dz)], r, (((1,), (1,)), ((), ())), preferred_element_type=f32
                    )
                    total = part if total is None else total + part
                acc[m, h] = total if first else acc[m, h] + total
            return carry

        lax.fori_loop(0, 2, body, 0)

    dev = ((x * 4 + y) * 2 + c) * 8 + z
    dev_other = ((x * 4 + y) * 2 + other) * 8 + z
    offsets = (dev * rows, dev_other * rows)

    def spread(quantity):
        j = lax.broadcasted_iota(jnp.int32, (128, 128), 0)
        l = lax.broadcasted_iota(jnp.int32, (128, 128), 1)
        low = l % 16
        sel_ab = (j == low + jnp.where(l < 64, 0, 16)).astype(f32)
        sel_c = (j == low + 32).astype(f32)
        ab = jnp.dot(quantity, sel_ab, precision=lax.Precision.HIGHEST, preferred_element_type=f32)
        cc = jnp.dot(quantity, sel_c, precision=lax.Precision.HIGHEST, preferred_element_type=f32)
        d = lax.broadcasted_iota(jnp.int32, (16, 128), 0)
        l = lax.broadcasted_iota(jnp.int32, (16, 128), 1)
        q = (l // 16) % 4
        result = jnp.zeros((8, 128), f32)
        for a in range(4):
            owner = jnp.where(l < 64, a * 4 + q, q * 4 + a)
            row = jnp.sum(jnp.where(d == owner, ab, 0.0), axis=0, keepdims=True)
            result = jnp.where(sub == a, row, result)
        for a in range(2):
            owner = (2 * a + l // 64) * 4 + q
            row = jnp.sum(jnp.where(d == owner, cc, 0.0), axis=0, keepdims=True)
            result = jnp.where(sub == 4 + a, row, result)
        return result

    def stats(group, wanted):
        acc = accs[group]
        width = acc.shape[-1]
        if group == "C":
            places = [sub == 4, sub == 5]
        else:
            places = [
                sub == jnp.where(lane < 64, at("x", d), at("y", d))
                for d in {0: (0,), 1: (-1, 1), 2: (2,)}[group]
            ]
        want = [jnp.sum(jnp.where(p, wanted, 0.0), axis=0, keepdims=True) for p in places]
        want = jnp.concatenate(want, axis=1).astype(jnp.int32) if len(want) > 1 else want[0].astype(jnp.int32)
        vocab = lax.broadcasted_iota(jnp.int32, (rows, width), 0)
        lses, hits = [], []
        for m in (0, 1):
            peak = jnp.maximum(
                jnp.max(acc[m, 0], axis=0, keepdims=True), jnp.max(acc[m, 1], axis=0, keepdims=True)
            )
            total = jnp.zeros((1, width), f32)
            hit = jnp.zeros((1, width), f32)
            for h in (0, 1):
                logits = acc[m, h]
                total += jnp.sum(jnp.exp(logits - peak), axis=0, keepdims=True)
                match = vocab == want - offsets[h]
                hit += jnp.sum(jnp.where(match, logits, 0.0), axis=0, keepdims=True)
            lses.append(peak + jnp.log(total))
            hits.append(hit)
        for k, row in enumerate((lses[0], lses[1], hits[0] - hits[1])):
            value = st[k]
            for b, place in enumerate(places):
                value = jnp.where(place, row[:, 128 * b : 128 * (b + 1)], value)
            st[k] = value

    tables = {}
    pending = {g: sum(1 for w in WORK if w[0] == g) for g in accs}
    steps = 0
    for kind, i in order:
        if kind == "send":
            send(i)
        elif kind == "recv":
            if not steps:
                for d in (1, 2, 3):
                    meta_send("y", d)
                for q, dz in enumerate(RING8):
                    for m in (0, 1):
                        swap(m, dz, q)
            steps += 1
            with jax.named_scope("recv"):
                receive(i)
        else:
            if not done_heads:
                wait(M0.at[pl.ds(0, 3)], m_recv.at[0])
                M1[x] = M0[...]
                for d in (1, 2, 3):
                    meta_send("x", d)
            with jax.named_scope(f"compute_{i}"):
                compute(i)
            group = WORK[i][0]
            pending[group] -= 1
            if not pending[group]:
                if not tables:
                    wait(M1.at[pl.ds(0, 3)], m_recv.at[1])
                    for k, name in enumerate(("targets", "domains", "keep")):
                        tables[name] = spread(M1[:, :, k, :].reshape(16, 128))
                with jax.named_scope(f"stats_{group}"):
                    stats(group, tables["targets"])

    def exchange(buf, axis, stage):
        n, mine = pos[axis][1], pos[axis][0]
        for d in range(1, n):
            pltpu.make_async_remote_copy(
                src_ref=buf.at[mine], dst_ref=buf.at[mine],
                send_sem=s_send.at[stage], recv_sem=s_recv.at[stage],
                device_id=peer(axis, d), device_id_type=MESH,
            ).start()
        wait(buf.at[pl.ds(0, n - 1)], s_recv.at[stage])
        parts = [[buf[s, k] for k in range(3)] for s in range(n)]
        combined = []
        for k in (0, 1):
            peak = parts[0][k]
            for s in range(1, n):
                peak = jnp.maximum(peak, parts[s][k])
            total = jnp.exp(parts[0][k] - peak)
            for s in range(1, n):
                total = total + jnp.exp(parts[s][k] - peak)
            combined.append(peak + jnp.log(total))
        hit = parts[0][2]
        for s in range(1, n):
            hit = hit + parts[s][2]
        combined.append(hit)
        return combined

    zbuf[z] = st[...]
    with jax.named_scope("exchange_z"):
        result = exchange(zbuf, "z", 0)
    for k in range(3):
        ybuf[y, k] = result[k]
    with jax.named_scope("exchange_y"):
        result = exchange(ybuf, "y", 1)
    for k in range(3):
        xbuf[x, k] = result[k]
    with jax.named_scope("exchange_x"):
        lse0, lse1, hit = exchange(xbuf, "x", 2)

    keep = tables["keep"]
    gap = (lse0 - lse1) - hit
    excess = gap * keep
    clipped = jnp.maximum(gap, 0.0) * keep
    q = (lane // 16) % 4
    low = lane % 16
    owner = jnp.where(sub < 4, jnp.where(lane < 64, sub * 4 + q, q * 4 + sub), (2 * (sub - 4) + lane // 64) * 4 + q)
    colour = jnp.where(sub < 4, jnp.where(lane < 64, 0, 1), 2)
    token = (owner * 2 + c) * 48 + 16 * colour + low
    batch = token // 512
    label = lax.broadcasted_iota(jnp.int32, (128, 128), 0).astype(f32)
    left, right = [], []
    for b in range(6):
        bb = batch[b : b + 1, :]
        top = jnp.where(bb == sub, clipped[b : b + 1, :], 0.0)
        low_rows = jnp.where(bb == sub - 3, keep[b : b + 1, :], 0.0)
        left.append(jnp.where(sub < 3, top, low_rows))
        right.append((tables["domains"][b : b + 1, :] == label).astype(f32))
    sums = lax.dot_general(
        jnp.concatenate(left, axis=1), jnp.concatenate(right, axis=1), (((1,), (1,)), ((), ())),
        precision=lax.Precision.HIGHEST, preferred_element_type=f32,
    )
    dbuf[c] = sums

    def last_copy(slot):
        return pltpu.make_async_remote_copy(
            src_ref=dbuf.at[slot], dst_ref=dbuf.at[slot], send_sem=s_send.at[3], recv_sem=s_recv.at[3],
            device_id={"dp_2": other}, device_id_type=MESH,
        )

    last_copy(c).start()
    me = x * 4 + y
    here = jnp.where((owner == me) & (sub < 6), excess, 0.0)
    j = lax.broadcasted_iota(jnp.int32, (128, 128), 0)
    l = lax.broadcasted_iota(jnp.int32, (128, 128), 1)
    sel_ab = (j == l % 16 + jnp.where(l < 64, 0, 16)).astype(f32)
    sel_c = (j == l % 16 + 32).astype(f32)
    spots = jnp.concatenate([jnp.where(sub < 4, here, 0.0), jnp.where(sub >= 4, here, 0.0)], axis=1)
    mine_out = lax.dot_general(
        spots, jnp.concatenate([sel_ab, sel_c], axis=1), (((1,), (1,)), ((), ())),
        precision=lax.Precision.HIGHEST, preferred_element_type=f32,
    )
    mine_row = jnp.sum(mine_out, axis=0, keepdims=True)
    prior = prv[...]
    weights = prior / jnp.sum(prior, axis=1, keepdims=True)
    with jax.named_scope("partner_sums"):
        last_copy(other).wait_recv()
    both = dbuf[0] + dbuf[1]
    for s in range(STEPS):
        gain = both[s : s + 1, :] / jnp.maximum(both[3 + s : 4 + s, :], 1.0)
        raised = weights * jnp.exp(step_size * gain)
        weights = (1.0 - smoothing) * raised / jnp.sum(raised, axis=1, keepdims=True) + smoothing / DOMAINS
    out_weights[...] = jnp.log(weights)
    out_excess[...] = mine_row[:, 0:tokens]

    with jax.named_scope("sends_done"):
        for k in range(2):
            wait(G.at[k, :, 0, 0, :, pl.ds(0, 7 * 512)], g_send.at[3 * k])
            wait(G.at[k, :, 0, pl.ds(0, 3)], g_send.at[3 * k + 1])
            wait(G.at[k, :, pl.ds(0, 3)], g_send.at[3 * k + 2])
        wait(G.at[2, :, :, :, :, pl.ds(0, 7 * 512)], g_send.at[6])
        wait(G.at[2, :, pl.ds(0, 3), 0, :, pl.ds(0, 512)], g_send.at[7])
        wait(G.at[2, :, pl.ds(0, 3), :, :, pl.ds(0, 512)], g_send.at[8])
        wait(W.at[:, 1], swap_send)
        wait(M0.at[pl.ds(0, 3)], m_send.at[0])
        wait(M1.at[pl.ds(0, 3)], m_send.at[1])
        wait(zbuf.at[pl.ds(0, 7)], s_send.at[0])
        wait(ybuf.at[pl.ds(0, 3)], s_send.at[1])
        wait(xbuf.at[pl.ds(0, 3)], s_send.at[2])
        last_copy(c).wait_send()


def local(ph, rh, pw, rw, targets, domains, keep_mask, prior):
    rows, tokens = pw.shape[0], targets.shape[0]
    copies = gather_plan()
    order = schedule(copies, WORK)
    arrivals = len({c["arrival"] for c in copies})
    f32, bf16 = jnp.float32, jnp.bfloat16
    dma = pltpu.SemaphoreType.DMA
    anywhere = pl.BlockSpec(memory_space=pl.ANY)

    def body(*refs):
        kernel(copies, order, rows, tokens, *refs)

    out = pl.pallas_call(
        body,
        name="doremi",
        out_shape=[jax.ShapeDtypeStruct((1, tokens), f32), jax.ShapeDtypeStruct((1, 128), f32)],
        in_specs=[anywhere] * 8,
        out_specs=[pl.BlockSpec(memory_space=pltpu.VMEM)] * 2,
        scratch_shapes=[
            pltpu.VMEM((3, 2, 4, 4, 16, 4096), bf16),
            pltpu.VMEM((2, 2, rows, 4096), bf16),
            pltpu.VMEM((2, 2, rows, 128), f32),
            pltpu.VMEM((2, 2, rows, 256), f32),
            pltpu.VMEM((2, 2, rows, 128), f32),
            pltpu.VMEM((2, 2, rows, 256), f32),
            pltpu.VMEM((1, tokens), jnp.int32),
            pltpu.VMEM((1, tokens), jnp.int32),
            pltpu.VMEM((1, tokens), jnp.int32),
            pltpu.VMEM((1, 128), f32),
            pltpu.VMEM((4, 8, 128), f32),
            pltpu.VMEM((4, 4, 8, 128), f32),
            pltpu.VMEM((3, 8, 128), f32),
            pltpu.VMEM((8, 3, 8, 128), f32),
            pltpu.VMEM((4, 3, 8, 128), f32),
            pltpu.VMEM((4, 3, 8, 128), f32),
            pltpu.VMEM((2, 8, 128), f32),
            dma, dma((4,)), dma, dma, dma((8,)),
            dma((9,)), dma((arrivals,)),
            dma((2,)), dma((2,)), dma((4,)), dma((4,)),
        ],
        compiler_params=pltpu.CompilerParams(
            collective_id=0, has_side_effects=True, vmem_limit_bytes=60 * 1024 * 1024
        ),
        cost_estimate=pl.CostEstimate(flops=12_900_000_000, bytes_accessed=34_000_000, transcendentals=2_000_000),
    )(ph, rh, pw, rw, targets[None], domains[None], keep_mask[None], prior[None])
    return out[0][0], out[1][0]


def solution(mesh):
    split = Mesh(
        mesh.devices.reshape(4, 4, 2, mesh.shape["tensor"]), ("dp_0", "dp_1", "dp_2", "tensor")
    )
    return jax.shard_map(
        local,
        mesh=split,
        in_specs=(
            P(DP, "tensor"),
            P(DP, "tensor"),
            P(DP_TENSOR, None),
            P(DP_TENSOR, None),
            P(DP),
            P(DP),
            P(DP),
            P(),
        ),
        out_specs=(P(DP), P()),
        check_vma=False,
    )
```

```python
import jax
import jax.numpy as jnp
from jax import lax
from jax.experimental import pallas as pl
from jax.experimental.pallas import tpu as pltpu
from jax.sharding import Mesh
from jax.sharding import PartitionSpec as P

DOMAINS = 128
STEPS = 3
DP = ("dp_0", "dp_1", "dp_2")
DP_TENSOR = ("dp_0", "dp_1", "dp_2", "tensor")
AXIS = {"x": "dp_0", "y": "dp_1", "z": "tensor"}
MESH = pl.DeviceIdType.MESH

step_size = 1.0
smoothing = 0.001

KB = 1024
RATE = 46.6e3
HOP = 3.5
BACKLOG = 1.5
LAG = 0.6
FINE = (0, 1, -1)
RING4 = (0, 1, -1, 2)
RING8 = (0, 1, -1, 2, -2, 3, -3, 4)


def ring(add, axis, size, token, need, far, rank, arrival, lag=0.01):
    for k in range(1, far + 1):
        halves = (0, 1) if k == far else (None, None)
        for sign, half in ((1, halves[0]), (-1, halves[1])):
            offset = far if k == far else -sign * k
            add(
                dict(
                    axis=axis,
                    sign=sign,
                    size=size // 2 if k == far else size,
                    source=token(-sign * (k - 1), half),
                    need=need if k == 1 else [token(-sign * (k - 1), None)],
                    given=token(offset, half),
                    rank=rank + lag * (k - 1),
                    arrival=arrival + (offset,),
                )
            )


def gather_plan():
    copies = []
    add = copies.append
    piece = 32 * KB
    for colour, first, last in (("A", "y", "x"), ("B", "x", "y")):
        own = [(colour, "z", 0, None)]
        ring(add, "z", piece, lambda d, h: (colour, "z", d, h), own, 4, 0, ("AB", "z"))
        for q, dz in enumerate(RING8):
            have = [(colour, "z", dz, None)]
            ring(add, first, piece, lambda d, h: (colour, "f", dz, d, h), have, 2, 1, ("AB", "f", dz))
            rank = 3 + 0.1 * q
            if dz in FINE:
                for df in RING4:
                    need = have if df == 0 else [(colour, "f", dz, df, None)]
                    token = lambda d, h: (colour, "p", dz, df, d, h)
                    ring(add, last, piece, token, need, 2, rank, ("AB", "p", dz, abs(df)), LAG)
            else:
                need = have + [(colour, "f", dz, d, None) for d in (1, -1, 2)]
                token = lambda d, h: (colour, "l", dz, d, h)
                ring(add, last, 4 * piece, token, need, 2, rank, ("AB", "l", dz), LAG)
    piece = 16 * KB
    own = [("C", "o", 0, None)]
    ring(add, "z", 2 * piece, lambda d, h: ("C", "o", d, h), own, 4, 2, ("C", "o"))
    for colour, first, last in (("C0", "x", "y"), ("C1", "y", "x")):
        ring(add, first, piece, lambda d, h: (colour, "f", d, h), own, 2, 0, ("C", "f"))
        need = own + [(colour, "f", d, None) for d in (1, -1, 2)]
        ring(add, last, 4 * piece, lambda d, h: (colour, "l", d, h), need, 2, 0, ("C", "l"))
        for j in (1, -1, 2):
            need = [(colour, "f", j, None)]
            ring(add, "z", piece, lambda d, h: (colour, "y", j, d, h), need, 4, 2, ("C", "y", j))
        for j in (1, -1, 2):
            need = [(colour, "l", j, None)]
            ring(add, "z", 4 * piece, lambda d, h: (colour, "z", j, d, h), need, 4, 2, ("C", "z", j))
    return copies


OWN = {("A", "z", 0, None), ("B", "z", 0, None), ("C", "o", 0, None)}


def tokens_of(group, dzs):
    out = []
    for dz in dzs:
        if group == "C":
            if dz:
                out.append(("C", "o", dz, None))
            for colour in ("C0", "C1"):
                for j in (1, -1, 2):
                    if dz:
                        out += [(colour, "y", j, dz, None), (colour, "z", j, dz, None)]
                    else:
                        out += [(colour, "f", j, None), (colour, "l", j, None)]
            continue
        for colour in ("A", "B"):
            if group == 0:
                out += [(colour, "z", dz, None)] + [(colour, "f", dz, d, None) for d in (1, -1, 2)]
                continue
            for d in (1, -1) if group == 1 else (2,):
                if dz in FINE:
                    out += [(colour, "p", dz, df, d, None) for df in RING4]
                else:
                    out.append((colour, "l", dz, d, None))
    return out


WORK = [
    (0, (0,)), (0, (1, -1)), (0, (2, -2)), (0, (3, -3, 4)),
    (1, (0,)), (1, (1, -1)), (1, (2, -2)), (1, (3, -3)), (1, (4,)),
    (2, (0,)), (2, (1, -1)), (2, (2, -2)), (2, (3, -3)), (2, (4,)),
    ("C", (0,)), ("C", (1, -1)), ("C", (2, -2)), ("C", (3, -3)), ("C", (4,)),
]
STATS_TIME = {0: 0.34, 1: 0.74, 2: 0.34, "C": 0.74}


def schedule(copies, works):
    arrival_of = {c["given"]: c["arrival"] for c in copies}
    members = {}
    for i, c in enumerate(copies):
        members.setdefault(c["arrival"], []).append(i)

    def arrivals(tokens):
        found = set()
        for t in tokens:
            if t not in OWN:
                found |= {arrival_of[p] for p in (t, t[:-1] + (0,), t[:-1] + (1,)) if p in arrival_of}
        return found

    deps = [arrivals(c["need"]) for c in copies]
    needs = [arrivals(tokens_of(*w)) for w in works]
    links = {}
    for i, c in enumerate(copies):
        links.setdefault((c["axis"], c["sign"]), []).append(i)
    got, free, landed = set(), dict.fromkeys(links, 0.0), {}
    unsent, undone = set(range(len(copies))), set(range(len(works)))
    left = {g: sum(1 for w in works if w[0] == g) for g in STATS_TIME}
    now, order = 0.0, []
    while unsent or undone or len(got) < len(members):
        coming = {
            a: max(landed[i] for i in m)
            for a, m in members.items()
            if a not in got and all(i in landed for i in m)
        }
        here = sorted((when, str(a), a) for a, when in coming.items() if when <= now + 1e-9)
        if here:
            for _, _, a in here:
                got.add(a)
                order.append(("recv", a))
                now += 0.02
            continue
        sent = False
        for link, all_of in links.items():
            while free[link] - now < BACKLOG:
                ready = [i for i in all_of if i in unsent and deps[i] <= got]
                if not ready:
                    break
                i = min(ready, key=lambda i: (copies[i]["rank"], i))
                free[link] = max(now, free[link]) + copies[i]["size"] / RATE
                landed[i] = free[link] + HOP
                unsent.discard(i)
                order.append(("send", i))
                now += 0.012
                sent = True
        if sent:
            continue
        ready = [i for i in undone if needs[i] <= got]
        if ready:
            i = min(ready)
            undone.discard(i)
            order.append(("compute", i))
            now += 0.25 + 0.54 * len(works[i][1])
            left[works[i][0]] -= 1
            if not left[works[i][0]]:
                now += STATS_TIME[works[i][0]]
            continue
        times = list(coming.values())
        for link, all_of in links.items():
            if any(i in unsent and deps[i] <= got for i in all_of):
                times.append(free[link] - BACKLOG + 1e-6)
        now = max(now, min(times))
    return order


SEND_CLASS = {
    ("A", "z"): 0, ("A", "f"): 1, ("A", "p"): 2, ("A", "l"): 2,
    ("B", "z"): 3, ("B", "f"): 4, ("B", "p"): 5, ("B", "l"): 5,
    ("C", "o"): 6, ("C0", "y"): 6, ("C1", "y"): 6, ("C0", "z"): 6, ("C1", "z"): 6,
    ("C0", "f"): 7, ("C1", "f"): 7, ("C0", "l"): 8, ("C1", "l"): 8,
}


def kernel(
    copies, order, rows, tokens,
    ph, rh, pw, rw, tg, dm, kp, pr, out_excess, out_weights,
    G, W, acc0, acc1, acc2, accC, tgv, dmv, kpv, prv, M0, M1, st, zbuf, ybuf, xbuf, dbuf,
    own_sem, small_sem, head_sem, swap_send, swap_recv, g_send, g_recv, m_send, m_recv, s_send, s_recv,
):
    x, y, c, z = (lax.axis_index(a) for a in ("dp_0", "dp_1", "dp_2", "tensor"))
    other = 1 - c
    pos = {"x": (x, 4), "y": (y, 4), "z": (z, 8)}

    def at(axis, d):
        p, n = pos[axis]
        return lax.rem(p + (d % n), n) if d % n else p

    def peer(axis, d):
        return {AXIS[axis]: at(axis, d)}

    def cols(dz, half=None):
        begin = at("z", dz) * 512
        if half is None:
            return pl.ds(pl.multiple_of(begin, 512), 512)
        return pl.ds(pl.multiple_of(begin + 256 * half, 256), 256)

    def view(token):
        colour, phase, half = token[0], token[1], token[-1]
        ms = slice(0, 2) if half is None else half
        if colour in ("A", "B"):
            k = 0 if colour == "A" else 1
            last, first = ("x", "y") if colour == "A" else ("y", "x")
            dz = token[2]
            if phase == "z":
                return G.at[k, ms, at(last, 0), at(first, 0), :, cols(dz)]
            if phase == "f":
                return G.at[k, ms, at(last, 0), at(first, token[3]), :, cols(dz)]
            if phase == "p":
                return G.at[k, ms, at(last, token[4]), at(first, token[3]), :, cols(dz)]
            return G.at[k, ms, at(last, token[3]), :, :, cols(dz)]
        d = token[2]
        if colour == "C":
            return G.at[2, ms, x, y, :, cols(d)]
        if phase in ("f", "y"):
            cs = cols(0 if phase == "f" else token[3], half)
            if colour == "C0":
                return G.at[2, 0, at("x", d), y, :, cs]
            return G.at[2, 1, x, at("y", d), :, cs]
        cs = cols(0 if phase == "l" else token[3], half)
        if colour == "C0":
            return G.at[2, 0, :, at("y", d), :, cs]
        return G.at[2, 1, at("x", d), :, :, cs]

    arrival_at = {}
    for cp in copies:
        arrival_at.setdefault(cp["arrival"], [len(arrival_at), 0])[1] += cp["size"]
    amounts = {
        32 * KB: G.at[0, :, 0, 0, :, pl.ds(0, 512)],
        64 * KB: G.at[0, 0, 0, :, :, pl.ds(0, 512)],
        128 * KB: G.at[0, :, 0, :, :, pl.ds(0, 512)],
        256 * KB: G.at[0:2, :, 0, :, :, pl.ds(0, 512)],
    }

    def wait(ref, sem):
        pltpu.make_async_copy(ref, ref, sem).wait()

    def send(i):
        cp = copies[i]
        ref = view(cp["source"])
        pltpu.make_async_remote_copy(
            src_ref=ref, dst_ref=ref,
            send_sem=g_send.at[SEND_CLASS[cp["source"][:2]]], recv_sem=g_recv.at[arrival_at[cp["arrival"]][0]],
            device_id=peer(cp["axis"], cp["sign"]), device_id_type=MESH,
        ).start()

    def receive(arrival):
        index, size = arrival_at[arrival]
        wait(amounts[size], g_recv.at[index])

    for m, src in enumerate((ph, rh)):
        for k in range(3):
            dst = G.at[k, m, y, x, :, cols(0)] if k == 1 else G.at[k, m, x, y, :, cols(0)]
            pltpu.make_async_copy(src.at[pl.ds(16 * k, 16), :], dst, own_sem).start()
    small = ((tg, tgv), (dm, dmv), (kp, kpv), (pr, prv))
    for k, (src, dst) in enumerate(small):
        pltpu.make_async_copy(src, dst, small_sem.at[k]).start()
    heads = (pw, rw)
    for m in (0, 1):
        pltpu.make_async_copy(heads[m], W.at[m, 0], head_sem).start()

    barrier = pltpu.get_barrier_semaphore()
    peers = [peer("z", d) for d in range(1, 8)] + [peer(a, d) for a in "xy" for d in (1, 2, 3)]
    peers.append({"dp_2": other})
    for target in peers:
        pl.semaphore_signal(barrier, inc=1, device_id=target, device_id_type=MESH)
    st[...] = jnp.zeros_like(st)
    M0[y] = jnp.zeros((8, 128), jnp.float32)
    with jax.named_scope("entry_barrier"):
        pl.semaphore_wait(barrier, len(peers))
    with jax.named_scope("own_blocks"):
        wait(G.at[:, :, 0, 0, :, pl.ds(0, 512)], own_sem)

    def meta_send(axis, d):
        src, dst, k = (M0.at[y], M0.at[y], 0) if axis == "y" else (M0, M1.at[x], 1)
        pltpu.make_async_remote_copy(
            src_ref=src, dst_ref=dst, send_sem=m_send.at[k], recv_sem=m_recv.at[k],
            device_id=peer(axis, d), device_id_type=MESH,
        ).start()

    def swap(m, dz, q):
        pltpu.make_async_remote_copy(
            src_ref=heads[m].at[:, cols(dz)], dst_ref=W.at[m, 1, :, cols(dz)],
            send_sem=swap_send, recv_sem=swap_recv.at[q],
            device_id={"dp_2": other}, device_id_type=MESH,
        ).start()

    f32 = jnp.float32
    lane = lax.broadcasted_iota(jnp.int32, (8, 128), 1)
    sub = lax.broadcasted_iota(jnp.int32, (8, 128), 0)
    accs = {0: acc0, 1: acc1, 2: acc2, "C": accC}

    def block(group, m, dz):
        cs = cols(dz)
        if group == "C":
            return G[2, m, :, :, :, cs].reshape(256, 512)
        pieces = []
        for d in {0: (0,), 1: (-1, 1), 2: (2,)}[group]:
            pieces.append(G[0, m, at("x", d), :, :, cs].reshape(64, 512))
            pieces.append(G[1, m, at("y", d), :, :, cs].reshape(64, 512))
        return jnp.concatenate(pieces, axis=0)

    done_heads = set()

    def compute(i):
        group, dzs = WORK[i]
        if not done_heads:
            wait(W.at[:, 0], head_sem)
        for dz in dzs:
            if dz not in done_heads:
                wait(W.at[:, 1, :, cols(dz)], swap_recv.at[RING8.index(dz)])
                done_heads.add(dz)
        acc = accs[group]
        first = 0 in dzs

        for m in (0, 1):
            rhs = [block(group, m, dz) for dz in dzs]
            for h in (0, 1):
                total = None
                for dz, r in zip(dzs, rhs):
                    part = lax.dot_general(
                        W[m, h, :, cols(dz)], r, (((1,), (1,)), ((), ())), preferred_element_type=f32
                    )
                    total = part if total is None else total + part
                acc[m, h] = total if first else acc[m, h] + total

    dev = ((x * 4 + y) * 2 + c) * 8 + z
    dev_other = ((x * 4 + y) * 2 + other) * 8 + z
    offsets = (dev * rows, dev_other * rows)

    def spread(quantity):
        j = lax.broadcasted_iota(jnp.int32, (128, 128), 0)
        l = lax.broadcasted_iota(jnp.int32, (128, 128), 1)
        low = l % 16
        sel_ab = (j == low + jnp.where(l < 64, 0, 16)).astype(f32)
        sel_c = (j == low + 32).astype(f32)
        ab = jnp.dot(quantity, sel_ab, precision=lax.Precision.HIGHEST, preferred_element_type=f32)
        cc = jnp.dot(quantity, sel_c, precision=lax.Precision.HIGHEST, preferred_element_type=f32)
        d = lax.broadcasted_iota(jnp.int32, (16, 128), 0)
        l = lax.broadcasted_iota(jnp.int32, (16, 128), 1)
        q = (l // 16) % 4
        result = jnp.zeros((8, 128), f32)
        for a in range(4):
            owner = jnp.where(l < 64, a * 4 + q, q * 4 + a)
            row = jnp.sum(jnp.where(d == owner, ab, 0.0), axis=0, keepdims=True)
            result = jnp.where(sub == a, row, result)
        for a in range(2):
            owner = (2 * a + l // 64) * 4 + q
            row = jnp.sum(jnp.where(d == owner, cc, 0.0), axis=0, keepdims=True)
            result = jnp.where(sub == 4 + a, row, result)
        return result

    def stats(group, wanted):
        acc = accs[group]
        width = acc.shape[-1]
        if group == "C":
            places = [sub == 4, sub == 5]
        else:
            places = [
                sub == jnp.where(lane < 64, at("x", d), at("y", d))
                for d in {0: (0,), 1: (-1, 1), 2: (2,)}[group]
            ]
        want = [jnp.sum(jnp.where(p, wanted, 0.0), axis=0, keepdims=True) for p in places]
        want = jnp.concatenate(want, axis=1).astype(jnp.int32) if len(want) > 1 else want[0].astype(jnp.int32)
        vocab = lax.broadcasted_iota(jnp.int32, (rows, width), 0)
        lses, hits = [], []
        for m in (0, 1):
            peak = jnp.maximum(
                jnp.max(acc[m, 0], axis=0, keepdims=True), jnp.max(acc[m, 1], axis=0, keepdims=True)
            )
            total = jnp.zeros((1, width), f32)
            hit = jnp.zeros((1, width), f32)
            for h in (0, 1):
                logits = acc[m, h]
                total += jnp.sum(jnp.exp(logits - peak), axis=0, keepdims=True)
                match = vocab == want - offsets[h]
                hit += jnp.sum(jnp.where(match, logits, 0.0), axis=0, keepdims=True)
            lses.append(peak + jnp.log(total))
            hits.append(hit)
        for k, row in enumerate((lses[0], lses[1], hits[0] - hits[1])):
            value = st[k]
            for b, place in enumerate(places):
                value = jnp.where(place, row[:, 128 * b : 128 * (b + 1)], value)
            st[k] = value

    tables = {}
    pending = {g: sum(1 for w in WORK if w[0] == g) for g in accs}
    steps = 0
    for kind, i in order:
        if kind == "send":
            send(i)
        elif kind == "recv":
            if not steps:
                with jax.named_scope("small_inputs"):
                    for k, (src, dst) in enumerate(small):
                        pltpu.make_async_copy(src, dst, small_sem.at[k]).wait()
                for k, ref in enumerate((tgv, dmv, kpv)):
                    M0[y, k : k + 1, 0:tokens] = ref[...].astype(f32)
                for q, dz in enumerate(RING8):
                    for m in (0, 1):
                        swap(m, dz, q)
                for d in (1, 2, 3):
                    meta_send("y", d)
            steps += 1
            with jax.named_scope("recv"):
                receive(i)
        else:
            if not done_heads:
                wait(M0.at[pl.ds(0, 3)], m_recv.at[0])
                M1[x] = M0[...]
                for d in (1, 2, 3):
                    meta_send("x", d)
            with jax.named_scope(f"compute_{i}"):
                compute(i)
            group = WORK[i][0]
            pending[group] -= 1
            if not pending[group]:
                if not tables:
                    wait(M1.at[pl.ds(0, 3)], m_recv.at[1])
                    for k, name in enumerate(("targets", "domains", "keep")):
                        tables[name] = spread(M1[:, :, k, :].reshape(16, 128))
                with jax.named_scope(f"stats_{group}"):
                    stats(group, tables["targets"])

    def exchange(buf, axis, stage):
        n, mine = pos[axis][1], pos[axis][0]
        for d in (4, 3, 5, 2, 6, 1, 7) if n == 8 else (2, 1, 3):
            pltpu.make_async_remote_copy(
                src_ref=buf.at[mine], dst_ref=buf.at[mine],
                send_sem=s_send.at[stage], recv_sem=s_recv.at[stage],
                device_id=peer(axis, d), device_id_type=MESH,
            ).start()
        wait(buf.at[pl.ds(0, n - 1)], s_recv.at[stage])
        parts = [[buf[s, k] for k in range(3)] for s in range(n)]
        combined = []
        for k in (0, 1):
            peak = parts[0][k]
            for s in range(1, n):
                peak = jnp.maximum(peak, parts[s][k])
            total = jnp.exp(parts[0][k] - peak)
            for s in range(1, n):
                total = total + jnp.exp(parts[s][k] - peak)
            combined.append(peak + jnp.log(total))
        hit = parts[0][2]
        for s in range(1, n):
            hit = hit + parts[s][2]
        combined.append(hit)
        return combined

    zbuf[z] = st[...]
    with jax.named_scope("exchange_z"):
        result = exchange(zbuf, "z", 0)
    for k in range(3):
        ybuf[y, k] = result[k]
    with jax.named_scope("exchange_y"):
        result = exchange(ybuf, "y", 1)
    for k in range(3):
        xbuf[x, k] = result[k]
    with jax.named_scope("exchange_x"):
        lse0, lse1, hit = exchange(xbuf, "x", 2)

    keep = tables["keep"]
    gap = (lse0 - lse1) - hit
    excess = gap * keep
    clipped = jnp.maximum(gap, 0.0) * keep
    q = (lane // 16) % 4
    low = lane % 16
    owner = jnp.where(sub < 4, jnp.where(lane < 64, sub * 4 + q, q * 4 + sub), (2 * (sub - 4) + lane // 64) * 4 + q)
    colour = jnp.where(sub < 4, jnp.where(lane < 64, 0, 1), 2)
    token = (owner * 2 + c) * 48 + 16 * colour + low
    batch = token // 512
    label = lax.broadcasted_iota(jnp.int32, (128, 128), 0).astype(f32)
    left, right = [], []
    for b in range(6):
        bb = batch[b : b + 1, :]
        top = jnp.where(bb == sub, clipped[b : b + 1, :], 0.0)
        low_rows = jnp.where(bb == sub - 3, keep[b : b + 1, :], 0.0)
        left.append(jnp.where(sub < 3, top, low_rows))
        right.append((tables["domains"][b : b + 1, :] == label).astype(f32))
    sums = lax.dot_general(
        jnp.concatenate(left, axis=1), jnp.concatenate(right, axis=1), (((1,), (1,)), ((), ())),
        precision=lax.Precision.HIGHEST, preferred_element_type=f32,
    )
    dbuf[c] = sums

    def last_copy(slot):
        return pltpu.make_async_remote_copy(
            src_ref=dbuf.at[slot], dst_ref=dbuf.at[slot], send_sem=s_send.at[3], recv_sem=s_recv.at[3],
            device_id={"dp_2": other}, device_id_type=MESH,
        )

    last_copy(c).start()
    me = x * 4 + y
    here = jnp.where((owner == me) & (sub < 6), excess, 0.0)
    j = lax.broadcasted_iota(jnp.int32, (128, 128), 0)
    l = lax.broadcasted_iota(jnp.int32, (128, 128), 1)
    sel_ab = (j == l % 16 + jnp.where(l < 64, 0, 16)).astype(f32)
    sel_c = (j == l % 16 + 32).astype(f32)
    spots = jnp.concatenate([jnp.where(sub < 4, here, 0.0), jnp.where(sub >= 4, here, 0.0)], axis=1)
    mine_out = lax.dot_general(
        spots, jnp.concatenate([sel_ab, sel_c], axis=1), (((1,), (1,)), ((), ())),
        precision=lax.Precision.HIGHEST, preferred_element_type=f32,
    )
    mine_row = jnp.sum(mine_out, axis=0, keepdims=True)
    prior = prv[...]
    weights = prior / jnp.sum(prior, axis=1, keepdims=True)
    with jax.named_scope("partner_sums"):
        last_copy(other).wait_recv()
    both = dbuf[0] + dbuf[1]
    for s in range(STEPS):
        gain = both[s : s + 1, :] / jnp.maximum(both[3 + s : 4 + s, :], 1.0)
        raised = weights * jnp.exp(step_size * gain)
        weights = (1.0 - smoothing) * raised / jnp.sum(raised, axis=1, keepdims=True) + smoothing / DOMAINS
    out_weights[...] = jnp.log(weights)
    out_excess[...] = mine_row[:, 0:tokens]

    with jax.named_scope("sends_done"):
        for k in range(2):
            wait(G.at[k, :, 0, 0, :, pl.ds(0, 7 * 512)], g_send.at[3 * k])
            wait(G.at[k, :, 0, pl.ds(0, 3)], g_send.at[3 * k + 1])
            wait(G.at[k, :, pl.ds(0, 3)], g_send.at[3 * k + 2])
        wait(G.at[2, :, :, :, :, pl.ds(0, 7 * 512)], g_send.at[6])
        wait(G.at[2, :, pl.ds(0, 3), 0, :, pl.ds(0, 512)], g_send.at[7])
        wait(G.at[2, :, pl.ds(0, 3), :, :, pl.ds(0, 512)], g_send.at[8])
        wait(W.at[:, 1], swap_send)
        wait(M0.at[pl.ds(0, 3)], m_send.at[0])
        wait(M1.at[pl.ds(0, 3)], m_send.at[1])
        wait(zbuf.at[pl.ds(0, 7)], s_send.at[0])
        wait(ybuf.at[pl.ds(0, 3)], s_send.at[1])
        wait(xbuf.at[pl.ds(0, 3)], s_send.at[2])
        last_copy(c).wait_send()


def local(ph, rh, pw, rw, targets, domains, keep_mask, prior):
    rows, tokens = pw.shape[0], targets.shape[0]
    copies = gather_plan()
    order = schedule(copies, WORK)
    arrivals = len({c["arrival"] for c in copies})
    f32, bf16 = jnp.float32, jnp.bfloat16
    dma = pltpu.SemaphoreType.DMA
    anywhere = pl.BlockSpec(memory_space=pltpu.HBM)
    inside = pl.BlockSpec(memory_space=pltpu.VMEM)

    def body(*refs):
        kernel(copies, order, rows, tokens, *refs)

    out = pl.pallas_call(
        body,
        name="doremi",
        out_shape=[jax.ShapeDtypeStruct((1, tokens), f32), jax.ShapeDtypeStruct((1, 128), f32)],
        in_specs=[anywhere] * 8,
        out_specs=[inside] * 2,
        scratch_shapes=[
            pltpu.VMEM((3, 2, 4, 4, 16, 4096), bf16),
            pltpu.VMEM((2, 2, rows, 4096), bf16),
            pltpu.VMEM((2, 2, rows, 128), f32),
            pltpu.VMEM((2, 2, rows, 256), f32),
            pltpu.VMEM((2, 2, rows, 128), f32),
            pltpu.VMEM((2, 2, rows, 256), f32),
            pltpu.VMEM((1, tokens), jnp.int32),
            pltpu.VMEM((1, tokens), jnp.int32),
            pltpu.VMEM((1, tokens), jnp.int32),
            pltpu.VMEM((1, 128), f32),
            pltpu.VMEM((4, 8, 128), f32),
            pltpu.VMEM((4, 4, 8, 128), f32),
            pltpu.VMEM((3, 8, 128), f32),
            pltpu.VMEM((8, 3, 8, 128), f32),
            pltpu.VMEM((4, 3, 8, 128), f32),
            pltpu.VMEM((4, 3, 8, 128), f32),
            pltpu.VMEM((2, 8, 128), f32),
            dma, dma((4,)), dma, dma, dma((8,)),
            dma((9,)), dma((arrivals,)),
            dma((2,)), dma((2,)), dma((4,)), dma((4,)),
        ],
        compiler_params=pltpu.CompilerParams(
            collective_id=0, has_side_effects=True, vmem_limit_bytes=53 * 1024 * 1024
        ),
        cost_estimate=pl.CostEstimate(flops=12_900_000_000, bytes_accessed=34_000_000, transcendentals=2_000_000),
    )(*(
        pltpu.with_memory_space_constraint(a, pltpu.HBM)
        for a in (ph, rh, pw, rw, targets[None], domains[None], keep_mask[None], prior[None])
    ))
    return out[0][0], out[1][0]


def solution(mesh):
    split = Mesh(
        mesh.devices.reshape(4, 4, 2, mesh.shape["tensor"]), ("dp_0", "dp_1", "dp_2", "tensor")
    )
    return jax.shard_map(
        local,
        mesh=split,
        in_specs=(
            P(DP, "tensor"),
            P(DP, "tensor"),
            P(DP_TENSOR, None),
            P(DP_TENSOR, None),
            P(DP),
            P(DP),
            P(DP),
            P(),
        ),
        out_specs=(P(DP), P()),
        check_vma=False,
    )
```

```python
import jax
import jax.numpy as jnp
from jax import lax
from jax.experimental import pallas as pl
from jax.experimental.pallas import tpu as pltpu
from jax.sharding import Mesh
from jax.sharding import PartitionSpec as P

DOMAINS = 128
STEPS = 3
DP = ("dp_0", "dp_1", "dp_2")
DP_TENSOR = ("dp_0", "dp_1", "dp_2", "tensor")
AXIS = {"x": "dp_0", "y": "dp_1", "z": "tensor"}
MESH = pl.DeviceIdType.MESH

step_size = 1.0
smoothing = 0.001

KB = 1024
RATE = 46.6e3
HOP = 3.5
BACKLOG = 1.5
LAG = 0.6
FINE = (0, 1, -1)
RING4 = (0, 1, -1, 2)
RING8 = (0, 1, -1, 2, -2, 3, -3, 4)
PLANE = [(dx, dy) for dx in (2, 1, 3, 0) for dy in (2, 1, 3, 0) if dx or dy]
PLANE.sort(key=lambda p: -min(p[0], 4 - p[0]) - min(p[1], 4 - p[1]))


def ring(add, axis, size, token, need, far, rank, arrival, lag=0.01):
    for k in range(1, far + 1):
        halves = (0, 1) if k == far else (None, None)
        for sign, half in ((1, halves[0]), (-1, halves[1])):
            offset = far if k == far else -sign * k
            add(
                dict(
                    axis=axis,
                    sign=sign,
                    size=size // 2 if k == far else size,
                    source=token(-sign * (k - 1), half),
                    need=need if k == 1 else [token(-sign * (k - 1), None)],
                    given=token(offset, half),
                    rank=rank + lag * (k - 1),
                    arrival=arrival + (offset,),
                )
            )


def gather_plan():
    copies = []
    add = copies.append
    piece = 32 * KB
    for colour, first, last in (("A", "y", "x"), ("B", "x", "y")):
        own = [(colour, "z", 0, None)]
        ring(add, "z", piece, lambda d, h: (colour, "z", d, h), own, 4, 0, ("AB", "z"))
        for q, dz in enumerate(RING8):
            have = [(colour, "z", dz, None)]
            ring(add, first, piece, lambda d, h: (colour, "f", dz, d, h), have, 2, 1, ("AB", "f", dz))
            rank = 3 + 0.1 * q
            if dz in FINE:
                for df in RING4:
                    need = have if df == 0 else [(colour, "f", dz, df, None)]
                    token = lambda d, h: (colour, "p", dz, df, d, h)
                    ring(add, last, piece, token, need, 2, rank, ("AB", "p", dz, abs(df)), LAG)
            else:
                need = have + [(colour, "f", dz, d, None) for d in (1, -1, 2)]
                token = lambda d, h: (colour, "l", dz, d, h)
                ring(add, last, 4 * piece, token, need, 2, rank, ("AB", "l", dz), LAG)
    piece = 16 * KB
    own = [("C", "o", 0, None)]
    ring(add, "z", 2 * piece, lambda d, h: ("C", "o", d, h), own, 4, 2, ("C", "o"))
    for colour, first, last in (("C0", "x", "y"), ("C1", "y", "x")):
        ring(add, first, piece, lambda d, h: (colour, "f", d, h), own, 2, 0, ("C", "f"))
        need = own + [(colour, "f", d, None) for d in (1, -1, 2)]
        ring(add, last, 4 * piece, lambda d, h: (colour, "l", d, h), need, 2, 0, ("C", "l"))
        for j in (1, -1, 2):
            need = [(colour, "f", j, None)]
            ring(add, "z", piece, lambda d, h: (colour, "y", j, d, h), need, 4, 2, ("C", "y", j))
        for j in (1, -1, 2):
            need = [(colour, "l", j, None)]
            ring(add, "z", 4 * piece, lambda d, h: (colour, "z", j, d, h), need, 4, 2, ("C", "z", j))
    return copies


OWN = {("A", "z", 0, None), ("B", "z", 0, None), ("C", "o", 0, None)}


def tokens_of(group, dzs):
    out = []
    for dz in dzs:
        if group == "C":
            if dz:
                out.append(("C", "o", dz, None))
            for colour in ("C0", "C1"):
                for j in (1, -1, 2):
                    if dz:
                        out += [(colour, "y", j, dz, None), (colour, "z", j, dz, None)]
                    else:
                        out += [(colour, "f", j, None), (colour, "l", j, None)]
            continue
        for colour in ("A", "B"):
            if group == 0:
                out += [(colour, "z", dz, None)] + [(colour, "f", dz, d, None) for d in (1, -1, 2)]
                continue
            for d in (1, -1) if group == 1 else (2,):
                if dz in FINE:
                    out += [(colour, "p", dz, df, d, None) for df in RING4]
                else:
                    out.append((colour, "l", dz, d, None))
    return out


WORK = [
    (0, (0,)), (0, (1, -1)), (0, (2, -2)), (0, (3, -3, 4)),
    (1, (0,)), (1, (1, -1)), (1, (2, -2)), (1, (3, -3)), (1, (4,)),
    (2, (0,)), (2, (1, -1)), (2, (2, -2)), (2, (3, -3)), (2, (4,)),
    ("C", (0,)), ("C", (1, -1)), ("C", (2, -2)), ("C", (3, -3)), ("C", (4,)),
]
STATS_TIME = {0: 0.34, 1: 0.74, 2: 0.34, "C": 0.74}


def schedule(copies, works):
    arrival_of = {c["given"]: c["arrival"] for c in copies}
    members = {}
    for i, c in enumerate(copies):
        members.setdefault(c["arrival"], []).append(i)

    def arrivals(tokens):
        found = set()
        for t in tokens:
            if t not in OWN:
                found |= {arrival_of[p] for p in (t, t[:-1] + (0,), t[:-1] + (1,)) if p in arrival_of}
        return found

    deps = [arrivals(c["need"]) for c in copies]
    needs = [arrivals(tokens_of(*w)) for w in works]
    links = {}
    for i, c in enumerate(copies):
        links.setdefault((c["axis"], c["sign"]), []).append(i)
    got, free, landed = set(), dict.fromkeys(links, 0.0), {}
    unsent, undone = set(range(len(copies))), set(range(len(works)))
    left = {g: sum(1 for w in works if w[0] == g) for g in STATS_TIME}
    now, order = 0.0, []
    while unsent or undone or len(got) < len(members):
        coming = {
            a: max(landed[i] for i in m)
            for a, m in members.items()
            if a not in got and all(i in landed for i in m)
        }
        here = sorted((when, str(a), a) for a, when in coming.items() if when <= now + 1e-9)
        if here:
            for _, _, a in here:
                got.add(a)
                order.append(("recv", a))
                now += 0.02
            continue
        sent = False
        for link, all_of in links.items():
            while free[link] - now < BACKLOG:
                ready = [i for i in all_of if i in unsent and deps[i] <= got]
                if not ready:
                    break
                i = min(ready, key=lambda i: (copies[i]["rank"], i))
                free[link] = max(now, free[link]) + copies[i]["size"] / RATE
                landed[i] = free[link] + HOP
                unsent.discard(i)
                order.append(("send", i))
                now += 0.012
                sent = True
        if sent:
            continue
        ready = [i for i in undone if needs[i] <= got]
        if ready:
            i = min(ready)
            undone.discard(i)
            order.append(("compute", i))
            now += 0.25 + 0.54 * len(works[i][1])
            left[works[i][0]] -= 1
            if not left[works[i][0]]:
                now += STATS_TIME[works[i][0]]
            continue
        times = list(coming.values())
        for link, all_of in links.items():
            if any(i in unsent and deps[i] <= got for i in all_of):
                times.append(free[link] - BACKLOG + 1e-6)
        now = max(now, min(times))
    return order


SEND_CLASS = {
    ("A", "z"): 0, ("A", "f"): 1, ("A", "p"): 2, ("A", "l"): 2,
    ("B", "z"): 3, ("B", "f"): 4, ("B", "p"): 5, ("B", "l"): 5,
    ("C", "o"): 6, ("C0", "y"): 6, ("C1", "y"): 6, ("C0", "z"): 6, ("C1", "z"): 6,
    ("C0", "f"): 7, ("C1", "f"): 7, ("C0", "l"): 8, ("C1", "l"): 8,
}


def kernel(
    copies, order, rows, tokens,
    ph, rh, pw, rw, tg, dm, kp, pr, out_excess, out_weights,
    G, W, acc0, acc1, acc2, accC, tgv, dmv, kpv, prv, M0, M1, onehot, early, late, zearly, zlate, pearly, plate, dbuf,
    own_sem, small_sem, head_sem, swap_send, swap_recv, g_send, g_recv, m_send, m_recv, s_send, s_recv,
):
    x, y, c, z = (lax.axis_index(a) for a in ("dp_0", "dp_1", "dp_2", "tensor"))
    other = 1 - c
    pos = {"x": (x, 4), "y": (y, 4), "z": (z, 8)}

    def at(axis, d):
        p, n = pos[axis]
        return lax.rem(p + (d % n), n) if d % n else p

    def peer(axis, d):
        return {AXIS[axis]: at(axis, d)}

    def cols(dz, half=None):
        begin = at("z", dz) * 512
        if half is None:
            return pl.ds(pl.multiple_of(begin, 512), 512)
        return pl.ds(pl.multiple_of(begin + 256 * half, 256), 256)

    def view(token):
        colour, phase, half = token[0], token[1], token[-1]
        ms = slice(0, 2) if half is None else half
        if colour in ("A", "B"):
            k = 0 if colour == "A" else 1
            last, first = ("x", "y") if colour == "A" else ("y", "x")
            dz = token[2]
            if phase == "z":
                return G.at[k, ms, at(last, 0), at(first, 0), :, cols(dz)]
            if phase == "f":
                return G.at[k, ms, at(last, 0), at(first, token[3]), :, cols(dz)]
            if phase == "p":
                return G.at[k, ms, at(last, token[4]), at(first, token[3]), :, cols(dz)]
            return G.at[k, ms, at(last, token[3]), :, :, cols(dz)]
        d = token[2]
        if colour == "C":
            return G.at[2, ms, x, y, :, cols(d)]
        if phase in ("f", "y"):
            cs = cols(0 if phase == "f" else token[3], half)
            if colour == "C0":
                return G.at[2, 0, at("x", d), y, :, cs]
            return G.at[2, 1, x, at("y", d), :, cs]
        cs = cols(0 if phase == "l" else token[3], half)
        if colour == "C0":
            return G.at[2, 0, :, at("y", d), :, cs]
        return G.at[2, 1, at("x", d), :, :, cs]

    arrival_at = {}
    for cp in copies:
        arrival_at.setdefault(cp["arrival"], [len(arrival_at), 0])[1] += cp["size"]
    amounts = {
        32 * KB: G.at[0, :, 0, 0, :, pl.ds(0, 512)],
        64 * KB: G.at[0, 0, 0, :, :, pl.ds(0, 512)],
        128 * KB: G.at[0, :, 0, :, :, pl.ds(0, 512)],
        256 * KB: G.at[0:2, :, 0, :, :, pl.ds(0, 512)],
    }

    def wait(ref, sem):
        pltpu.make_async_copy(ref, ref, sem).wait()

    def send(i):
        cp = copies[i]
        ref = view(cp["source"])
        pltpu.make_async_remote_copy(
            src_ref=ref, dst_ref=ref,
            send_sem=g_send.at[SEND_CLASS[cp["source"][:2]]], recv_sem=g_recv.at[arrival_at[cp["arrival"]][0]],
            device_id=peer(cp["axis"], cp["sign"]), device_id_type=MESH,
        ).start()

    def receive(arrival):
        index, size = arrival_at[arrival]
        wait(amounts[size], g_recv.at[index])

    for m, src in enumerate((ph, rh)):
        for k in range(3):
            dst = G.at[k, m, y, x, :, cols(0)] if k == 1 else G.at[k, m, x, y, :, cols(0)]
            pltpu.make_async_copy(src.at[pl.ds(16 * k, 16), :], dst, own_sem).start()
    small = ((tg, tgv), (dm, dmv), (kp, kpv), (pr, prv))
    for k, (src, dst) in enumerate(small):
        pltpu.make_async_copy(src, dst, small_sem.at[k]).start()
    heads = (pw, rw)
    for m in (0, 1):
        pltpu.make_async_copy(heads[m], W.at[m, 0], head_sem).start()

    barrier = pltpu.get_barrier_semaphore()
    peers = [peer(a, d) for a in "xyz" for d in (1, -1)] + [{"dp_2": other}]
    for target in peers:
        pl.semaphore_signal(barrier, inc=1, device_id=target, device_id_type=MESH)
    early[...] = jnp.zeros_like(early)
    late[...] = jnp.zeros_like(late)
    M0[y] = jnp.zeros((8, 128), jnp.float32)
    with jax.named_scope("entry_barrier"):
        pl.semaphore_wait(barrier, len(peers))
    with jax.named_scope("own_blocks"):
        wait(G.at[:, :, 0, 0, :, pl.ds(0, 512)], own_sem)

    def meta_send(axis, d):
        src, dst, k = (M0.at[y], M0.at[y], 0) if axis == "y" else (M0, M1.at[x], 1)
        pltpu.make_async_remote_copy(
            src_ref=src, dst_ref=dst, send_sem=m_send.at[k], recv_sem=m_recv.at[k],
            device_id=peer(axis, d), device_id_type=MESH,
        ).start()

    def swap(m, dz, q):
        pltpu.make_async_remote_copy(
            src_ref=heads[m].at[:, cols(dz)], dst_ref=W.at[m, 1, :, cols(dz)],
            send_sem=swap_send, recv_sem=swap_recv.at[q],
            device_id={"dp_2": other}, device_id_type=MESH,
        ).start()

    f32 = jnp.float32
    lane = lax.broadcasted_iota(jnp.int32, (8, 128), 1)
    sub = lax.broadcasted_iota(jnp.int32, (8, 128), 0)
    accs = {0: acc0, 1: acc1, 2: acc2, "C": accC}

    def block(group, m, dz):
        cs = cols(dz)
        if group == "C":
            return G[2, m, :, :, :, cs].reshape(256, 512)
        pieces = []
        for d in {0: (0,), 1: (-1, 1), 2: (2,)}[group]:
            pieces.append(G[0, m, at("x", d), :, :, cs].reshape(64, 512))
            pieces.append(G[1, m, at("y", d), :, :, cs].reshape(64, 512))
        return jnp.concatenate(pieces, axis=0)

    done_heads = set()

    def compute(i):
        group, dzs = WORK[i]
        if not done_heads:
            wait(W.at[:, 0], head_sem)
        for dz in dzs:
            if dz not in done_heads:
                wait(W.at[:, 1, :, cols(dz)], swap_recv.at[RING8.index(dz)])
                done_heads.add(dz)
        acc = accs[group]
        first = 0 in dzs

        for m in (0, 1):
            rhs = [block(group, m, dz) for dz in dzs]
            for h in (0, 1):
                total = None
                for dz, r in zip(dzs, rhs):
                    part = lax.dot_general(
                        W[m, h, :, cols(dz)], r, (((1,), (1,)), ((), ())), preferred_element_type=f32
                    )
                    total = part if total is None else total + part
                acc[m, h] = total if first else acc[m, h] + total

    dev = ((x * 4 + y) * 2 + c) * 8 + z
    dev_other = ((x * 4 + y) * 2 + other) * 8 + z
    offsets = (dev * rows, dev_other * rows)

    def spread(quantity):
        j = lax.broadcasted_iota(jnp.int32, (128, 128), 0)
        l = lax.broadcasted_iota(jnp.int32, (128, 128), 1)
        low = l % 16
        sel_ab = (j == low + jnp.where(l < 64, 0, 16)).astype(f32)
        sel_c = (j == low + 32).astype(f32)
        ab = jnp.dot(quantity, sel_ab, precision=lax.Precision.HIGHEST, preferred_element_type=f32)
        cc = jnp.dot(quantity, sel_c, precision=lax.Precision.HIGHEST, preferred_element_type=f32)
        d = lax.broadcasted_iota(jnp.int32, (16, 128), 0)
        l = lax.broadcasted_iota(jnp.int32, (16, 128), 1)
        q = (l // 16) % 4
        result = jnp.zeros((8, 128), f32)
        for a in range(4):
            owner = jnp.where(l < 64, a * 4 + q, q * 4 + a)
            row = jnp.sum(jnp.where(d == owner, ab, 0.0), axis=0, keepdims=True)
            result = jnp.where(sub == a, row, result)
        for a in range(2):
            owner = (2 * a + l // 64) * 4 + q
            row = jnp.sum(jnp.where(d == owner, cc, 0.0), axis=0, keepdims=True)
            result = jnp.where(sub == 4 + a, row, result)
        return result

    def stats(group, wanted):
        acc = accs[group]
        width = acc.shape[-1]
        if group == "C":
            spots = [jnp.full((8, 128), b, jnp.int32) for b in range(2)]
            want = [wanted[4 + b : 5 + b, :] for b in range(2)]
        else:
            spots = [
                jnp.where(lane < 64, at("x", d), at("y", d)) for d in {0: (0,), 1: (-1, 1), 2: (2,)}[group]
            ]
            want = [jnp.sum(jnp.where(sub == p, wanted, 0.0), axis=0, keepdims=True) for p in spots]
        want = jnp.concatenate(want, axis=1).astype(jnp.int32) if len(want) > 1 else want[0].astype(jnp.int32)
        vocab = lax.broadcasted_iota(jnp.int32, (rows, width), 0)
        lses, hits = [], []
        for m in (0, 1):
            peak = jnp.maximum(
                jnp.max(acc[m, 0], axis=0, keepdims=True), jnp.max(acc[m, 1], axis=0, keepdims=True)
            )
            total = jnp.zeros((1, width), f32)
            hit = jnp.zeros((1, width), f32)
            for h in (0, 1):
                logits = acc[m, h]
                total += jnp.sum(jnp.exp(logits - peak), axis=0, keepdims=True)
                match = vocab == want - offsets[h]
                hit += jnp.sum(jnp.where(match, logits, 0.0), axis=0, keepdims=True)
            lses.append(peak + jnp.log(total))
            hits.append(hit)
        for b, spot in enumerate(spots):
            one, two, hit = (r[:, 128 * b : 128 * (b + 1)] for r in (lses[0], lses[1], hits[0] - hits[1]))
            if group == "C":
                value = jnp.where(sub == spot, one, late[...])
                value = jnp.where(sub == spot + 2, two, value)
                late[...] = jnp.where(sub == spot + 4, hit, value)
            else:
                value = jnp.where(sub == spot, one, early[0])
                early[0] = jnp.where(sub == spot + 4, two, value)
                early[1] = jnp.where(sub == spot, hit, early[1])

    me = x * 4 + y
    label = lax.broadcasted_iota(jnp.int32, (128, 128), 0).astype(f32)

    def spread_z(buf, value, stage):
        buf[z] = value
        for d in (4, 3, 5, 2, 6, 1, 7):
            pltpu.make_async_remote_copy(
                src_ref=buf.at[z], dst_ref=buf.at[z], send_sem=s_send.at[stage], recv_sem=s_recv.at[stage],
                device_id=peer("z", d), device_id_type=MESH,
            ).start()

    def spread_xy(buf, value, stage):
        buf[me] = value
        for dx, dy in PLANE:
            pltpu.make_async_remote_copy(
                src_ref=buf.at[me], dst_ref=buf.at[me], send_sem=s_send.at[stage], recv_sem=s_recv.at[stage],
                device_id={**peer("x", dx), **peer("y", dy)}, device_id_type=MESH,
            ).start()

    def arrived(buf, stage):
        wait(buf.at[pl.ds(0, buf.shape[0] - 1)], s_recv.at[stage])

    def joined(parts):
        peak = parts[0]
        for p in parts[1:]:
            peak = jnp.maximum(peak, p)
        total = jnp.exp(parts[0] - peak)
        for p in parts[1:]:
            total = total + jnp.exp(p - peak)
        return peak + jnp.log(total)

    def added(parts):
        total = parts[0]
        for p in parts[1:]:
            total = total + p
        return total

    def join_early(buf):
        n = buf.shape[0]
        return jnp.stack([joined([buf[s, 0] for s in range(n)]), added([buf[s, 1] for s in range(n)])])

    def join_late(buf):
        parts = [buf[s] for s in range(buf.shape[0])]
        return jnp.where(sub < 4, joined(parts), added(parts))

    tables = {}
    pending = {g: sum(1 for w in WORK if w[0] == g) for g in accs}
    steps = computes = 0
    for kind, i in order:
        if kind == "send":
            send(i)
        elif kind == "recv":
            if not steps:
                with jax.named_scope("small_inputs"):
                    for k, (src, dst) in enumerate(small):
                        pltpu.make_async_copy(src, dst, small_sem.at[k]).wait()
                for k, ref in enumerate((tgv, dmv, kpv)):
                    M0[y, k : k + 1, 0:tokens] = ref[...].astype(f32)
                for q, dz in enumerate(RING8):
                    for m in (0, 1):
                        swap(m, dz, q)
            steps += 1
            with jax.named_scope("recv"):
                receive(i)
        else:
            if computes == 0:
                for d in (1, 2, 3):
                    meta_send("y", d)
            if computes == 3:
                wait(M0.at[pl.ds(0, 3)], m_recv.at[0])
                M1[x] = M0[...]
                for d in (1, 2, 3):
                    meta_send("x", d)
            computes += 1
            with jax.named_scope(f"compute_{i}"):
                compute(i)
            group = WORK[i][0]
            pending[group] -= 1
            if not pending[group]:
                if not tables:
                    wait(M1.at[pl.ds(0, 3)], m_recv.at[1])
                    for k, name in enumerate(("targets", "domains", "keep")):
                        tables[name] = spread(M1[:, :, k, :].reshape(16, 128))
                    onehot[...] = jnp.concatenate(
                        [(tables["domains"][b : b + 1, :] == label).astype(f32) for b in range(6)], axis=1
                    )
                with jax.named_scope(f"stats_{group}"):
                    stats(group, tables["targets"])
                if group == "C":
                    spread_z(zlate, late[...], 1)
                elif not any(pending[g] for g in (0, 1, 2)):
                    spread_z(zearly, early[...], 0)

    keep = tables["keep"]
    q = (lane // 16) % 4
    owner = jnp.where(sub < 4, jnp.where(lane < 64, sub * 4 + q, q * 4 + sub), (2 * (sub - 4) + lane // 64) * 4 + q)
    colour = jnp.where(sub < 4, jnp.where(lane < 64, 0, 1), 2)
    batch = ((owner * 2 + c) * 48 + 16 * colour + lane % 16) // 512

    def domain_sums(clipped, first, last):
        left = []
        for b in range(first, last):
            bb = batch[b : b + 1, :]
            top = jnp.where(bb == sub, clipped[b - first : b - first + 1, :], 0.0)
            low_rows = jnp.where(bb == sub - 3, keep[b : b + 1, :], 0.0)
            left.append(jnp.where(sub < 3, top, low_rows))
        return lax.dot_general(
            jnp.concatenate(left, axis=1), onehot[:, 128 * first : 128 * last], (((1,), (1,)), ((), ())),
            precision=lax.Precision.HIGHEST, preferred_element_type=f32,
        )

    with jax.named_scope("exchange_z"):
        arrived(zearly, 0)
        spread_xy(pearly, join_early(zearly), 2)
        with jax.named_scope("late_z"):
            arrived(zlate, 1)
        spread_xy(plate, join_late(zlate), 3)
    with jax.named_scope("exchange_xy"):
        arrived(pearly, 2)
        pair = join_early(pearly)
        gap_early = (pair[0, 0:4] - pair[0, 4:8]) - pair[1, 0:4]
        sums_early = domain_sums(jnp.maximum(gap_early, 0.0) * keep[0:4], 0, 4)
        with jax.named_scope("late_xy"):
            arrived(plate, 3)
    tile = join_late(plate)
    gap_late = (tile[0:2] - tile[2:4]) - tile[4:6]
    sums = sums_early + domain_sums(jnp.maximum(gap_late, 0.0) * keep[4:6], 4, 6)
    gap = jnp.concatenate([gap_early, gap_late, jnp.zeros((2, 128), f32)], axis=0)
    excess = gap * keep
    dbuf[c] = sums

    def last_copy(slot):
        return pltpu.make_async_remote_copy(
            src_ref=dbuf.at[slot], dst_ref=dbuf.at[slot], send_sem=s_send.at[4], recv_sem=s_recv.at[4],
            device_id={"dp_2": other}, device_id_type=MESH,
        )

    last_copy(c).start()
    here = jnp.where((owner == me) & (sub < 6), excess, 0.0)
    j = lax.broadcasted_iota(jnp.int32, (128, 128), 0)
    l = lax.broadcasted_iota(jnp.int32, (128, 128), 1)
    sel_ab = (j == l % 16 + jnp.where(l < 64, 0, 16)).astype(f32)
    sel_c = (j == l % 16 + 32).astype(f32)
    spots = jnp.concatenate([jnp.where(sub < 4, here, 0.0), jnp.where(sub >= 4, here, 0.0)], axis=1)
    mine_out = lax.dot_general(
        spots, jnp.concatenate([sel_ab, sel_c], axis=1), (((1,), (1,)), ((), ())),
        precision=lax.Precision.HIGHEST, preferred_element_type=f32,
    )
    mine_row = jnp.sum(mine_out, axis=0, keepdims=True)
    prior = prv[...]
    weights = prior / jnp.sum(prior, axis=1, keepdims=True)
    with jax.named_scope("partner_sums"):
        last_copy(other).wait_recv()
    both = dbuf[0] + dbuf[1]
    for s in range(STEPS):
        gain = both[s : s + 1, :] / jnp.maximum(both[3 + s : 4 + s, :], 1.0)
        raised = weights * jnp.exp(step_size * gain)
        weights = (1.0 - smoothing) * raised / jnp.sum(raised, axis=1, keepdims=True) + smoothing / DOMAINS
    out_weights[...] = jnp.log(weights)
    out_excess[...] = mine_row[:, 0:tokens]

    with jax.named_scope("sends_done"):
        for k in range(2):
            wait(G.at[k, :, 0, 0, :, pl.ds(0, 7 * 512)], g_send.at[3 * k])
            wait(G.at[k, :, 0, pl.ds(0, 3)], g_send.at[3 * k + 1])
            wait(G.at[k, :, pl.ds(0, 3)], g_send.at[3 * k + 2])
        wait(G.at[2, :, :, :, :, pl.ds(0, 7 * 512)], g_send.at[6])
        wait(G.at[2, :, pl.ds(0, 3), 0, :, pl.ds(0, 512)], g_send.at[7])
        wait(G.at[2, :, pl.ds(0, 3), :, :, pl.ds(0, 512)], g_send.at[8])
        wait(W.at[:, 1], swap_send)
        wait(M0.at[pl.ds(0, 3)], m_send.at[0])
        wait(M1.at[pl.ds(0, 3)], m_send.at[1])
        for k, buf in enumerate((zearly, zlate, pearly, plate)):
            wait(buf.at[pl.ds(0, buf.shape[0] - 1)], s_send.at[k])
        last_copy(c).wait_send()


def local(ph, rh, pw, rw, targets, domains, keep_mask, prior):
    rows, tokens = pw.shape[0], targets.shape[0]
    copies = gather_plan()
    order = schedule(copies, WORK)
    arrivals = len({c["arrival"] for c in copies})
    f32, bf16 = jnp.float32, jnp.bfloat16
    dma = pltpu.SemaphoreType.DMA
    anywhere = pl.BlockSpec(memory_space=pltpu.HBM)
    inside = pl.BlockSpec(memory_space=pltpu.VMEM)

    def body(*refs):
        kernel(copies, order, rows, tokens, *refs)

    out = pl.pallas_call(
        body,
        name="doremi",
        out_shape=[jax.ShapeDtypeStruct((1, tokens), f32), jax.ShapeDtypeStruct((1, 128), f32)],
        in_specs=[anywhere] * 8,
        out_specs=[inside] * 2,
        scratch_shapes=[
            pltpu.VMEM((3, 2, 4, 4, 16, 4096), bf16),
            pltpu.VMEM((2, 2, rows, 4096), bf16),
            pltpu.VMEM((2, 2, rows, 128), f32),
            pltpu.VMEM((2, 2, rows, 256), f32),
            pltpu.VMEM((2, 2, rows, 128), f32),
            pltpu.VMEM((2, 2, rows, 256), f32),
            pltpu.VMEM((1, tokens), jnp.int32),
            pltpu.VMEM((1, tokens), jnp.int32),
            pltpu.VMEM((1, tokens), jnp.int32),
            pltpu.VMEM((1, 128), f32),
            pltpu.VMEM((4, 8, 128), f32),
            pltpu.VMEM((4, 4, 8, 128), f32),
            pltpu.VMEM((128, 768), f32),
            pltpu.VMEM((2, 8, 128), f32),
            pltpu.VMEM((8, 128), f32),
            pltpu.VMEM((8, 2, 8, 128), f32),
            pltpu.VMEM((8, 8, 128), f32),
            pltpu.VMEM((16, 2, 8, 128), f32),
            pltpu.VMEM((16, 8, 128), f32),
            pltpu.VMEM((2, 8, 128), f32),
            dma, dma((4,)), dma, dma, dma((8,)),
            dma((9,)), dma((arrivals,)),
            dma((2,)), dma((2,)), dma((5,)), dma((5,)),
        ],
        compiler_params=pltpu.CompilerParams(
            collective_id=0, has_side_effects=True, vmem_limit_bytes=53 * 1024 * 1024
        ),
        cost_estimate=pl.CostEstimate(flops=12_900_000_000, bytes_accessed=34_000_000, transcendentals=2_000_000),
    )(*(
        pltpu.with_memory_space_constraint(a, pltpu.HBM)
        for a in (ph, rh, pw, rw, targets[None], domains[None], keep_mask[None], prior[None])
    ))
    return out[0][0], out[1][0]


def solution(mesh):
    split = Mesh(
        mesh.devices.reshape(4, 4, 2, mesh.shape["tensor"]), ("dp_0", "dp_1", "dp_2", "tensor")
    )
    return jax.shard_map(
        local,
        mesh=split,
        in_specs=(
            P(DP, "tensor"),
            P(DP, "tensor"),
            P(DP_TENSOR, None),
            P(DP_TENSOR, None),
            P(DP),
            P(DP),
            P(DP),
            P(),
        ),
        out_specs=(P(DP), P()),
        check_vma=False,
    )
```

```python
import jax
import jax.numpy as jnp
from jax import lax
from jax.experimental import pallas as pl
from jax.experimental.pallas import tpu as pltpu
from jax.sharding import Mesh
from jax.sharding import PartitionSpec as P

DOMAINS = 128
STEPS = 3
DP = ("dp_0", "dp_1", "dp_2")
DP_TENSOR = ("dp_0", "dp_1", "dp_2", "tensor")
AXIS = {"x": "dp_0", "y": "dp_1", "z": "tensor"}
MESH = pl.DeviceIdType.MESH
DMA = pltpu.SemaphoreType.DMA

step_size = 1.0
smoothing = 0.001

KB = 1024
RATE = 46.6e3
HOP = 3.5
BACKLOG = 1.5
LAG = 0.6
FINE = (0, 1, -1)
RING4 = (0, 1, -1, 2)
RING8 = (0, 1, -1, 2, -2, 3, -3, 4)
PLANE = [(dx, dy) for dx in (2, 1, 3, 0) for dy in (2, 1, 3, 0) if dx or dy]
PLANE.sort(key=lambda p: -min(p[0], 4 - p[0]) - min(p[1], 4 - p[1]))


def ring(add, axis, size, token, need, far, rank, arrival, lag=0.01):
    for k in range(1, far + 1):
        halves = (0, 1) if k == far else (None, None)
        for sign, half in ((1, halves[0]), (-1, halves[1])):
            offset = far if k == far else -sign * k
            add(
                dict(
                    axis=axis,
                    sign=sign,
                    size=size // 2 if k == far else size,
                    source=token(-sign * (k - 1), half),
                    need=need if k == 1 else [token(-sign * (k - 1), None)],
                    given=token(offset, half),
                    rank=rank + lag * (k - 1),
                    arrival=arrival + (offset,),
                )
            )


def gather_plan():
    copies = []
    add = copies.append
    piece = 32 * KB
    for colour, first, last in (("A", "y", "x"), ("B", "x", "y")):
        own = [(colour, "z", 0, None)]
        ring(add, "z", piece, lambda d, h: (colour, "z", d, h), own, 4, 0, ("AB", "z"))
        for q, dz in enumerate(RING8):
            have = [(colour, "z", dz, None)]
            ring(add, first, piece, lambda d, h: (colour, "f", dz, d, h), have, 2, 1, ("AB", "f", dz))
            rank = 3 + 0.1 * q
            if dz in FINE:
                for df in RING4:
                    need = have if df == 0 else [(colour, "f", dz, df, None)]
                    token = lambda d, h: (colour, "p", dz, df, d, h)
                    ring(add, last, piece, token, need, 2, rank, ("AB", "p", dz, abs(df)), LAG)
            else:
                need = have + [(colour, "f", dz, d, None) for d in (1, -1, 2)]
                token = lambda d, h: (colour, "l", dz, d, h)
                ring(add, last, 4 * piece, token, need, 2, rank, ("AB", "l", dz), LAG)
    piece = 16 * KB
    own = [("C", "o", 0, None)]
    ring(add, "z", 2 * piece, lambda d, h: ("C", "o", d, h), own, 4, 2, ("C", "o"))
    for colour, first, last in (("C0", "x", "y"), ("C1", "y", "x")):
        ring(add, first, piece, lambda d, h: (colour, "f", d, h), own, 2, 0, ("C", "f"))
        need = own + [(colour, "f", d, None) for d in (1, -1, 2)]
        ring(add, last, 4 * piece, lambda d, h: (colour, "l", d, h), need, 2, 0, ("C", "l"))
        for j in (1, -1, 2):
            need = [(colour, "f", j, None)]
            ring(add, "z", piece, lambda d, h: (colour, "y", j, d, h), need, 4, 2, ("C", "y", j))
        for j in (1, -1, 2):
            need = [(colour, "l", j, None)]
            ring(add, "z", 4 * piece, lambda d, h: (colour, "z", j, d, h), need, 4, 2, ("C", "z", j))
    return copies


OWN = {("A", "z", 0, None), ("B", "z", 0, None), ("C", "o", 0, None)}


def tokens_of(group, dzs):
    out = []
    for dz in dzs:
        if group == "C":
            if dz:
                out.append(("C", "o", dz, None))
            for colour in ("C0", "C1"):
                for j in (1, -1, 2):
                    if dz:
                        out += [(colour, "y", j, dz, None), (colour, "z", j, dz, None)]
                    else:
                        out += [(colour, "f", j, None), (colour, "l", j, None)]
            continue
        for colour in ("A", "B"):
            if group == 0:
                out += [(colour, "z", dz, None)] + [(colour, "f", dz, d, None) for d in (1, -1, 2)]
                continue
            for d in (1, -1) if group == 1 else (2,):
                if dz in FINE:
                    out += [(colour, "p", dz, df, d, None) for df in RING4]
                else:
                    out.append((colour, "l", dz, d, None))
    return out


WORK = [
    (0, (0,)), (0, (1, -1)), (0, (2, -2)), (0, (3, -3, 4)),
    (1, (0,)), (1, (1, -1)), (1, (2, -2)), (1, (3, -3)), (1, (4,)),
    (2, (0,)), (2, (1, -1)), (2, (2, -2)), (2, (3,)), (2, (-3,)), (2, (4,)),
    ("C", (0,)), ("C", (1, -1)), ("C", (2, -2)), ("C", (3, -3)), ("C", (4,)),
]
STATS_TIME = {0: 0.34, 1: 0.74, 2: 0.34, "C": 0.74}


def schedule(copies, works):
    arrival_of = {c["given"]: c["arrival"] for c in copies}
    members = {}
    for i, c in enumerate(copies):
        members.setdefault(c["arrival"], []).append(i)

    def arrivals(tokens):
        found = set()
        for t in tokens:
            if t not in OWN:
                found |= {arrival_of[p] for p in (t, t[:-1] + (0,), t[:-1] + (1,)) if p in arrival_of}
        return found

    deps = [arrivals(c["need"]) for c in copies]
    needs = [arrivals(tokens_of(*w)) for w in works]
    links = {}
    for i, c in enumerate(copies):
        links.setdefault((c["axis"], c["sign"]), []).append(i)
    got, free, landed = set(), dict.fromkeys(links, 0.0), {}
    unsent, undone = set(range(len(copies))), set(range(len(works)))
    left = {g: sum(1 for w in works if w[0] == g) for g in STATS_TIME}
    now, order = 0.0, []
    while unsent or undone or len(got) < len(members):
        coming = {
            a: max(landed[i] for i in m)
            for a, m in members.items()
            if a not in got and all(i in landed for i in m)
        }
        here = sorted((when, str(a), a) for a, when in coming.items() if when <= now + 1e-9)
        if here:
            for _, _, a in here:
                got.add(a)
                order.append(("recv", a))
                now += 0.02
            continue
        sent = False
        for link, all_of in links.items():
            while free[link] - now < BACKLOG:
                ready = [i for i in all_of if i in unsent and deps[i] <= got]
                if not ready:
                    break
                i = min(ready, key=lambda i: (copies[i]["rank"], i))
                free[link] = max(now, free[link]) + copies[i]["size"] / RATE
                landed[i] = free[link] + HOP
                unsent.discard(i)
                order.append(("send", i))
                now += 0.012
                sent = True
        if sent:
            continue
        ready = [i for i in undone if needs[i] <= got]
        if ready:
            i = min(ready)
            undone.discard(i)
            order.append(("compute", i))
            now += 0.2 + 0.54 * len(works[i][1])
            left[works[i][0]] -= 1
            if not left[works[i][0]]:
                now += STATS_TIME[works[i][0]]
            continue
        times = list(coming.values())
        for link, all_of in links.items():
            if any(i in unsent and deps[i] <= got for i in all_of):
                times.append(free[link] - BACKLOG + 1e-6)
        now = max(now, min(times))
    return order


SEND_CLASS = {
    ("A", "z"): 0, ("A", "f"): 1, ("A", "p"): 2, ("A", "l"): 2,
    ("B", "z"): 3, ("B", "f"): 4, ("B", "p"): 5, ("B", "l"): 5,
    ("C", "o"): 6, ("C0", "y"): 6, ("C1", "y"): 6, ("C0", "z"): 6, ("C1", "z"): 6,
    ("C0", "f"): 7, ("C1", "f"): 7, ("C0", "l"): 8, ("C1", "l"): 8,
}


def kernel(
    copies, order, rows, tokens,
    ph, rh, pw, rw, tg, dm, kp, pr, out_excess, out_weights,
    G, W, acc0, acc1, acc2, accC, tgv, dmv, kpv, prv, M0, M1, onehot, early, late, zearly, zlate, pearly, plate, dbuf,
    keep_ref, s_send, s_recv,
):
    x, y, c, z = (lax.axis_index(a) for a in ("dp_0", "dp_1", "dp_2", "tensor"))
    other = 1 - c
    pos = {"x": (x, 4), "y": (y, 4), "z": (z, 8)}

    def at(axis, d):
        p, n = pos[axis]
        return lax.rem(p + (d % n), n) if d % n else p

    def peer(axis, d):
        return {AXIS[axis]: at(axis, d)}

    def cols(dz, half=None):
        begin = at("z", dz) * 512
        if half is None:
            return pl.ds(pl.multiple_of(begin, 512), 512)
        return pl.ds(pl.multiple_of(begin + 256 * half, 256), 256)

    def view(token):
        colour, phase, half = token[0], token[1], token[-1]
        ms = slice(0, 2) if half is None else half
        if colour in ("A", "B"):
            k = 0 if colour == "A" else 1
            last, first = ("x", "y") if colour == "A" else ("y", "x")
            dz = token[2]
            if phase == "z":
                return G.at[k, ms, at(last, 0), at(first, 0), :, cols(dz)]
            if phase == "f":
                return G.at[k, ms, at(last, 0), at(first, token[3]), :, cols(dz)]
            if phase == "p":
                return G.at[k, ms, at(last, token[4]), at(first, token[3]), :, cols(dz)]
            return G.at[k, ms, at(last, token[3]), :, :, cols(dz)]
        d = token[2]
        if colour == "C":
            return G.at[2, ms, x, y, :, cols(d)]
        if phase in ("f", "y"):
            cs = cols(0 if phase == "f" else token[3], half)
            if colour == "C0":
                return G.at[2, 0, at("x", d), y, :, cs]
            return G.at[2, 1, x, at("y", d), :, cs]
        cs = cols(0 if phase == "l" else token[3], half)
        if colour == "C0":
            return G.at[2, 0, :, at("y", d), :, cs]
        return G.at[2, 1, at("x", d), :, :, cs]

    def wait(ref, sem):
        pltpu.make_async_copy(ref, ref, sem).wait()

    f32 = jnp.float32
    lane = lax.broadcasted_iota(jnp.int32, (8, 128), 1)
    sub = lax.broadcasted_iota(jnp.int32, (8, 128), 0)

    me = x * 4 + y
    label = lax.broadcasted_iota(jnp.int32, (128, 128), 0).astype(f32)

    def spread_z(buf, value, stage):
        buf[z] = value
        for d in (4, 3, 5, 2, 6, 1, 7):
            pltpu.make_async_remote_copy(
                src_ref=buf.at[z], dst_ref=buf.at[z], send_sem=s_send.at[stage], recv_sem=s_recv.at[stage],
                device_id=peer("z", d), device_id_type=MESH,
            ).start()

    def spread_xy(buf, value, stage):
        buf[me] = value
        for dx, dy in PLANE:
            pltpu.make_async_remote_copy(
                src_ref=buf.at[me], dst_ref=buf.at[me], send_sem=s_send.at[stage], recv_sem=s_recv.at[stage],
                device_id={**peer("x", dx), **peer("y", dy)}, device_id_type=MESH,
            ).start()

    def arrived(buf, stage):
        wait(buf.at[pl.ds(0, buf.shape[0] - 1)], s_recv.at[stage])

    def joined(parts):
        peak = parts[0]
        for p in parts[1:]:
            peak = jnp.maximum(peak, p)
        total = jnp.exp(parts[0] - peak)
        for p in parts[1:]:
            total = total + jnp.exp(p - peak)
        return peak + jnp.log(total)

    def added(parts):
        total = parts[0]
        for p in parts[1:]:
            total = total + p
        return total

    def join_early(buf):
        n = buf.shape[0]
        return jnp.stack([joined([buf[s, 0] for s in range(n)]), added([buf[s, 1] for s in range(n)])])

    def join_late(buf):
        parts = [buf[s] for s in range(buf.shape[0])]
        return jnp.where(sub < 4, joined(parts), added(parts))

    def gather(own_sem, small_sem, head_sem, swap_send, swap_recv, g_send, g_recv, m_send, m_recv):
        arrival_at = {}
        for cp in copies:
            arrival_at.setdefault(cp["arrival"], [len(arrival_at), 0])[1] += cp["size"]
        amounts = {
            32 * KB: G.at[0, :, 0, 0, :, pl.ds(0, 512)],
            64 * KB: G.at[0, 0, 0, :, :, pl.ds(0, 512)],
            128 * KB: G.at[0, :, 0, :, :, pl.ds(0, 512)],
            256 * KB: G.at[0:2, :, 0, :, :, pl.ds(0, 512)],
        }

        def send(i):
            cp = copies[i]
            ref = view(cp["source"])
            pltpu.make_async_remote_copy(
                src_ref=ref, dst_ref=ref,
                send_sem=g_send.at[SEND_CLASS[cp["source"][:2]]], recv_sem=g_recv.at[arrival_at[cp["arrival"]][0]],
                device_id=peer(cp["axis"], cp["sign"]), device_id_type=MESH,
            ).start()

        def receive(arrival):
            index, size = arrival_at[arrival]
            wait(amounts[size], g_recv.at[index])

        for m, src in enumerate((ph, rh)):
            for k in range(3):
                dst = G.at[k, m, y, x, :, cols(0)] if k == 1 else G.at[k, m, x, y, :, cols(0)]
                pltpu.make_async_copy(src.at[pl.ds(16 * k, 16), :], dst, own_sem).start()
        small = ((tg, tgv), (dm, dmv), (kp, kpv), (pr, prv))
        for k, (src, dst) in enumerate(small):
            pltpu.make_async_copy(src, dst, small_sem.at[k]).start()
        heads = (pw, rw)

        barrier = pltpu.get_barrier_semaphore()
        peers = [peer(a, d) for a in "xyz" for d in (1, -1)] + [{"dp_2": other}]
        for target in peers:
            pl.semaphore_signal(barrier, inc=1, device_id=target, device_id_type=MESH)
        early[...] = jnp.zeros_like(early)
        late[...] = jnp.zeros_like(late)
        M0[y] = jnp.zeros((8, 128), jnp.float32)
        with jax.named_scope("entry_barrier"):
            pl.semaphore_wait(barrier, len(peers))
        with jax.named_scope("own_blocks"):
            wait(G.at[:, :, 0, 0, :, pl.ds(0, 512)], own_sem)

        def meta_send(axis, d):
            src, dst, k = (M0.at[y], M0.at[y], 0) if axis == "y" else (M0, M1.at[x], 1)
            pltpu.make_async_remote_copy(
                src_ref=src, dst_ref=dst, send_sem=m_send.at[k], recv_sem=m_recv.at[k],
                device_id=peer(axis, d), device_id_type=MESH,
            ).start()

        def swap(m, dz, q):
            pltpu.make_async_remote_copy(
                src_ref=heads[m].at[:, cols(dz)], dst_ref=W.at[m, 1, :, cols(dz)],
                send_sem=swap_send, recv_sem=swap_recv.at[q],
                device_id={"dp_2": other}, device_id_type=MESH,
            ).start()

        accs = {0: acc0, 1: acc1, 2: acc2, "C": accC}

        def block(group, m, dz):
            cs = cols(dz)
            if group == "C":
                return G[2, m, :, :, :, cs].reshape(256, 512)
            pieces = []
            for d in {0: (0,), 1: (-1, 1), 2: (2,)}[group]:
                pieces.append(G[0, m, at("x", d), :, :, cs].reshape(64, 512))
                pieces.append(G[1, m, at("y", d), :, :, cs].reshape(64, 512))
            return jnp.concatenate(pieces, axis=0)

        done_heads = set()

        def compute(i):
            group, dzs = WORK[i]
            if not done_heads:
                wait(W.at[:, 0], head_sem)
            for dz in dzs:
                if dz not in done_heads:
                    wait(W.at[:, 1, :, cols(dz)], swap_recv.at[RING8.index(dz)])
                    done_heads.add(dz)
            acc = accs[group]
            first = 0 in dzs

            for m in (0, 1):
                rhs = [block(group, m, dz) for dz in dzs]
                for h in (0, 1):
                    total = None
                    for dz, r in zip(dzs, rhs):
                        part = lax.dot_general(
                            W[m, h, :, cols(dz)], r, (((1,), (1,)), ((), ())), preferred_element_type=f32
                        )
                        total = part if total is None else total + part
                    acc[m, h] = total if first else acc[m, h] + total

        dev = ((x * 4 + y) * 2 + c) * 8 + z
        dev_other = ((x * 4 + y) * 2 + other) * 8 + z
        offsets = (dev * rows, dev_other * rows)

        def spread(quantity):
            j = lax.broadcasted_iota(jnp.int32, (128, 128), 0)
            l = lax.broadcasted_iota(jnp.int32, (128, 128), 1)
            low = l % 16
            sel_ab = (j == low + jnp.where(l < 64, 0, 16)).astype(f32)
            sel_c = (j == low + 32).astype(f32)
            ab = jnp.dot(quantity, sel_ab, precision=lax.Precision.HIGHEST, preferred_element_type=f32)
            cc = jnp.dot(quantity, sel_c, precision=lax.Precision.HIGHEST, preferred_element_type=f32)
            d = lax.broadcasted_iota(jnp.int32, (16, 128), 0)
            l = lax.broadcasted_iota(jnp.int32, (16, 128), 1)
            q = (l // 16) % 4
            result = jnp.zeros((8, 128), f32)
            for a in range(4):
                owner = jnp.where(l < 64, a * 4 + q, q * 4 + a)
                row = jnp.sum(jnp.where(d == owner, ab, 0.0), axis=0, keepdims=True)
                result = jnp.where(sub == a, row, result)
            for a in range(2):
                owner = (2 * a + l // 64) * 4 + q
                row = jnp.sum(jnp.where(d == owner, cc, 0.0), axis=0, keepdims=True)
                result = jnp.where(sub == 4 + a, row, result)
            return result

        def stats(group, wanted):
            acc = accs[group]
            width = acc.shape[-1]
            if group == "C":
                spots = [jnp.full((8, 128), b, jnp.int32) for b in range(2)]
                want = [wanted[4 + b : 5 + b, :] for b in range(2)]
            else:
                spots = [
                    jnp.where(lane < 64, at("x", d), at("y", d)) for d in {0: (0,), 1: (-1, 1), 2: (2,)}[group]
                ]
                want = [jnp.sum(jnp.where(sub == p, wanted, 0.0), axis=0, keepdims=True) for p in spots]
            want = jnp.concatenate(want, axis=1).astype(jnp.int32) if len(want) > 1 else want[0].astype(jnp.int32)
            vocab = lax.broadcasted_iota(jnp.int32, (rows, width), 0)
            lses, hits = [], []
            for m in (0, 1):
                peak = jnp.maximum(
                    jnp.max(acc[m, 0], axis=0, keepdims=True), jnp.max(acc[m, 1], axis=0, keepdims=True)
                )
                total = jnp.zeros((1, width), f32)
                hit = jnp.zeros((1, width), f32)
                for h in (0, 1):
                    logits = acc[m, h]
                    total += jnp.sum(jnp.exp(logits - peak), axis=0, keepdims=True)
                    match = vocab == want - offsets[h]
                    hit += jnp.sum(jnp.where(match, logits, 0.0), axis=0, keepdims=True)
                lses.append(peak + jnp.log(total))
                hits.append(hit)
            for b, spot in enumerate(spots):
                one, two, hit = (r[:, 128 * b : 128 * (b + 1)] for r in (lses[0], lses[1], hits[0] - hits[1]))
                if group == "C":
                    value = jnp.where(sub == spot, one, late[...])
                    value = jnp.where(sub == spot + 2, two, value)
                    late[...] = jnp.where(sub == spot + 4, hit, value)
                else:
                    value = jnp.where(sub == spot, one, early[0])
                    early[0] = jnp.where(sub == spot + 4, two, value)
                    early[1] = jnp.where(sub == spot, hit, early[1])

        tables = {}
        pending = {g: sum(1 for w in WORK if w[0] == g) for g in accs}
        steps = computes = 0
        for kind, i in order:
            if kind == "send":
                send(i)
            elif kind == "recv":
                if not steps:
                    for q, dz in enumerate(RING8):
                        for m in (0, 1):
                            swap(m, dz, q)
                    for m in (0, 1):
                        pltpu.make_async_copy(heads[m], W.at[m, 0], head_sem).start()
                    with jax.named_scope("small_inputs"):
                        for k, (src, dst) in enumerate(small):
                            pltpu.make_async_copy(src, dst, small_sem.at[k]).wait()
                    for k, ref in enumerate((tgv, dmv, kpv)):
                        M0[y, k : k + 1, 0:tokens] = ref[...].astype(f32)
                steps += 1
                with jax.named_scope("recv"):
                    receive(i)
            else:
                if computes == 0:
                    for d in (1, 2, 3):
                        meta_send("y", d)
                if computes == 3:
                    wait(M0.at[pl.ds(0, 3)], m_recv.at[0])
                    M1[x] = M0[...]
                    for d in (1, 2, 3):
                        meta_send("x", d)
                computes += 1
                with jax.named_scope(f"compute_{i}"):
                    compute(i)
                group = WORK[i][0]
                pending[group] -= 1
                if not pending[group]:
                    if not tables:
                        wait(M1.at[pl.ds(0, 3)], m_recv.at[1])
                        for k, name in enumerate(("targets", "domains", "keep")):
                            tables[name] = spread(M1[:, :, k, :].reshape(16, 128))
                        onehot[...] = jnp.concatenate(
                            [(tables["domains"][b : b + 1, :] == label).astype(jnp.bfloat16) for b in range(6)], axis=1
                        )
                    with jax.named_scope(f"stats_{group}"):
                        stats(group, tables["targets"])
                    if group == "C":
                        spread_z(zlate, late[...], 1)
                    elif not any(pending[g] for g in (0, 1, 2)):
                        spread_z(zearly, early[...], 0)

        keep_ref[...] = tables["keep"]
        with jax.named_scope("sends_done"):
            for k in range(2):
                wait(G.at[k, :, 0, 0, :, pl.ds(0, 7 * 512)], g_send.at[3 * k])
                wait(G.at[k, :, 0, pl.ds(0, 3)], g_send.at[3 * k + 1])
                wait(G.at[k, :, pl.ds(0, 3)], g_send.at[3 * k + 2])
            wait(G.at[2, :, :, :, :, pl.ds(0, 7 * 512)], g_send.at[6])
            wait(G.at[2, :, pl.ds(0, 3), 0, :, pl.ds(0, 512)], g_send.at[7])
            wait(G.at[2, :, pl.ds(0, 3), :, :, pl.ds(0, 512)], g_send.at[8])
            wait(W.at[:, 1], swap_send)
            wait(M0.at[pl.ds(0, 3)], m_send.at[0])
            wait(M1.at[pl.ds(0, 3)], m_send.at[1])

    pl.run_scoped(
        gather, DMA, DMA((4,)), DMA, DMA, DMA((8,)), DMA((9,)),
        DMA((len({cp["arrival"] for cp in copies}),)), DMA((2,)), DMA((2,)),
    )

    keep = keep_ref[...]
    q = (lane // 16) % 4
    owner = jnp.where(sub < 4, jnp.where(lane < 64, sub * 4 + q, q * 4 + sub), (2 * (sub - 4) + lane // 64) * 4 + q)
    colour = jnp.where(sub < 4, jnp.where(lane < 64, 0, 1), 2)
    batch = ((owner * 2 + c) * 48 + 16 * colour + lane % 16) // 512

    def domain_sums(clipped, first, last):
        left = []
        for b in range(first, last):
            bb = batch[b : b + 1, :]
            top = jnp.where(bb == sub, clipped[b - first : b - first + 1, :], 0.0)
            low_rows = jnp.where(bb == sub - 3, keep[b : b + 1, :], 0.0)
            left.append(jnp.where(sub < 3, top, low_rows))
        left = jnp.concatenate(left, axis=1)
        thirds = []
        for _ in range(3):
            third = left.astype(jnp.bfloat16)
            thirds.append(third)
            left = left - third.astype(f32)
        parts = lax.dot_general(
            jnp.concatenate(thirds, axis=0), onehot[:, 128 * first : 128 * last], (((1,), (1,)), ((), ())),
            preferred_element_type=f32,
        )
        return parts[0:8] + (parts[8:16] + parts[16:24])

    def picked(values, spots):
        row = jnp.sum(jnp.where(spots, values, 0.0), axis=0, keepdims=True)
        row = jnp.broadcast_to(row, (8, 128))
        for shift in (64, 32, 16):
            row = row + pltpu.roll(row, shift, 1)
        return row

    with jax.named_scope("exchange_z"):
        arrived(zearly, 0)
        spread_xy(pearly, join_early(zearly), 2)
        with jax.named_scope("late_z"):
            arrived(zlate, 1)
        spread_xy(plate, join_late(zlate), 3)
    with jax.named_scope("exchange_xy"):
        arrived(pearly, 2)
        pair = join_early(pearly)
        gap_early = (pair[0, 0:4] - pair[0, 4:8]) - pair[1, 0:4]
        sums_early = domain_sums(jnp.maximum(gap_early, 0.0) * keep[0:4], 0, 4)
        nothing = jnp.zeros((4, 128), f32)
        excess = jnp.concatenate([gap_early, nothing], axis=0) * keep
        mine_a = picked(excess, (owner == me) & (colour == 0))
        mine_b = picked(excess, (owner == me) & (colour == 1))
        with jax.named_scope("late_xy"):
            arrived(plate, 3)
    tile = join_late(plate)
    gap_late = (tile[0:2] - tile[2:4]) - tile[4:6]
    sums = sums_early + domain_sums(jnp.maximum(gap_late, 0.0) * keep[4:6], 4, 6)
    dbuf[c] = sums

    def last_copy(slot):
        return pltpu.make_async_remote_copy(
            src_ref=dbuf.at[slot], dst_ref=dbuf.at[slot], send_sem=s_send.at[4], recv_sem=s_recv.at[4],
            device_id={"dp_2": other}, device_id_type=MESH,
        )

    last_copy(c).start()
    excess = jnp.concatenate([nothing, gap_late, nothing[0:2]], axis=0) * keep
    mine_c = picked(excess, (owner == me) & (colour == 2) & (sub < 6))
    mine_row = jnp.where(lane < 16, mine_a, jnp.where(lane < 32, mine_b, mine_c))[0:1, :]
    prior = prv[...]
    weights = prior / jnp.sum(prior, axis=1, keepdims=True)
    with jax.named_scope("partner_sums"):
        last_copy(other).wait_recv()
    both = dbuf[0] + dbuf[1]
    for s in range(STEPS):
        gain = both[s : s + 1, :] / jnp.maximum(both[3 + s : 4 + s, :], 1.0)
        raised = weights * jnp.exp(step_size * gain)
        weights = (1.0 - smoothing) * raised / jnp.sum(raised, axis=1, keepdims=True) + smoothing / DOMAINS
    out_weights[...] = jnp.log(weights)
    out_excess[...] = mine_row[:, 0:tokens]

    with jax.named_scope("sends_done"):
        for k, buf in enumerate((zearly, zlate, pearly, plate)):
            wait(buf.at[pl.ds(0, buf.shape[0] - 1)], s_send.at[k])
        last_copy(c).wait_send()


def local(ph, rh, pw, rw, targets, domains, keep_mask, prior):
    rows, tokens = pw.shape[0], targets.shape[0]
    copies = gather_plan()
    order = schedule(copies, WORK)
    f32, bf16 = jnp.float32, jnp.bfloat16
    anywhere = pl.BlockSpec(memory_space=pltpu.HBM)
    inside = pl.BlockSpec(memory_space=pltpu.VMEM)

    def body(*refs):
        kernel(copies, order, rows, tokens, *refs)

    out = pl.pallas_call(
        body,
        name="doremi",
        out_shape=[jax.ShapeDtypeStruct((1, tokens), f32), jax.ShapeDtypeStruct((1, 128), f32)],
        in_specs=[anywhere] * 8,
        out_specs=[inside] * 2,
        scratch_shapes=[
            pltpu.VMEM((3, 2, 4, 4, 16, 4096), bf16),
            pltpu.VMEM((2, 2, rows, 4096), bf16),
            pltpu.VMEM((2, 2, rows, 128), f32),
            pltpu.VMEM((2, 2, rows, 256), f32),
            pltpu.VMEM((2, 2, rows, 128), f32),
            pltpu.VMEM((2, 2, rows, 256), f32),
            pltpu.VMEM((1, tokens), jnp.int32),
            pltpu.VMEM((1, tokens), jnp.int32),
            pltpu.VMEM((1, tokens), jnp.int32),
            pltpu.VMEM((1, 128), f32),
            pltpu.VMEM((4, 8, 128), f32),
            pltpu.VMEM((4, 4, 8, 128), f32),
            pltpu.VMEM((128, 768), bf16),
            pltpu.VMEM((2, 8, 128), f32),
            pltpu.VMEM((8, 128), f32),
            pltpu.VMEM((8, 2, 8, 128), f32),
            pltpu.VMEM((8, 8, 128), f32),
            pltpu.VMEM((16, 2, 8, 128), f32),
            pltpu.VMEM((16, 8, 128), f32),
            pltpu.VMEM((2, 8, 128), f32),
            pltpu.VMEM((8, 128), f32),
            DMA((5,)), DMA((5,)),
        ],
        compiler_params=pltpu.CompilerParams(
            collective_id=0, has_side_effects=True, vmem_limit_bytes=53 * 1024 * 1024
        ),
        cost_estimate=pl.CostEstimate(flops=12_900_000_000, bytes_accessed=34_000_000, transcendentals=2_000_000),
    )(*(
        pltpu.with_memory_space_constraint(a, pltpu.HBM)
        for a in (ph, rh, pw, rw, targets[None], domains[None], keep_mask[None], prior[None])
    ))
    return out[0][0], out[1][0]


def solution(mesh):
    split = Mesh(
        mesh.devices.reshape(4, 4, 2, mesh.shape["tensor"]), ("dp_0", "dp_1", "dp_2", "tensor")
    )
    return jax.shard_map(
        local,
        mesh=split,
        in_specs=(
            P(DP, "tensor"),
            P(DP, "tensor"),
            P(DP_TENSOR, None),
            P(DP_TENSOR, None),
            P(DP),
            P(DP),
            P(DP),
            P(),
        ),
        out_specs=(P(DP), P()),
        check_vma=False,
    )
```

```python
import jax
import jax.numpy as jnp
from jax import lax
from jax.experimental import pallas as pl
from jax.experimental.pallas import tpu as pltpu
from jax.sharding import Mesh
from jax.sharding import PartitionSpec as P

DOMAINS = 128
STEPS = 3
DP = ("dp_0", "dp_1", "dp_2")
DP_TENSOR = ("dp_0", "dp_1", "dp_2", "tensor")
AXIS = {"x": "dp_0", "y": "dp_1", "z": "tensor"}
MESH = pl.DeviceIdType.MESH
DMA = pltpu.SemaphoreType.DMA

step_size = 1.0
smoothing = 0.001

KB = 1024
RATE = 46.6e3
HOP = 3.5
BACKLOG = 1.5
LAG = 0.6
FINE = (0, 1, -1)
AHEAD = 20
CHECKPOINTS = range(140, 470, 10)
RING4 = (0, 1, -1, 2)
RING8 = (0, 1, -1, 2, -2, 3, -3, 4)
PLANE = [(dx, dy) for dx in (2, 1, 3, 0) for dy in (2, 1, 3, 0) if dx or dy]
PLANE.sort(key=lambda p: -min(p[0], 4 - p[0]) - min(p[1], 4 - p[1]))


def ring(add, axis, size, token, need, far, rank, arrival, lag=0.01):
    for k in range(1, far + 1):
        halves = (0, 1) if k == far else (None, None)
        for sign, half in ((1, halves[0]), (-1, halves[1])):
            offset = far if k == far else -sign * k
            add(
                dict(
                    axis=axis,
                    sign=sign,
                    size=size // 2 if k == far else size,
                    source=token(-sign * (k - 1), half),
                    need=need if k == 1 else [token(-sign * (k - 1), None)],
                    given=token(offset, half),
                    rank=rank + lag * (k - 1),
                    arrival=arrival + (offset,),
                )
            )


def gather_plan():
    copies = []
    add = copies.append
    piece = 32 * KB
    for colour, first, last in (("A", "y", "x"), ("B", "x", "y")):
        own = [(colour, "z", 0, None)]
        ring(add, "z", piece, lambda d, h: (colour, "z", d, h), own, 4, 0, ("AB", "z"))
        for q, dz in enumerate(RING8):
            have = [(colour, "z", dz, None)]
            ring(add, first, piece, lambda d, h: (colour, "f", dz, d, h), have, 2, 1, ("AB", "f", dz))
            rank = 3 + 0.1 * q
            if dz in FINE:
                for df in RING4:
                    need = have if df == 0 else [(colour, "f", dz, df, None)]
                    token = lambda d, h: (colour, "p", dz, df, d, h)
                    ring(add, last, piece, token, need, 2, rank, ("AB", "p", dz, abs(df)), LAG)
            else:
                need = have + [(colour, "f", dz, d, None) for d in (1, -1, 2)]
                token = lambda d, h: (colour, "l", dz, d, h)
                ring(add, last, 4 * piece, token, need, 2, rank, ("AB", "l", dz), LAG)
    piece = 16 * KB
    own = [("C", "o", 0, None)]
    ring(add, "z", 2 * piece, lambda d, h: ("C", "o", d, h), own, 4, 2, ("C", "o"))
    for colour, first, last in (("C0", "x", "y"), ("C1", "y", "x")):
        ring(add, first, piece, lambda d, h: (colour, "f", d, h), own, 2, 0, ("C", "f"))
        need = own + [(colour, "f", d, None) for d in (1, -1, 2)]
        ring(add, last, 4 * piece, lambda d, h: (colour, "l", d, h), need, 2, 0, ("C", "l"))
        for j in (1, -1, 2):
            need = [(colour, "f", j, None)]
            ring(add, "z", piece, lambda d, h: (colour, "y", j, d, h), need, 4, 2, ("C", "y", j))
        for j in (1, -1, 2):
            need = [(colour, "l", j, None)]
            ring(add, "z", 4 * piece, lambda d, h: (colour, "z", j, d, h), need, 4, 2, ("C", "z", j))
    return copies


OWN = {("A", "z", 0, None), ("B", "z", 0, None), ("C", "o", 0, None)}


def tokens_of(group, dzs):
    out = []
    for dz in dzs:
        if group == "C":
            if dz:
                out.append(("C", "o", dz, None))
            for colour in ("C0", "C1"):
                for j in (1, -1, 2):
                    if dz:
                        out += [(colour, "y", j, dz, None), (colour, "z", j, dz, None)]
                    else:
                        out += [(colour, "f", j, None), (colour, "l", j, None)]
            continue
        for colour in ("A", "B"):
            if group == 0:
                out += [(colour, "z", dz, None)] + [(colour, "f", dz, d, None) for d in (1, -1, 2)]
                continue
            for d in (1, -1) if group == 1 else (2,):
                if dz in FINE:
                    out += [(colour, "p", dz, df, d, None) for df in RING4]
                else:
                    out.append((colour, "l", dz, d, None))
    return out


WORK = [
    (0, (0,)), (0, (1, -1)), (0, (2, -2)), (0, (3, -3, 4)),
    (1, (0,)), (1, (1, -1)), (1, (2, -2)), (1, (3, -3)), (1, (4,)),
    (2, (0,)), (2, (1, -1)), (2, (2, -2)), (2, (3,)), (2, (-3,)), (2, (4,)),
    ("C", (0,)), ("C", (1, -1)), ("C", (2, -2)), ("C", (3, -3)), ("C", (4,)),
]
STATS_TIME = {0: 0.34, 1: 0.74, 2: 0.34, "C": 0.74}


def schedule(copies, works):
    arrival_of = {c["given"]: c["arrival"] for c in copies}
    members = {}
    for i, c in enumerate(copies):
        members.setdefault(c["arrival"], []).append(i)

    def arrivals(tokens):
        found = set()
        for t in tokens:
            if t not in OWN:
                found |= {arrival_of[p] for p in (t, t[:-1] + (0,), t[:-1] + (1,)) if p in arrival_of}
        return found

    deps = [arrivals(c["need"]) for c in copies]
    needs = [arrivals(tokens_of(*w)) for w in works]
    links = {}
    for i, c in enumerate(copies):
        links.setdefault((c["axis"], c["sign"]), []).append(i)
    got, free, landed = set(), dict.fromkeys(links, 0.0), {}
    unsent, undone = set(range(len(copies))), set(range(len(works)))
    left = {g: sum(1 for w in works if w[0] == g) for g in STATS_TIME}
    now, order = 0.0, []
    while unsent or undone or len(got) < len(members):
        coming = {
            a: max(landed[i] for i in m)
            for a, m in members.items()
            if a not in got and all(i in landed for i in m)
        }
        here = sorted((when, str(a), a) for a, when in coming.items() if when <= now + 1e-9)
        if here:
            for _, _, a in here:
                got.add(a)
                order.append(("recv", a))
                now += 0.02
            continue
        sent = False
        for link, all_of in links.items():
            while free[link] - now < BACKLOG:
                ready = [i for i in all_of if i in unsent and deps[i] <= got]
                if not ready:
                    break
                i = min(ready, key=lambda i: (copies[i]["rank"], i))
                free[link] = max(now, free[link]) + copies[i]["size"] / RATE
                landed[i] = free[link] + HOP
                unsent.discard(i)
                order.append(("send", i))
                now += 0.012
                sent = True
        if sent:
            continue
        ready = [i for i in undone if needs[i] <= got]
        if ready:
            i = min(ready)
            undone.discard(i)
            order.append(("compute", i))
            now += 0.2 + 0.54 * len(works[i][1])
            left[works[i][0]] -= 1
            if not left[works[i][0]]:
                now += STATS_TIME[works[i][0]]
            continue
        times = list(coming.values())
        for link, all_of in links.items():
            if any(i in unsent and deps[i] <= got for i in all_of):
                times.append(free[link] - BACKLOG + 1e-6)
        now = max(now, min(times))
    return order


SEND_CLASS = {
    ("A", "z"): 0, ("A", "f"): 1, ("A", "p"): 2, ("A", "l"): 2,
    ("B", "z"): 3, ("B", "f"): 4, ("B", "p"): 5, ("B", "l"): 5,
    ("C", "o"): 6, ("C0", "y"): 6, ("C1", "y"): 6, ("C0", "z"): 6, ("C1", "z"): 6,
    ("C0", "f"): 7, ("C1", "f"): 7, ("C0", "l"): 8, ("C1", "l"): 8,
}


def kernel(
    copies, order, rows, tokens,
    ph, rh, pw, rw, tg, dm, kp, pr, out_excess, out_weights,
    G, W, acc0, acc1, acc2, accC, tgv, dmv, kpv, prv, M0, M1, onehot, early, late, zearly, zlate, pearly, plate, dbuf,
    keep_ref, s_send, s_recv,
):
    x, y, c, z = (lax.axis_index(a) for a in ("dp_0", "dp_1", "dp_2", "tensor"))
    other = 1 - c
    pos = {"x": (x, 4), "y": (y, 4), "z": (z, 8)}

    def at(axis, d):
        p, n = pos[axis]
        return lax.rem(p + (d % n), n) if d % n else p

    def peer(axis, d):
        return {AXIS[axis]: at(axis, d)}

    def cols(dz, half=None):
        begin = at("z", dz) * 512
        if half is None:
            return pl.ds(pl.multiple_of(begin, 512), 512)
        return pl.ds(pl.multiple_of(begin + 256 * half, 256), 256)

    def view(token):
        colour, phase, half = token[0], token[1], token[-1]
        ms = slice(0, 2) if half is None else half
        if colour in ("A", "B"):
            k = 0 if colour == "A" else 1
            last, first = ("x", "y") if colour == "A" else ("y", "x")
            dz = token[2]
            if phase == "z":
                return G.at[k, ms, at(last, 0), at(first, 0), :, cols(dz)]
            if phase == "f":
                return G.at[k, ms, at(last, 0), at(first, token[3]), :, cols(dz)]
            if phase == "p":
                return G.at[k, ms, at(last, token[4]), at(first, token[3]), :, cols(dz)]
            return G.at[k, ms, at(last, token[3]), :, :, cols(dz)]
        d = token[2]
        if colour == "C":
            return G.at[2, ms, x, y, :, cols(d)]
        if phase in ("f", "y"):
            cs = cols(0 if phase == "f" else token[3], half)
            if colour == "C0":
                return G.at[2, 0, at("x", d), y, :, cs]
            return G.at[2, 1, x, at("y", d), :, cs]
        cs = cols(0 if phase == "l" else token[3], half)
        if colour == "C0":
            return G.at[2, 0, :, at("y", d), :, cs]
        return G.at[2, 1, at("x", d), :, :, cs]

    def wait(ref, sem):
        pltpu.make_async_copy(ref, ref, sem).wait()

    f32 = jnp.float32
    lane = lax.broadcasted_iota(jnp.int32, (8, 128), 1)
    sub = lax.broadcasted_iota(jnp.int32, (8, 128), 0)

    me = x * 4 + y
    label = lax.broadcasted_iota(jnp.int32, (128, 128), 0).astype(f32)

    def spread_z(buf, value, stage):
        buf[z] = value
        for d in (4, 3, 5, 2, 6, 1, 7):
            pltpu.make_async_remote_copy(
                src_ref=buf.at[z], dst_ref=buf.at[z], send_sem=s_send.at[stage], recv_sem=s_recv.at[stage],
                device_id=peer("z", d), device_id_type=MESH,
            ).start()

    def spread_xy(buf, value, stage):
        buf[me] = value
        for dx, dy in PLANE:
            pltpu.make_async_remote_copy(
                src_ref=buf.at[me], dst_ref=buf.at[me], send_sem=s_send.at[stage], recv_sem=s_recv.at[stage],
                device_id={**peer("x", dx), **peer("y", dy)}, device_id_type=MESH,
            ).start()

    def arrived(buf, stage):
        wait(buf.at[pl.ds(0, buf.shape[0] - 1)], s_recv.at[stage])

    def joined(parts):
        peak = parts[0]
        for p in parts[1:]:
            peak = jnp.maximum(peak, p)
        total = jnp.exp(parts[0] - peak)
        for p in parts[1:]:
            total = total + jnp.exp(p - peak)
        return peak + jnp.log(total)

    def added(parts):
        total = parts[0]
        for p in parts[1:]:
            total = total + p
        return total

    def join_early(buf):
        n = buf.shape[0]
        return jnp.stack([joined([buf[s, 0] for s in range(n)]), added([buf[s, 1] for s in range(n)])])

    def join_late(buf):
        parts = [buf[s] for s in range(buf.shape[0])]
        return jnp.where(sub < 4, joined(parts), added(parts))

    def gather(own_sem, small_sem, head_sem, swap_send, swap_recv, g_send, g_recv, m_send, m_recv, pace):
        arrival_at = {}
        for cp in copies:
            arrival_at.setdefault(cp["arrival"], [len(arrival_at), 0])[1] += cp["size"]
        amounts = {
            32 * KB: G.at[0, :, 0, 0, :, pl.ds(0, 512)],
            64 * KB: G.at[0, 0, 0, :, :, pl.ds(0, 512)],
            128 * KB: G.at[0, :, 0, :, :, pl.ds(0, 512)],
            256 * KB: G.at[0:2, :, 0, :, :, pl.ds(0, 512)],
        }

        def send(i):
            cp = copies[i]
            ref = view(cp["source"])
            pltpu.make_async_remote_copy(
                src_ref=ref, dst_ref=ref,
                send_sem=g_send.at[SEND_CLASS[cp["source"][:2]]], recv_sem=g_recv.at[arrival_at[cp["arrival"]][0]],
                device_id=peer(cp["axis"], cp["sign"]), device_id_type=MESH,
            ).start()

        def receive(arrival):
            index, size = arrival_at[arrival]
            wait(amounts[size], g_recv.at[index])

        for m, src in enumerate((ph, rh)):
            for k in range(3):
                dst = G.at[k, m, y, x, :, cols(0)] if k == 1 else G.at[k, m, x, y, :, cols(0)]
                pltpu.make_async_copy(src.at[pl.ds(16 * k, 16), :], dst, own_sem).start()
        small = ((tg, tgv), (dm, dmv), (kp, kpv), (pr, prv))
        for k, (src, dst) in enumerate(small):
            pltpu.make_async_copy(src, dst, small_sem.at[k]).start()
        heads = (pw, rw)

        barrier = pltpu.get_barrier_semaphore()
        peers = [peer(a, d) for a in "xyz" for d in (1, -1)] + [{"dp_2": other}]
        for target in peers:
            pl.semaphore_signal(barrier, inc=1, device_id=target, device_id_type=MESH)
        early[...] = jnp.zeros_like(early)
        late[...] = jnp.zeros_like(late)
        M0[y] = jnp.zeros((8, 128), jnp.float32)
        with jax.named_scope("entry_barrier"):
            pl.semaphore_wait(barrier, len(peers))
        with jax.named_scope("own_blocks"):
            wait(G.at[:, :, 0, 0, :, pl.ds(0, 512)], own_sem)

        def meta_send(axis, d):
            src, dst, k = (M0.at[y], M0.at[y], 0) if axis == "y" else (M0, M1.at[x], 1)
            pltpu.make_async_remote_copy(
                src_ref=src, dst_ref=dst, send_sem=m_send.at[k], recv_sem=m_recv.at[k],
                device_id=peer(axis, d), device_id_type=MESH,
            ).start()

        def swap(m, dz, q):
            pltpu.make_async_remote_copy(
                src_ref=heads[m].at[:, cols(dz)], dst_ref=W.at[m, 1, :, cols(dz)],
                send_sem=swap_send, recv_sem=swap_recv.at[q],
                device_id={"dp_2": other}, device_id_type=MESH,
            ).start()

        accs = {0: acc0, 1: acc1, 2: acc2, "C": accC}

        def block(group, m, dz):
            cs = cols(dz)
            if group == "C":
                return G[2, m, :, :, :, cs].reshape(256, 512)
            pieces = []
            for d in {0: (0,), 1: (-1, 1), 2: (2,)}[group]:
                pieces.append(G[0, m, at("x", d), :, :, cs].reshape(64, 512))
                pieces.append(G[1, m, at("y", d), :, :, cs].reshape(64, 512))
            return jnp.concatenate(pieces, axis=0)

        done_heads = set()

        def compute(i):
            group, dzs = WORK[i]
            if not done_heads:
                wait(W.at[:, 0], head_sem)
            for dz in dzs:
                if dz not in done_heads:
                    wait(W.at[:, 1, :, cols(dz)], swap_recv.at[RING8.index(dz)])
                    done_heads.add(dz)
            acc = accs[group]
            first = 0 in dzs

            for m in (0, 1):
                rhs = [block(group, m, dz) for dz in dzs]
                for h in (0, 1):
                    total = None
                    for dz, r in zip(dzs, rhs):
                        part = lax.dot_general(
                            W[m, h, :, cols(dz)], r, (((1,), (1,)), ((), ())), preferred_element_type=f32
                        )
                        total = part if total is None else total + part
                    acc[m, h] = total if first else acc[m, h] + total

        dev = ((x * 4 + y) * 2 + c) * 8 + z
        dev_other = ((x * 4 + y) * 2 + other) * 8 + z
        offsets = (dev * rows, dev_other * rows)

        def spread(quantity):
            j = lax.broadcasted_iota(jnp.int32, (128, 128), 0)
            l = lax.broadcasted_iota(jnp.int32, (128, 128), 1)
            low = l % 16
            sel_ab = (j == low + jnp.where(l < 64, 0, 16)).astype(f32)
            sel_c = (j == low + 32).astype(f32)
            ab = jnp.dot(quantity, sel_ab, precision=lax.Precision.HIGHEST, preferred_element_type=f32)
            cc = jnp.dot(quantity, sel_c, precision=lax.Precision.HIGHEST, preferred_element_type=f32)
            d = lax.broadcasted_iota(jnp.int32, (16, 128), 0)
            l = lax.broadcasted_iota(jnp.int32, (16, 128), 1)
            q = (l // 16) % 4
            result = jnp.zeros((8, 128), f32)
            for a in range(4):
                owner = jnp.where(l < 64, a * 4 + q, q * 4 + a)
                row = jnp.sum(jnp.where(d == owner, ab, 0.0), axis=0, keepdims=True)
                result = jnp.where(sub == a, row, result)
            for a in range(2):
                owner = (2 * a + l // 64) * 4 + q
                row = jnp.sum(jnp.where(d == owner, cc, 0.0), axis=0, keepdims=True)
                result = jnp.where(sub == 4 + a, row, result)
            return result

        def stats(group, wanted):
            acc = accs[group]
            width = acc.shape[-1]
            if group == "C":
                spots = [jnp.full((8, 128), b, jnp.int32) for b in range(2)]
                want = [wanted[4 + b : 5 + b, :] for b in range(2)]
            else:
                spots = [
                    jnp.where(lane < 64, at("x", d), at("y", d)) for d in {0: (0,), 1: (-1, 1), 2: (2,)}[group]
                ]
                want = [jnp.sum(jnp.where(sub == p, wanted, 0.0), axis=0, keepdims=True) for p in spots]
            want = jnp.concatenate(want, axis=1).astype(jnp.int32) if len(want) > 1 else want[0].astype(jnp.int32)
            vocab = lax.broadcasted_iota(jnp.int32, (rows, width), 0)
            lses, hits = [], []
            for m in (0, 1):
                peak = jnp.maximum(
                    jnp.max(acc[m, 0], axis=0, keepdims=True), jnp.max(acc[m, 1], axis=0, keepdims=True)
                )
                total = jnp.zeros((1, width), f32)
                hit = jnp.zeros((1, width), f32)
                for h in (0, 1):
                    logits = acc[m, h]
                    total += jnp.sum(jnp.exp(logits - peak), axis=0, keepdims=True)
                    match = vocab == want - offsets[h]
                    hit += jnp.sum(jnp.where(match, logits, 0.0), axis=0, keepdims=True)
                lses.append(peak + jnp.log(total))
                hits.append(hit)
            for b, spot in enumerate(spots):
                one, two, hit = (r[:, 128 * b : 128 * (b + 1)] for r in (lses[0], lses[1], hits[0] - hits[1]))
                if group == "C":
                    value = jnp.where(sub == spot, one, late[...])
                    value = jnp.where(sub == spot + 2, two, value)
                    late[...] = jnp.where(sub == spot + 4, hit, value)
                else:
                    value = jnp.where(sub == spot, one, early[0])
                    early[0] = jnp.where(sub == spot + 4, two, value)
                    early[1] = jnp.where(sub == spot, hit, early[1])

        tables = {}
        pending = {g: sum(1 for w in WORK if w[0] == g) for g in accs}
        steps = computes = 0
        assert CHECKPOINTS[-1] < len(order)
        for position, (kind, i) in enumerate(order):
            if position in CHECKPOINTS:
                @pl.when(c == 0)
                def _():
                    pl.semaphore_signal(pace, inc=1, device_id={"dp_2": other}, device_id_type=MESH)
            if position + AHEAD in CHECKPOINTS:
                @pl.when(c == 1)
                def _():
                    pl.semaphore_wait(pace, 1)
            if kind == "send":
                send(i)
            elif kind == "recv":
                if not steps:
                    for q, dz in enumerate(RING8):
                        for m in (0, 1):
                            swap(m, dz, q)
                    for m in (0, 1):
                        pltpu.make_async_copy(heads[m], W.at[m, 0], head_sem).start()
                    with jax.named_scope("small_inputs"):
                        for k, (src, dst) in enumerate(small):
                            pltpu.make_async_copy(src, dst, small_sem.at[k]).wait()
                    for k, ref in enumerate((tgv, dmv, kpv)):
                        M0[y, k : k + 1, 0:tokens] = ref[...].astype(f32)
                steps += 1
                with jax.named_scope("recv"):
                    receive(i)
            else:
                if computes == 0:
                    for d in (1, 2, 3):
                        meta_send("y", d)
                if computes == 3:
                    wait(M0.at[pl.ds(0, 3)], m_recv.at[0])
                    M1[x] = M0[...]
                    for d in (1, 2, 3):
                        meta_send("x", d)
                computes += 1
                with jax.named_scope(f"compute_{i}"):
                    compute(i)
                group = WORK[i][0]
                pending[group] -= 1
                if not pending[group]:
                    if not tables:
                        wait(M1.at[pl.ds(0, 3)], m_recv.at[1])
                        for k, name in enumerate(("targets", "domains", "keep")):
                            tables[name] = spread(M1[:, :, k, :].reshape(16, 128))
                        onehot[...] = jnp.concatenate(
                            [(tables["domains"][b : b + 1, :] == label).astype(jnp.bfloat16) for b in range(6)], axis=1
                        )
                    with jax.named_scope(f"stats_{group}"):
                        stats(group, tables["targets"])
                    if group == "C":
                        spread_z(zlate, late[...], 1)
                    elif not any(pending[g] for g in (0, 1, 2)):
                        spread_z(zearly, early[...], 0)

        keep_ref[...] = tables["keep"]
        with jax.named_scope("sends_done"):
            for k in range(2):
                wait(G.at[k, :, 0, 0, :, pl.ds(0, 7 * 512)], g_send.at[3 * k])
                wait(G.at[k, :, 0, pl.ds(0, 3)], g_send.at[3 * k + 1])
                wait(G.at[k, :, pl.ds(0, 3)], g_send.at[3 * k + 2])
            wait(G.at[2, :, :, :, :, pl.ds(0, 7 * 512)], g_send.at[6])
            wait(G.at[2, :, pl.ds(0, 3), 0, :, pl.ds(0, 512)], g_send.at[7])
            wait(G.at[2, :, pl.ds(0, 3), :, :, pl.ds(0, 512)], g_send.at[8])
            wait(W.at[:, 1], swap_send)
            wait(M0.at[pl.ds(0, 3)], m_send.at[0])
            wait(M1.at[pl.ds(0, 3)], m_send.at[1])

    pl.run_scoped(
        gather, DMA, DMA((4,)), DMA, DMA, DMA((8,)), DMA((9,)),
        DMA((len({cp["arrival"] for cp in copies}),)), DMA((2,)), DMA((2,)), pltpu.SemaphoreType.REGULAR,
    )

    keep = keep_ref[...]
    q = (lane // 16) % 4
    owner = jnp.where(sub < 4, jnp.where(lane < 64, sub * 4 + q, q * 4 + sub), (2 * (sub - 4) + lane // 64) * 4 + q)
    colour = jnp.where(sub < 4, jnp.where(lane < 64, 0, 1), 2)
    batch = ((owner * 2 + c) * 48 + 16 * colour + lane % 16) // 512

    def domain_sums(clipped, first, last):
        left = []
        for b in range(first, last):
            bb = batch[b : b + 1, :]
            top = jnp.where(bb == sub, clipped[b - first : b - first + 1, :], 0.0)
            low_rows = jnp.where(bb == sub - 3, keep[b : b + 1, :], 0.0)
            left.append(jnp.where(sub < 3, top, low_rows))
        left = jnp.concatenate(left, axis=1)
        thirds = []
        for _ in range(3):
            third = left.astype(jnp.bfloat16)
            thirds.append(third)
            left = left - third.astype(f32)
        parts = lax.dot_general(
            jnp.concatenate(thirds, axis=0), onehot[:, 128 * first : 128 * last], (((1,), (1,)), ((), ())),
            preferred_element_type=f32,
        )
        return parts[0:8] + (parts[8:16] + parts[16:24])

    def picked(values, spots):
        row = jnp.sum(jnp.where(spots, values, 0.0), axis=0, keepdims=True)
        row = jnp.broadcast_to(row, (8, 128))
        for shift in (64, 32, 16):
            row = row + pltpu.roll(row, shift, 1)
        return row

    with jax.named_scope("exchange_z"):
        arrived(zearly, 0)
        spread_xy(pearly, join_early(zearly), 2)
        with jax.named_scope("late_z"):
            arrived(zlate, 1)
        spread_xy(plate, join_late(zlate), 3)
    with jax.named_scope("exchange_xy"):
        arrived(pearly, 2)
        pair = join_early(pearly)
        gap_early = (pair[0, 0:4] - pair[0, 4:8]) - pair[1, 0:4]
        sums_early = domain_sums(jnp.maximum(gap_early, 0.0) * keep[0:4], 0, 4)
        nothing = jnp.zeros((4, 128), f32)
        excess = jnp.concatenate([gap_early, nothing], axis=0) * keep
        mine_a = picked(excess, (owner == me) & (colour == 0))
        mine_b = picked(excess, (owner == me) & (colour == 1))
        with jax.named_scope("late_xy"):
            arrived(plate, 3)
    tile = join_late(plate)
    gap_late = (tile[0:2] - tile[2:4]) - tile[4:6]
    sums = sums_early + domain_sums(jnp.maximum(gap_late, 0.0) * keep[4:6], 4, 6)
    dbuf[c] = sums

    def last_copy(slot):
        return pltpu.make_async_remote_copy(
            src_ref=dbuf.at[slot], dst_ref=dbuf.at[slot], send_sem=s_send.at[4], recv_sem=s_recv.at[4],
            device_id={"dp_2": other}, device_id_type=MESH,
        )

    last_copy(c).start()
    excess = jnp.concatenate([nothing, gap_late, nothing[0:2]], axis=0) * keep
    mine_c = picked(excess, (owner == me) & (colour == 2) & (sub < 6))
    mine_row = jnp.where(lane < 16, mine_a, jnp.where(lane < 32, mine_b, mine_c))[0:1, :]
    prior = prv[...]
    weights = prior / jnp.sum(prior, axis=1, keepdims=True)
    with jax.named_scope("partner_sums"):
        last_copy(other).wait_recv()
    both = dbuf[0] + dbuf[1]
    for s in range(STEPS):
        gain = both[s : s + 1, :] / jnp.maximum(both[3 + s : 4 + s, :], 1.0)
        raised = weights * jnp.exp(step_size * gain)
        weights = (1.0 - smoothing) * raised / jnp.sum(raised, axis=1, keepdims=True) + smoothing / DOMAINS
    out_weights[...] = jnp.log(weights)
    out_excess[...] = mine_row[:, 0:tokens]

    with jax.named_scope("sends_done"):
        for k, buf in enumerate((zearly, zlate, pearly, plate)):
            wait(buf.at[pl.ds(0, buf.shape[0] - 1)], s_send.at[k])
        last_copy(c).wait_send()


def local(ph, rh, pw, rw, targets, domains, keep_mask, prior):
    rows, tokens = pw.shape[0], targets.shape[0]
    copies = gather_plan()
    order = schedule(copies, WORK)
    f32, bf16 = jnp.float32, jnp.bfloat16
    anywhere = pl.BlockSpec(memory_space=pltpu.HBM)
    inside = pl.BlockSpec(memory_space=pltpu.VMEM)

    def body(*refs):
        kernel(copies, order, rows, tokens, *refs)

    out = pl.pallas_call(
        body,
        name="doremi",
        out_shape=[jax.ShapeDtypeStruct((1, tokens), f32), jax.ShapeDtypeStruct((1, 128), f32)],
        in_specs=[anywhere] * 8,
        out_specs=[inside] * 2,
        scratch_shapes=[
            pltpu.VMEM((3, 2, 4, 4, 16, 4096), bf16),
            pltpu.VMEM((2, 2, rows, 4096), bf16),
            pltpu.VMEM((2, 2, rows, 128), f32),
            pltpu.VMEM((2, 2, rows, 256), f32),
            pltpu.VMEM((2, 2, rows, 128), f32),
            pltpu.VMEM((2, 2, rows, 256), f32),
            pltpu.VMEM((1, tokens), jnp.int32),
            pltpu.VMEM((1, tokens), jnp.int32),
            pltpu.VMEM((1, tokens), jnp.int32),
            pltpu.VMEM((1, 128), f32),
            pltpu.VMEM((4, 8, 128), f32),
            pltpu.VMEM((4, 4, 8, 128), f32),
            pltpu.VMEM((128, 768), bf16),
            pltpu.VMEM((2, 8, 128), f32),
            pltpu.VMEM((8, 128), f32),
            pltpu.VMEM((8, 2, 8, 128), f32),
            pltpu.VMEM((8, 8, 128), f32),
            pltpu.VMEM((16, 2, 8, 128), f32),
            pltpu.VMEM((16, 8, 128), f32),
            pltpu.VMEM((2, 8, 128), f32),
            pltpu.VMEM((8, 128), f32),
            DMA((5,)), DMA((5,)),
        ],
        compiler_params=pltpu.CompilerParams(
            collective_id=0, has_side_effects=True, vmem_limit_bytes=53 * 1024 * 1024
        ),
        cost_estimate=pl.CostEstimate(flops=12_900_000_000, bytes_accessed=34_000_000, transcendentals=2_000_000),
    )(*(
        pltpu.with_memory_space_constraint(a, pltpu.HBM)
        for a in (ph, rh, pw, rw, targets[None], domains[None], keep_mask[None], prior[None])
    ))
    return out[0][0], out[1][0]


def solution(mesh):
    split = Mesh(
        mesh.devices.reshape(4, 4, 2, mesh.shape["tensor"]), ("dp_0", "dp_1", "dp_2", "tensor")
    )
    return jax.shard_map(
        local,
        mesh=split,
        in_specs=(
            P(DP, "tensor"),
            P(DP, "tensor"),
            P(DP_TENSOR, None),
            P(DP_TENSOR, None),
            P(DP),
            P(DP),
            P(DP),
            P(),
        ),
        out_specs=(P(DP), P()),
        check_vma=False,
    )
```

```python
import jax
import jax.numpy as jnp
from jax import lax
from jax.experimental import pallas as pl
from jax.experimental.pallas import tpu as pltpu
from jax.sharding import Mesh
from jax.sharding import PartitionSpec as P

DOMAINS = 128
STEPS = 3
DP = ("dp_0", "dp_1", "dp_2")
DP_TENSOR = ("dp_0", "dp_1", "dp_2", "tensor")
AXIS = {"x": "dp_0", "y": "dp_1", "z": "tensor"}
MESH = pl.DeviceIdType.MESH
DMA = pltpu.SemaphoreType.DMA

step_size = 1.0
smoothing = 0.001

KB = 1024
RATE = 46.6e3
HOP = 3.5
BACKLOG = 1.5
LAG = 0.6
FINE = (0, 1, -1)
AHEAD = 20
CHECKPOINTS = range(140, 400, 10)
RING4 = (0, 1, -1, 2)
RING8 = (0, 1, -1, 2, -2, 3, -3, 4)
PLANE = [(dx, dy) for dx in (2, 1, 3, 0) for dy in (2, 1, 3, 0) if dx or dy]
PLANE.sort(key=lambda p: -min(p[0], 4 - p[0]) - min(p[1], 4 - p[1]))


def ring(add, axis, size, token, need, far, rank, arrival, lag=0.01):
    for k in range(1, far + 1):
        halves = (0, 1) if k == far else (None, None)
        for sign, half in ((1, halves[0]), (-1, halves[1])):
            offset = far if k == far else -sign * k
            add(
                dict(
                    axis=axis,
                    sign=sign,
                    size=size // 2 if k == far else size,
                    source=token(-sign * (k - 1), half),
                    need=need if k == 1 else [token(-sign * (k - 1), None)],
                    given=token(offset, half),
                    rank=rank + lag * (k - 1),
                    arrival=arrival + (offset,),
                )
            )


def gather_plan():
    copies = []
    add = copies.append
    piece = 32 * KB
    for colour, first, last in (("A", "y", "x"), ("B", "x", "y")):
        own = [(colour, "z", 0, None)]
        ring(add, "z", piece, lambda d, h: (colour, "z", d, h), own, 4, 0, ("AB", "z"))
        for q, dz in enumerate(RING8):
            have = [(colour, "z", dz, None)]
            ring(add, first, piece, lambda d, h: (colour, "f", dz, d, h), have, 2, 1, ("AB", "f", dz))
            rank = 3 + 0.1 * q
            if dz in FINE:
                for df in RING4:
                    need = have if df == 0 else [(colour, "f", dz, df, None)]
                    token = lambda d, h: (colour, "p", dz, df, d, h)
                    ring(add, last, piece, token, need, 2, rank, ("AB", "p", dz, abs(df)), LAG)
            else:
                need = have + [(colour, "f", dz, d, None) for d in (1, -1, 2)]
                token = lambda d, h: (colour, "l", dz, d, h)
                ring(add, last, 4 * piece, token, need, 2, rank, ("AB", "l", dz), LAG)
    piece = 16 * KB
    own = [("C", "o", 0, None)]
    ring(add, "z", 2 * piece, lambda d, h: ("C", "o", d, h), own, 4, 2, ("C", "o"))
    for colour, first, last in (("C0", "x", "y"), ("C1", "y", "x")):
        ring(add, first, piece, lambda d, h: (colour, "f", d, h), own, 2, 0, ("C", "f"))
        need = own + [(colour, "f", d, None) for d in (1, -1, 2)]
        ring(add, last, 4 * piece, lambda d, h: (colour, "l", d, h), need, 2, 0, ("C", "l"))
        for j in (1, -1, 2):
            need = [(colour, "f", j, None)]
            ring(add, "z", piece, lambda d, h: (colour, "y", j, d, h), need, 4, 2, ("C", "y", j))
        for j in (1, -1, 2):
            need = [(colour, "l", j, None)]
            ring(add, "z", 4 * piece, lambda d, h: (colour, "z", j, d, h), need, 4, 2, ("C", "z", j))
    return copies


OWN = {("A", "z", 0, None), ("B", "z", 0, None), ("C", "o", 0, None)}


def tokens_of(group, dzs):
    out = []
    for dz in dzs:
        if group == "C":
            if dz:
                out.append(("C", "o", dz, None))
            for colour in ("C0", "C1"):
                for j in (1, -1, 2):
                    if dz:
                        out += [(colour, "y", j, dz, None), (colour, "z", j, dz, None)]
                    else:
                        out += [(colour, "f", j, None), (colour, "l", j, None)]
            continue
        for colour in ("A", "B"):
            if group == 0:
                out += [(colour, "z", dz, None)] + [(colour, "f", dz, d, None) for d in (1, -1, 2)]
                continue
            for d in (1, -1) if group == 1 else (2,):
                if dz in FINE:
                    out += [(colour, "p", dz, df, d, None) for df in RING4]
                else:
                    out.append((colour, "l", dz, d, None))
    return out


WORK = [
    (0, (0,)), (0, (1, -1)), (0, (2, -2)), (0, (3, -3, 4)),
    (1, (0,)), (1, (1, -1)), (1, (2, -2)), (1, (3, -3)), (1, (4,)),
    (2, (0,)), (2, (1, -1)), (2, (2, -2)), (2, (3,)), (2, (-3,)), (2, (4,)),
    ("C", (0,)), ("C", (1, -1)), ("C", (2, -2)), ("C", (3, -3)), ("C", (4,)),
]
STATS_TIME = {0: 0.34, 1: 0.74, 2: 0.34, "C": 0.74}


def schedule(copies, works):
    arrival_of = {c["given"]: c["arrival"] for c in copies}
    members = {}
    for i, c in enumerate(copies):
        members.setdefault(c["arrival"], []).append(i)

    def arrivals(tokens):
        found = set()
        for t in tokens:
            if t not in OWN:
                found |= {arrival_of[p] for p in (t, t[:-1] + (0,), t[:-1] + (1,)) if p in arrival_of}
        return found

    deps = [arrivals(c["need"]) for c in copies]
    needs = [arrivals(tokens_of(*w)) for w in works]
    links = {}
    for i, c in enumerate(copies):
        links.setdefault((c["axis"], c["sign"]), []).append(i)
    got, free, landed = set(), dict.fromkeys(links, 0.0), {}
    unsent, undone = set(range(len(copies))), set(range(len(works)))
    left = {g: sum(1 for w in works if w[0] == g) for g in STATS_TIME}
    now, order = 0.0, []
    while unsent or undone or len(got) < len(members):
        coming = {
            a: max(landed[i] for i in m)
            for a, m in members.items()
            if a not in got and all(i in landed for i in m)
        }
        here = sorted((when, str(a), a) for a, when in coming.items() if when <= now + 1e-9)
        if here:
            for _, _, a in here:
                got.add(a)
                order.append(("recv", a))
                now += 0.02
            continue
        sent = False
        for link, all_of in links.items():
            while free[link] - now < BACKLOG:
                ready = [i for i in all_of if i in unsent and deps[i] <= got]
                if not ready:
                    break
                i = min(ready, key=lambda i: (copies[i]["rank"], i))
                free[link] = max(now, free[link]) + copies[i]["size"] / RATE
                landed[i] = free[link] + HOP
                unsent.discard(i)
                order.append(("send", i))
                now += 0.012
                sent = True
        if sent:
            continue
        ready = [i for i in undone if needs[i] <= got]
        if ready:
            i = min(ready)
            undone.discard(i)
            order.append(("compute", i))
            now += 0.2 + 0.54 * len(works[i][1])
            left[works[i][0]] -= 1
            if not left[works[i][0]]:
                now += STATS_TIME[works[i][0]]
            continue
        times = list(coming.values())
        for link, all_of in links.items():
            if any(i in unsent and deps[i] <= got for i in all_of):
                times.append(free[link] - BACKLOG + 1e-6)
        now = max(now, min(times))
    return order


SEND_CLASS = {
    ("A", "z"): 0, ("A", "f"): 1, ("A", "p"): 2, ("A", "l"): 2,
    ("B", "z"): 3, ("B", "f"): 4, ("B", "p"): 5, ("B", "l"): 5,
    ("C", "o"): 6, ("C0", "y"): 6, ("C1", "y"): 6, ("C0", "z"): 6, ("C1", "z"): 6,
    ("C0", "f"): 7, ("C1", "f"): 7, ("C0", "l"): 8, ("C1", "l"): 8,
}


def kernel(
    copies, order, rows, tokens,
    ph, rh, pw, rw, tg, dm, kp, pr, out_excess, out_weights,
    G, W, acc0, acc1, acc2, accC, tgv, dmv, kpv, prv, M0, M1, onehot, early, late, zearly, zlate, pearly, plate, dbuf,
    keep_ref, s_send, s_recv,
):
    x, y, c, z = (lax.axis_index(a) for a in ("dp_0", "dp_1", "dp_2", "tensor"))
    other = 1 - c
    pos = {"x": (x, 4), "y": (y, 4), "z": (z, 8)}

    def at(axis, d):
        p, n = pos[axis]
        return lax.rem(p + (d % n), n) if d % n else p

    def peer(axis, d):
        return {AXIS[axis]: at(axis, d)}

    def cols(dz, half=None):
        begin = at("z", dz) * 512
        if half is None:
            return pl.ds(pl.multiple_of(begin, 512), 512)
        return pl.ds(pl.multiple_of(begin + 256 * half, 256), 256)

    def view(token):
        colour, phase, half = token[0], token[1], token[-1]
        ms = slice(0, 2) if half is None else half
        if colour in ("A", "B"):
            k = 0 if colour == "A" else 1
            last, first = ("x", "y") if colour == "A" else ("y", "x")
            dz = token[2]
            if phase == "z":
                return G.at[k, ms, at(last, 0), at(first, 0), :, cols(dz)]
            if phase == "f":
                return G.at[k, ms, at(last, 0), at(first, token[3]), :, cols(dz)]
            if phase == "p":
                return G.at[k, ms, at(last, token[4]), at(first, token[3]), :, cols(dz)]
            return G.at[k, ms, at(last, token[3]), :, :, cols(dz)]
        d = token[2]
        if colour == "C":
            return G.at[2, ms, x, y, :, cols(d)]
        if phase in ("f", "y"):
            cs = cols(0 if phase == "f" else token[3], half)
            if colour == "C0":
                return G.at[2, 0, at("x", d), y, :, cs]
            return G.at[2, 1, x, at("y", d), :, cs]
        cs = cols(0 if phase == "l" else token[3], half)
        if colour == "C0":
            return G.at[2, 0, :, at("y", d), :, cs]
        return G.at[2, 1, at("x", d), :, :, cs]

    def wait(ref, sem):
        pltpu.make_async_copy(ref, ref, sem).wait()

    f32 = jnp.float32
    lane = lax.broadcasted_iota(jnp.int32, (8, 128), 1)
    sub = lax.broadcasted_iota(jnp.int32, (8, 128), 0)

    me = x * 4 + y
    label = lax.broadcasted_iota(jnp.int32, (128, 128), 0).astype(f32)

    def spread_z(buf, value, stage):
        buf[z] = value
        for d in (4, 3, 5, 2, 6, 1, 7):
            pltpu.make_async_remote_copy(
                src_ref=buf.at[z], dst_ref=buf.at[z], send_sem=s_send.at[stage], recv_sem=s_recv.at[stage],
                device_id=peer("z", d), device_id_type=MESH,
            ).start()

    def spread_xy(buf, value, stage):
        buf[me] = value
        for dx, dy in PLANE:
            pltpu.make_async_remote_copy(
                src_ref=buf.at[me], dst_ref=buf.at[me], send_sem=s_send.at[stage], recv_sem=s_recv.at[stage],
                device_id={**peer("x", dx), **peer("y", dy)}, device_id_type=MESH,
            ).start()

    def arrived(buf, stage):
        wait(buf.at[pl.ds(0, buf.shape[0] - 1)], s_recv.at[stage])

    def joined(parts):
        peak = parts[0]
        for p in parts[1:]:
            peak = jnp.maximum(peak, p)
        total = jnp.exp(parts[0] - peak)
        for p in parts[1:]:
            total = total + jnp.exp(p - peak)
        return peak + jnp.log(total)

    def added(parts):
        total = parts[0]
        for p in parts[1:]:
            total = total + p
        return total

    def join_early(buf):
        n = buf.shape[0]
        return jnp.stack([joined([buf[s, 0] for s in range(n)]), added([buf[s, 1] for s in range(n)])])

    def join_late(buf):
        parts = [buf[s] for s in range(buf.shape[0])]
        return jnp.where(sub < 4, joined(parts), added(parts))

    def gather(own_sem, small_sem, head_sem, swap_send, swap_recv, g_send, g_recv, m_send, m_recv, pace):
        arrival_at = {}
        for cp in copies:
            arrival_at.setdefault(cp["arrival"], [len(arrival_at), 0])[1] += cp["size"]
        amounts = {
            32 * KB: G.at[0, :, 0, 0, :, pl.ds(0, 512)],
            64 * KB: G.at[0, 0, 0, :, :, pl.ds(0, 512)],
            128 * KB: G.at[0, :, 0, :, :, pl.ds(0, 512)],
            256 * KB: G.at[0:2, :, 0, :, :, pl.ds(0, 512)],
        }

        def send(i):
            cp = copies[i]
            ref = view(cp["source"])
            pltpu.make_async_remote_copy(
                src_ref=ref, dst_ref=ref,
                send_sem=g_send.at[SEND_CLASS[cp["source"][:2]]], recv_sem=g_recv.at[arrival_at[cp["arrival"]][0]],
                device_id=peer(cp["axis"], cp["sign"]), device_id_type=MESH,
            ).start()

        def receive(arrival):
            index, size = arrival_at[arrival]
            wait(amounts[size], g_recv.at[index])

        for m, src in enumerate((ph, rh)):
            for k in range(3):
                dst = G.at[k, m, y, x, :, cols(0)] if k == 1 else G.at[k, m, x, y, :, cols(0)]
                pltpu.make_async_copy(src.at[pl.ds(16 * k, 16), :], dst, own_sem).start()
        small = ((tg, tgv), (dm, dmv), (kp, kpv), (pr, prv))
        for k, (src, dst) in enumerate(small):
            pltpu.make_async_copy(src, dst, small_sem.at[k]).start()
        heads = (pw, rw)

        barrier = pltpu.get_barrier_semaphore()
        peers = [peer(a, d) for a in "xyz" for d in (1, -1)] + [{"dp_2": other}]
        for target in peers:
            pl.semaphore_signal(barrier, inc=1, device_id=target, device_id_type=MESH)
        early[...] = jnp.zeros_like(early)
        late[...] = jnp.zeros_like(late)
        M0[y] = jnp.zeros((8, 128), jnp.float32)
        with jax.named_scope("entry_barrier"):
            pl.semaphore_wait(barrier, len(peers))
        with jax.named_scope("own_blocks"):
            wait(G.at[:, :, 0, 0, :, pl.ds(0, 512)], own_sem)

        def meta_send(axis, d):
            src, dst, k = (M0.at[y], M0.at[y], 0) if axis == "y" else (M0, M1.at[x], 1)
            pltpu.make_async_remote_copy(
                src_ref=src, dst_ref=dst, send_sem=m_send.at[k], recv_sem=m_recv.at[k],
                device_id=peer(axis, d), device_id_type=MESH,
            ).start()

        def swap(m, dz, q):
            pltpu.make_async_remote_copy(
                src_ref=heads[m].at[:, cols(dz)], dst_ref=W.at[m, 1, :, cols(dz)],
                send_sem=swap_send, recv_sem=swap_recv.at[q],
                device_id={"dp_2": other}, device_id_type=MESH,
            ).start()

        accs = {0: acc0, 1: acc1, 2: acc2, "C": accC}

        def block(group, m, dz):
            cs = cols(dz)
            if group == "C":
                return G[2, m, :, :, :, cs].reshape(256, 512)
            pieces = []
            for d in {0: (0,), 1: (-1, 1), 2: (2,)}[group]:
                pieces.append(G[0, m, at("x", d), :, :, cs].reshape(64, 512))
                pieces.append(G[1, m, at("y", d), :, :, cs].reshape(64, 512))
            return jnp.concatenate(pieces, axis=0)

        done_heads = set()

        def compute(i):
            group, dzs = WORK[i]
            if not done_heads:
                wait(W.at[:, 0], head_sem)
            for dz in dzs:
                if dz not in done_heads:
                    wait(W.at[:, 1, :, cols(dz)], swap_recv.at[RING8.index(dz)])
                    done_heads.add(dz)
            acc = accs[group]
            first = 0 in dzs

            for m in (0, 1):
                rhs = [block(group, m, dz) for dz in dzs]
                for h in (0, 1):
                    total = None
                    for dz, r in zip(dzs, rhs):
                        part = lax.dot_general(
                            W[m, h, :, cols(dz)], r, (((1,), (1,)), ((), ())), preferred_element_type=f32
                        )
                        total = part if total is None else total + part
                    acc[m, h] = total if first else acc[m, h] + total

        dev = ((x * 4 + y) * 2 + c) * 8 + z
        dev_other = ((x * 4 + y) * 2 + other) * 8 + z
        offsets = (dev * rows, dev_other * rows)

        def spread(quantity):
            j = lax.broadcasted_iota(jnp.int32, (128, 128), 0)
            l = lax.broadcasted_iota(jnp.int32, (128, 128), 1)
            low = l % 16
            sel_ab = (j == low + jnp.where(l < 64, 0, 16)).astype(f32)
            sel_c = (j == low + 32).astype(f32)
            ab = jnp.dot(quantity, sel_ab, precision=lax.Precision.HIGHEST, preferred_element_type=f32)
            cc = jnp.dot(quantity, sel_c, precision=lax.Precision.HIGHEST, preferred_element_type=f32)
            d = lax.broadcasted_iota(jnp.int32, (16, 128), 0)
            l = lax.broadcasted_iota(jnp.int32, (16, 128), 1)
            q = (l // 16) % 4
            result = jnp.zeros((8, 128), f32)
            for a in range(4):
                owner = jnp.where(l < 64, a * 4 + q, q * 4 + a)
                row = jnp.sum(jnp.where(d == owner, ab, 0.0), axis=0, keepdims=True)
                result = jnp.where(sub == a, row, result)
            for a in range(2):
                owner = (2 * a + l // 64) * 4 + q
                row = jnp.sum(jnp.where(d == owner, cc, 0.0), axis=0, keepdims=True)
                result = jnp.where(sub == 4 + a, row, result)
            return result

        def stats(group, wanted):
            acc = accs[group]
            width = acc.shape[-1]
            if group == "C":
                spots = [jnp.full((8, 128), b, jnp.int32) for b in range(2)]
                want = [wanted[4 + b : 5 + b, :] for b in range(2)]
            else:
                spots = [
                    jnp.where(lane < 64, at("x", d), at("y", d)) for d in {0: (0,), 1: (-1, 1), 2: (2,)}[group]
                ]
                want = [jnp.sum(jnp.where(sub == p, wanted, 0.0), axis=0, keepdims=True) for p in spots]
            want = jnp.concatenate(want, axis=1).astype(jnp.int32) if len(want) > 1 else want[0].astype(jnp.int32)
            vocab = lax.broadcasted_iota(jnp.int32, (rows, width), 0)
            lses, hits = [], []
            for m in (0, 1):
                peak = jnp.maximum(
                    jnp.max(acc[m, 0], axis=0, keepdims=True), jnp.max(acc[m, 1], axis=0, keepdims=True)
                )
                total = jnp.zeros((1, width), f32)
                hit = jnp.zeros((1, width), f32)
                for h in (0, 1):
                    logits = acc[m, h]
                    total += jnp.sum(jnp.exp(logits - peak), axis=0, keepdims=True)
                    match = vocab == want - offsets[h]
                    hit += jnp.sum(jnp.where(match, logits, 0.0), axis=0, keepdims=True)
                lses.append(peak + jnp.log(total))
                hits.append(hit)
            for b, spot in enumerate(spots):
                one, two, hit = (r[:, 128 * b : 128 * (b + 1)] for r in (lses[0], lses[1], hits[0] - hits[1]))
                if group == "C":
                    value = jnp.where(sub == spot, one, late[...])
                    value = jnp.where(sub == spot + 2, two, value)
                    late[...] = jnp.where(sub == spot + 4, hit, value)
                else:
                    value = jnp.where(sub == spot, one, early[0])
                    early[0] = jnp.where(sub == spot + 4, two, value)
                    early[1] = jnp.where(sub == spot, hit, early[1])

        tables = {}
        pending = {g: sum(1 for w in WORK if w[0] == g) for g in accs}
        steps = computes = 0
        assert CHECKPOINTS[-1] < len(order)
        for position, (kind, i) in enumerate(order):
            if position in CHECKPOINTS:
                @pl.when(c == 0)
                def _():
                    pl.semaphore_signal(pace, inc=1, device_id={"dp_2": other}, device_id_type=MESH)
            if position + AHEAD in CHECKPOINTS:
                @pl.when(c == 1)
                def _():
                    pl.semaphore_wait(pace, 1)
            if kind == "send":
                send(i)
            elif kind == "recv":
                if not steps:
                    for q, dz in enumerate(RING8):
                        for m in (0, 1):
                            swap(m, dz, q)
                    for m in (0, 1):
                        pltpu.make_async_copy(heads[m], W.at[m, 0], head_sem).start()
                    with jax.named_scope("small_inputs"):
                        for k, (src, dst) in enumerate(small):
                            pltpu.make_async_copy(src, dst, small_sem.at[k]).wait()
                    for k, ref in enumerate((tgv, dmv, kpv)):
                        M0[y, k : k + 1, 0:tokens] = ref[...].astype(f32)
                steps += 1
                with jax.named_scope("recv"):
                    receive(i)
            else:
                if computes == 0:
                    for d in (1, 2, 3):
                        meta_send("y", d)
                if computes == 3:
                    wait(M0.at[pl.ds(0, 3)], m_recv.at[0])
                    M1[x] = M0[...]
                    for d in (1, 2, 3):
                        meta_send("x", d)
                computes += 1
                with jax.named_scope(f"compute_{i}"):
                    compute(i)
                group = WORK[i][0]
                pending[group] -= 1
                if not pending[group]:
                    if not tables:
                        wait(M1.at[pl.ds(0, 3)], m_recv.at[1])
                        for k, name in enumerate(("targets", "domains", "keep")):
                            tables[name] = spread(M1[:, :, k, :].reshape(16, 128))
                        onehot[...] = jnp.concatenate(
                            [(tables["domains"][b : b + 1, :] == label).astype(jnp.bfloat16) for b in range(6)], axis=1
                        )
                    with jax.named_scope(f"stats_{group}"):
                        stats(group, tables["targets"])
                    if group == "C":
                        spread_z(zlate, late[...], 1)
                    elif not any(pending[g] for g in (0, 1, 2)):
                        spread_z(zearly, early[...], 0)

        keep_ref[...] = tables["keep"]
        with jax.named_scope("sends_done"):
            for k in range(2):
                wait(G.at[k, :, 0, 0, :, pl.ds(0, 7 * 512)], g_send.at[3 * k])
                wait(G.at[k, :, 0, pl.ds(0, 3)], g_send.at[3 * k + 1])
                wait(G.at[k, :, pl.ds(0, 3)], g_send.at[3 * k + 2])
            wait(G.at[2, :, :, :, :, pl.ds(0, 7 * 512)], g_send.at[6])
            wait(G.at[2, :, pl.ds(0, 3), 0, :, pl.ds(0, 512)], g_send.at[7])
            wait(G.at[2, :, pl.ds(0, 3), :, :, pl.ds(0, 512)], g_send.at[8])
            wait(W.at[:, 1], swap_send)
            wait(M0.at[pl.ds(0, 3)], m_send.at[0])
            wait(M1.at[pl.ds(0, 3)], m_send.at[1])

    pl.run_scoped(
        gather, DMA, DMA((4,)), DMA, DMA, DMA((8,)), DMA((9,)),
        DMA((len({cp["arrival"] for cp in copies}),)), DMA((2,)), DMA((2,)), pltpu.SemaphoreType.REGULAR,
    )

    keep = keep_ref[...]
    q = (lane // 16) % 4
    owner = jnp.where(sub < 4, jnp.where(lane < 64, sub * 4 + q, q * 4 + sub), (2 * (sub - 4) + lane // 64) * 4 + q)
    colour = jnp.where(sub < 4, jnp.where(lane < 64, 0, 1), 2)
    batch = ((owner * 2 + c) * 48 + 16 * colour + lane % 16) // 512

    def domain_sums(clipped, first, last):
        left = []
        for b in range(first, last):
            bb = batch[b : b + 1, :]
            top = jnp.where(bb == sub, clipped[b - first : b - first + 1, :], 0.0)
            low_rows = jnp.where(bb == sub - 3, keep[b : b + 1, :], 0.0)
            left.append(jnp.where(sub < 3, top, low_rows))
        left = jnp.concatenate(left, axis=1)
        thirds = []
        for _ in range(3):
            third = left.astype(jnp.bfloat16)
            thirds.append(third)
            left = left - third.astype(f32)
        parts = lax.dot_general(
            jnp.concatenate(thirds, axis=0), onehot[:, 128 * first : 128 * last], (((1,), (1,)), ((), ())),
            preferred_element_type=f32,
        )
        return parts[0:8] + (parts[8:16] + parts[16:24])

    def picked(values, spots):
        row = jnp.sum(jnp.where(spots, values, 0.0), axis=0, keepdims=True)
        row = jnp.broadcast_to(row, (8, 128))
        for shift in (64, 32, 16):
            row = row + pltpu.roll(row, shift, 1)
        return row

    with jax.named_scope("exchange_z"):
        arrived(zearly, 0)
        spread_xy(pearly, join_early(zearly), 2)
        with jax.named_scope("late_z"):
            arrived(zlate, 1)
        spread_xy(plate, join_late(zlate), 3)
    with jax.named_scope("exchange_xy"):
        arrived(pearly, 2)
        pair = join_early(pearly)
        gap_early = (pair[0, 0:4] - pair[0, 4:8]) - pair[1, 0:4]
        sums_early = domain_sums(jnp.maximum(gap_early, 0.0) * keep[0:4], 0, 4)
        nothing = jnp.zeros((4, 128), f32)
        excess = jnp.concatenate([gap_early, nothing], axis=0) * keep
        mine_a = picked(excess, (owner == me) & (colour == 0))
        mine_b = picked(excess, (owner == me) & (colour == 1))
        with jax.named_scope("late_xy"):
            arrived(plate, 3)
    tile = join_late(plate)
    gap_late = (tile[0:2] - tile[2:4]) - tile[4:6]
    sums = sums_early + domain_sums(jnp.maximum(gap_late, 0.0) * keep[4:6], 4, 6)
    dbuf[c] = sums

    def last_copy(slot):
        return pltpu.make_async_remote_copy(
            src_ref=dbuf.at[slot], dst_ref=dbuf.at[slot], send_sem=s_send.at[4], recv_sem=s_recv.at[4],
            device_id={"dp_2": other}, device_id_type=MESH,
        )

    last_copy(c).start()
    excess = jnp.concatenate([nothing, gap_late, nothing[0:2]], axis=0) * keep
    mine_c = picked(excess, (owner == me) & (colour == 2) & (sub < 6))
    mine_row = jnp.where(lane < 16, mine_a, jnp.where(lane < 32, mine_b, mine_c))[0:1, :]
    prior = prv[...]
    weights = prior / jnp.sum(prior, axis=1, keepdims=True)
    with jax.named_scope("partner_sums"):
        last_copy(other).wait_recv()
    both = dbuf[0] + dbuf[1]
    for s in range(STEPS):
        gain = both[s : s + 1, :] / jnp.maximum(both[3 + s : 4 + s, :], 1.0)
        raised = weights * jnp.exp(step_size * gain)
        weights = (1.0 - smoothing) * raised / jnp.sum(raised, axis=1, keepdims=True) + smoothing / DOMAINS
    out_weights[...] = jnp.log(weights)
    out_excess[...] = mine_row[:, 0:tokens]

    with jax.named_scope("sends_done"):
        for k, buf in enumerate((zearly, zlate, pearly, plate)):
            wait(buf.at[pl.ds(0, buf.shape[0] - 1)], s_send.at[k])
        last_copy(c).wait_send()


def local(ph, rh, pw, rw, targets, domains, keep_mask, prior):
    rows, tokens = pw.shape[0], targets.shape[0]
    copies = gather_plan()
    order = schedule(copies, WORK)
    f32, bf16 = jnp.float32, jnp.bfloat16
    anywhere = pl.BlockSpec(memory_space=pltpu.HBM)
    inside = pl.BlockSpec(memory_space=pltpu.VMEM)

    def body(*refs):
        kernel(copies, order, rows, tokens, *refs)

    out = pl.pallas_call(
        body,
        name="doremi",
        out_shape=[jax.ShapeDtypeStruct((1, tokens), f32), jax.ShapeDtypeStruct((1, 128), f32)],
        in_specs=[anywhere] * 8,
        out_specs=[inside] * 2,
        scratch_shapes=[
            pltpu.VMEM((3, 2, 4, 4, 16, 4096), bf16),
            pltpu.VMEM((2, 2, rows, 4096), bf16),
            pltpu.VMEM((2, 2, rows, 128), f32),
            pltpu.VMEM((2, 2, rows, 256), f32),
            pltpu.VMEM((2, 2, rows, 128), f32),
            pltpu.VMEM((2, 2, rows, 256), f32),
            pltpu.VMEM((1, tokens), jnp.int32),
            pltpu.VMEM((1, tokens), jnp.int32),
            pltpu.VMEM((1, tokens), jnp.int32),
            pltpu.VMEM((1, 128), f32),
            pltpu.VMEM((4, 8, 128), f32),
            pltpu.VMEM((4, 4, 8, 128), f32),
            pltpu.VMEM((128, 768), bf16),
            pltpu.VMEM((2, 8, 128), f32),
            pltpu.VMEM((8, 128), f32),
            pltpu.VMEM((8, 2, 8, 128), f32),
            pltpu.VMEM((8, 8, 128), f32),
            pltpu.VMEM((16, 2, 8, 128), f32),
            pltpu.VMEM((16, 8, 128), f32),
            pltpu.VMEM((2, 8, 128), f32),
            pltpu.VMEM((8, 128), f32),
            DMA((5,)), DMA((5,)),
        ],
        compiler_params=pltpu.CompilerParams(
            collective_id=0, has_side_effects=True, vmem_limit_bytes=53 * 1024 * 1024
        ),
        cost_estimate=pl.CostEstimate(flops=12_900_000_000, bytes_accessed=34_000_000, transcendentals=2_000_000),
    )(*(
        pltpu.with_memory_space_constraint(a, pltpu.HBM)
        for a in (ph, rh, pw, rw, targets[None], domains[None], keep_mask[None], prior[None])
    ))
    return out[0][0], out[1][0]


def solution(mesh):
    split = Mesh(
        mesh.devices.reshape(4, 4, 2, mesh.shape["tensor"]), ("dp_0", "dp_1", "dp_2", "tensor")
    )
    return jax.shard_map(
        local,
        mesh=split,
        in_specs=(
            P(DP, "tensor"),
            P(DP, "tensor"),
            P(DP_TENSOR, None),
            P(DP_TENSOR, None),
            P(DP),
            P(DP),
            P(DP),
            P(),
        ),
        out_specs=(P(DP), P()),
        check_vma=False,
    )
```
